32 devices in a mesh: ty: 8 (over z, y), tx: 4 (over x, core).
Axes of the slice: x: 2, y: 2, z: 4, core: 2. Of those that a mesh axis runs over, the one named last changes fastest.
Arguments:
- x_tok: bfloat16 [2048, 2560], P('ty', 'tx')
- dy_tok: bfloat16 [2048, 2560], P('ty', 'tx')
- ln_gain: float32 [2560], P('tx')
- w_gate: bfloat16 [2560, 10240], P('tx', 'ty')
- w_up: bfloat16 [2560, 10240], P('tx', 'ty')
- w_down: bfloat16 [10240, 2560], P('ty', 'tx')
Outputs:
- output 1: bfloat16 [2048, 2560], P('ty', 'tx')
- output 2: bfloat16 [2048, 2560], P('ty', 'tx')
- output 3: float32 [2560, 10240], P('tx', 'ty')
- output 4: float32 [2560, 10240], P('tx', 'ty')
- output 5: float32 [10240, 2560], P('ty', 'tx')
- output 6: float32 [2560], P('tx')
All inputs are finite; a program needn't handle non-finite values.
Results may differ from the reference program's by a relative error of at most 0.00128048.
Values are sent between devices in bfloat16 or wider.
A program may use at most 1 GiB of HBM per device.

```python
import jax
import jax.numpy as jnp
from jax import lax

TOKENS = 2048
D_MODEL = 2560
D_FF = 10240
LN_EPS = 1e-6


def setup_inputs(seed: int = 0) -> dict:
    key_list = jax.random.split(jax.random.key(seed), 9)
    x_tok = (jax.random.normal(key_list[0], (TOKENS, D_MODEL), jnp.float32)
             + 1.5 * jax.random.normal(key_list[1], (TOKENS, 1), jnp.float32)).astype(jnp.bfloat16)
    dy_tok = jax.random.normal(key_list[2], (TOKENS, D_MODEL), jnp.float32).astype(jnp.bfloat16)
    ln_gain = 1.0 + 0.5 * jax.random.normal(key_list[3], (D_MODEL,), jnp.float32)
    in_scale = D_MODEL ** -0.5
    w_gate = ((jax.random.normal(key_list[4], (D_MODEL, D_FF), jnp.float32)
               + jax.random.normal(key_list[5], (1, D_FF), jnp.float32)) * in_scale).astype(jnp.bfloat16)
    w_up = ((jax.random.normal(key_list[6], (D_MODEL, D_FF), jnp.float32)
             + jax.random.normal(key_list[7], (1, D_FF), jnp.float32)) * in_scale).astype(jnp.bfloat16)
    w_down = (jax.random.normal(key_list[8], (D_FF, D_MODEL), jnp.float32) * D_FF ** -0.5).astype(jnp.bfloat16)
    return {"x_tok": x_tok, "dy_tok": dy_tok, "ln_gain": ln_gain,
            "w_gate": w_gate, "w_up": w_up, "w_down": w_down}


def reference(x_tok, dy_tok, ln_gain, w_gate, w_up, w_down):
    x_float = x_tok.astype(jnp.float32)
    mean_x = jnp.mean(x_float, axis=1, keepdims=True)
    mean_sq = jnp.mean(x_float * x_float, axis=1, keepdims=True)
    inv_std = lax.rsqrt(mean_sq - mean_x * mean_x + LN_EPS)
    x_hat = (x_float - mean_x) * inv_std
    h_norm = (ln_gain * x_hat).astype(jnp.bfloat16)
    gate_pre = jnp.dot(h_norm, w_gate, preferred_element_type=jnp.float32)
    up_pre = jnp.dot(h_norm, w_up, preferred_element_type=jnp.float32)
    gate_sig = jax.nn.sigmoid(gate_pre)
    gate_swish = gate_pre * gate_sig
    act_out = (gate_swish * up_pre).astype(jnp.bfloat16)
    mlp_out = jnp.dot(act_out, w_down, preferred_element_type=jnp.float32)
    y_tok = (x_float + mlp_out).astype(jnp.bfloat16)
    dw_down = jnp.dot(act_out.T, dy_tok, preferred_element_type=jnp.float32)
    d_act = jnp.dot(dy_tok, w_down.T, preferred_element_type=jnp.float32)
    d_gate = (d_act * up_pre * gate_sig * (1.0 + gate_pre * (1.0 - gate_sig))).astype(jnp.bfloat16)
    d_up = (d_act * gate_swish).astype(jnp.bfloat16)
    dw_gate = jnp.dot(h_norm.T, d_gate, preferred_element_type=jnp.float32)
    dw_up = jnp.dot(h_norm.T, d_up, preferred_element_type=jnp.float32)
    d_hnorm = (jnp.dot(d_gate, w_gate.T, preferred_element_type=jnp.float32)
               + jnp.dot(d_up, w_up.T, preferred_element_type=jnp.float32))
    d_gain = jnp.sum(d_hnorm * x_hat, axis=0)
    d_xhat = d_hnorm * ln_gain
    dx_ln = inv_std * (d_xhat - jnp.mean(d_xhat, axis=1, keepdims=True)
                       - x_hat * jnp.mean(d_xhat * x_hat, axis=1, keepdims=True))
    dx_tok = (dy_tok.astype(jnp.float32) + dx_ln).astype(jnp.bfloat16)
    return (y_tok, dx_tok, dw_gate, dw_up, dw_down, d_gain)
```

```python
import functools

import jax
import jax.numpy as jnp
from jax import lax
from jax.experimental import pallas as pl
from jax.experimental.pallas import tpu as pltpu
from jax.sharding import PartitionSpec as P

LN_EPS = 1e-6
MESH = pl.DeviceIdType.MESH
F32 = jnp.float32
BF16 = jnp.bfloat16
NZ = 4
NTY = 8
NTX = 4


def contract_rows(left_op, right_op):
    return lax.dot_general(left_op, right_op, (((0,), (0,)), ((), ())), preferred_element_type=F32)


def contract_cols(left_op, right_op):
    return lax.dot_general(left_op, right_op, (((1,), (1,)), ((), ())), preferred_element_type=F32)


def remote(src, dst, send_sem, recv_sem, device):
    return pltpu.make_async_remote_copy(src_ref=src, dst_ref=dst, send_sem=send_sem, recv_sem=recv_sem,
                                        device_id=device, device_id_type=MESH)


def gather_kernel(x_ref, dy_ref, gain_ref, w1_ref, w3_ref, w2_ref,
                  a_out, du_out, dv_out, hq_out, dyq_out, stat_out,
                  h_buf, dy_buf, w1f, w3f, w2f, u_buf, v_buf, a_buf, du_buf, dv_buf, st_src, st_buf,
                  st_s, st_r, x_s, x_r, up_s, dn_s, z_r, y_s, y_r, d_s, d_r, w_s, w_r, w_l, e_s, e_r, e_l, o_l):
    ty, tx = lax.axis_index("ty"), lax.axis_index("tx")
    z, y, core = ty // 2, ty % 2, tx % 2
    yp, up, dn = ty + 1 - 2 * y, ty + 2, ty - 2
    cp, xp, dp = tx + 1 - 2 * core, (tx + 2) % NTX, NTX - 1 - tx
    tb, dq = x_ref.shape
    d_model = dq * NTX
    fh = w1_ref.shape[1] // 2

    barrier = pltpu.get_barrier_semaphore()
    for dev in ((yp, tx), (ty, cp), (ty, xp), (ty, dp)):
        pl.semaphore_signal(barrier, inc=1, device_id=dev, device_id_type=MESH)

    @pl.when(z < NZ - 1)
    def _():
        pl.semaphore_signal(barrier, inc=1, device_id=(up, tx), device_id_type=MESH)

    @pl.when(z > 0)
    def _():
        pl.semaphore_signal(barrier, inc=1, device_id=(dn, tx), device_id_type=MESH)

    x_float = x_ref[...].astype(F32)
    lane = lax.broadcasted_iota(jnp.int32, (tb, 128), 1)
    sum_1 = jnp.sum(x_float, axis=1, keepdims=True)
    sum_2 = jnp.sum(x_float * x_float, axis=1, keepdims=True)
    packed = jnp.where(lane == 0, sum_1, jnp.where(lane == 1, sum_2, 0.0))
    st_src[...] = packed.T[:8]

    pl.semaphore_wait(barrier, 5 + z * (NZ - 1 - z) // 2)

    tx_peers = ((0, cp), (1, xp), (2, dp))
    bufs = (h_buf, dy_buf)

    def block(t, q, row_ty):
        return bufs[t].at[pl.ds(pl.multiple_of(row_ty * tb, tb), tb), pl.ds(pl.multiple_of(q * dq, dq), dq)]

    def quarter(s, q):
        return q if s == 0 else (q + 2) % NTX

    def stat_copy(r, dev):
        return remote(st_src, st_buf.at[r], st_s.at[r], st_r.at[r], (ty, dev))

    def x_copy(t):
        ref = block(t, tx, ty)
        return remote(ref, ref, x_s.at[t], x_r.at[t], (ty, xp))

    def x_arrive(t):
        ref = block(t, xp, ty)
        return remote(ref, ref, x_s.at[t], x_r.at[t], (ty, xp))

    def z_copy(t, s, layer, sem, dev):
        ref = block(t, quarter(s, tx), layer * 2 + y)
        return remote(ref, ref, sem.at[t, s, layer], z_r.at[t, s, layer], (dev, tx))

    def y_copy(t, s, layer, row_ty):
        ref = block(t, quarter(s, tx), row_ty)
        return remote(ref, ref, y_s.at[t, s, layer], y_r.at[t, s, layer], (yp, tx))

    def d_copy(t, s, row_ty, q):
        ref = block(t, quarter(s, q), row_ty)
        return remote(ref, ref, d_s.at[t, s, row_ty], d_r.at[t, s, row_ty], (ty, cp))

    def spread(t, s, layer):
        y_copy(t, s, layer, layer * 2 + y).start()
        d_copy(t, s, layer * 2 + y, tx).start()

    def send_own(t, s):
        @pl.when(z < NZ - 1)
        def _():
            z_copy(t, s, z, up_s, up).start()

        @pl.when(z > 0)
        def _():
            z_copy(t, s, z, dn_s, dn).start()

        spread(t, s, z)

    w_shards = (w1_ref, w3_ref, w2_ref)
    w_full = (w1f, w3f, w2f)

    def w_copy(w, r, dev):
        half = pl.ds(pl.multiple_of((dev % 2) * fh, fh), fh)
        mine = pl.ds(pl.multiple_of(tx * dq, dq), dq)
        src = w_shards[w].at[half, :] if w == 2 else w_shards[w].at[:, half]
        dst = w_full[w].at[:, mine] if w == 2 else w_full[w].at[mine, :]
        return remote(src, dst, w_s.at[w, r], w_r.at[w, r], (ty, dev))

    def w_arrive(w, r, dev):
        theirs = pl.ds(pl.multiple_of(dev * dq, dq), dq)
        dst = w_full[w].at[:, theirs] if w == 2 else w_full[w].at[theirs, :]
        return remote(dst, dst, w_s.at[w, r], w_r.at[w, r], (ty, dev))

    def w_local(w):
        half = pl.ds(pl.multiple_of(core * fh, fh), fh)
        mine = pl.ds(pl.multiple_of(tx * dq, dq), dq)
        src = w_shards[w].at[half, :] if w == 2 else w_shards[w].at[:, half]
        dst = w_full[w].at[:, mine] if w == 2 else w_full[w].at[mine, :]
        return pltpu.make_async_copy(src, dst, w_l.at[w])

    for r, dev in tx_peers:
        stat_copy(r, dev).start()
    own_rows = pl.ds(pl.multiple_of(ty * tb, tb), tb)
    own_cols = pl.ds(pl.multiple_of(tx * dq, dq), dq)
    dy_buf[own_rows, own_cols] = dy_ref[...]
    for w in range(3):
        w_local(w).start()
        w_copy(w, 0, cp).start()
    x_copy(1).start()
    send_own(1, 0)
    for r, dev in tx_peers:
        stat_copy(r, dev).wait_recv()
    total = st_src[...] + st_buf[0] + st_buf[1] + st_buf[2]
    total = jnp.concatenate([total, jnp.zeros((120, tb), F32)], axis=0).T
    mean_x = total[:, 0:1] / d_model
    inv_std = lax.rsqrt(total[:, 1:2] / d_model - mean_x * mean_x + LN_EPS)
    x_hat = (x_float - mean_x) * inv_std
    h_buf[own_rows, own_cols] = (gain_ref[...] * x_hat).astype(BF16)
    stat_out[...] = jnp.where(lane == 0, mean_x, jnp.where(lane == 1, inv_std, 0.0))
    x_copy(0).start()
    send_own(0, 0)
    for w in range(3):
        w_copy(w, 1, xp).start()
        w_copy(w, 2, dp).start()

    for t in (1, 0):
        x_arrive(t).wait_recv()
        send_own(t, 1)
    order = ((1, 0), (0, 0), (1, 1), (0, 1))
    for k in range(1, NZ):
        for t, s in order:
            @pl.when(z >= k)
            def _():
                layer = z - k
                z_copy(t, s, layer, up_s, dn).wait_recv()

                @pl.when(z < NZ - 1)
                def _():
                    z_copy(t, s, layer, up_s, up).start()

                spread(t, s, layer)

            @pl.when(z + k < NZ)
            def _():
                layer = z + k
                z_copy(t, s, layer, dn_s, up).wait_recv()

                @pl.when(z > 0)
                def _():
                    z_copy(t, s, layer, dn_s, dn).start()

                spread(t, s, layer)

    def wait_w(w):
        w_local(w).wait()
        for r, dev in tx_peers:
            w_arrive(w, r, dev).wait_recv()

    def up_proj(row_ty):
        rows = pl.ds(pl.multiple_of(row_ty * tb, tb), tb)
        for s in (0, 1):
            d_copy(0, s, row_ty, cp).wait_recv()
        h_rows = h_buf[rows, :]
        u_buf[rows, :] = jnp.dot(h_rows, w1f[...], preferred_element_type=F32)
        v_buf[rows, :] = jnp.dot(h_rows, w3f[...], preferred_element_type=F32)

    wait_w(0)
    wait_w(1)

    def own_y(n, _):
        up_proj(n * 2 + y)
        return 0

    def other_y(n, _):
        row_ty = n * 2 + 1 - y
        for t, s in order:
            y_copy(t, s, n, row_ty).wait_recv()
            d_copy(t, s, row_ty, tx).start()
        up_proj(row_ty)
        return 0

    lax.fori_loop(0, NZ, own_y, 0)
    lax.fori_loop(0, NZ, other_y, 0)

    hq_copy = pltpu.make_async_copy(h_buf.at[:, own_cols], hq_out, o_l.at[0])
    dyq_copy = pltpu.make_async_copy(dy_buf.at[:, own_cols], dyq_out, o_l.at[1])
    hq_copy.start()
    dyq_copy.start()
    wait_w(2)

    res_bufs = (a_buf, du_buf, dv_buf)
    res_outs = (a_out, du_out, dv_out)

    def e_copy(i, row_ty, c):
        rows = pl.ds(pl.multiple_of(row_ty * tb, tb), tb)
        cols = pl.ds(pl.multiple_of(c * fh, fh), fh)
        return remote(res_bufs[i].at[rows, :], res_outs[i].at[rows, cols], e_s.at[i, row_ty], e_r.at[i, row_ty],
                      (ty, cp))

    def e_local(i, row_ty):
        rows = pl.ds(pl.multiple_of(row_ty * tb, tb), tb)
        cols = pl.ds(pl.multiple_of(core * fh, fh), fh)
        return pltpu.make_async_copy(res_bufs[i].at[rows, :], res_outs[i].at[rows, cols], e_l.at[i, row_ty])

    def down_proj(row_ty, _):
        rows = pl.ds(pl.multiple_of(row_ty * tb, tb), tb)
        for s in (0, 1):
            d_copy(1, s, row_ty, cp).wait_recv()
        d_act = contract_cols(dy_buf[rows, :], w2f[...])
        gate, up_v = u_buf[rows, :], v_buf[rows, :]
        sig = jax.nn.sigmoid(gate)
        swish = gate * sig
        a_buf[rows, :] = (swish * up_v).astype(BF16)
        du_buf[rows, :] = (d_act * up_v * sig * (1.0 + gate * (1.0 - sig))).astype(BF16)
        dv_buf[rows, :] = (d_act * swish).astype(BF16)

        @pl.when(row_ty > 0)
        def _():
            for i in range(3):
                e_copy(i, row_ty - 1, core).start()
                e_local(i, row_ty - 1).start()

        return 0

    lax.fori_loop(0, NTY, down_proj, 0)
    for i in range(3):
        e_copy(i, NTY - 1, core).start()
        e_local(i, NTY - 1).start()

    for r, dev in tx_peers:
        stat_copy(r, dev).wait_send()
        for w in range(3):
            w_copy(w, r, dev).wait_send()
    for t in (0, 1):
        x_copy(t).wait_send()

    def drain(layer, _):
        for t, s in order:
            @pl.when(jnp.logical_and(z < NZ - 1, layer <= z))
            def _():
                z_copy(t, s, layer, up_s, up).wait_send()

            @pl.when(jnp.logical_and(z > 0, layer >= z))
            def _():
                z_copy(t, s, layer, dn_s, dn).wait_send()

            y_copy(t, s, layer, layer * 2 + y).wait_send()
            d_copy(t, s, layer * 2, tx).wait_send()
            d_copy(t, s, layer * 2 + 1, tx).wait_send()
        return 0

    lax.fori_loop(0, NZ, drain, 0)

    def drain_e(row_ty, _):
        for i in range(3):
            e_copy(i, row_ty, core).wait_send()
            e_copy(i, row_ty, 1 - core).wait_recv()
            e_local(i, row_ty).wait()
        return 0

    lax.fori_loop(0, NTY, drain_e, 0)
    hq_copy.wait()
    dyq_copy.wait()


def gather_step(x_blk, dy_blk, gain_blk, w1, w3, w2):
    tb, dq = x_blk.shape
    tokens, d_model, f_loc = tb * NTY, dq * NTX, w1.shape[1]
    fh = f_loc // 2
    dma = pltpu.SemaphoreType.DMA
    vmem = pl.BlockSpec(memory_space=pltpu.VMEM)
    hbm = pl.BlockSpec(memory_space=pl.ANY)
    return pl.pallas_call(
        gather_kernel,
        out_shape=(
            [jax.ShapeDtypeStruct((tokens, f_loc), BF16)] * 3
            + [jax.ShapeDtypeStruct((tokens, dq), BF16)] * 2
            + [jax.ShapeDtypeStruct((tb, 128), F32)]),
        in_specs=[vmem, vmem, vmem, hbm, hbm, hbm],
        out_specs=[hbm] * 5 + [vmem],
        scratch_shapes=[
            pltpu.VMEM((tokens, d_model), BF16), pltpu.VMEM((tokens, d_model), BF16),
            pltpu.VMEM((d_model, fh), BF16), pltpu.VMEM((d_model, fh), BF16), pltpu.VMEM((fh, d_model), BF16),
            pltpu.VMEM((tokens, fh), F32), pltpu.VMEM((tokens, fh), F32),
            pltpu.VMEM((tokens, fh), BF16), pltpu.VMEM((tokens, fh), BF16), pltpu.VMEM((tokens, fh), BF16),
            pltpu.VMEM((8, tb), F32), pltpu.VMEM((3, 8, tb), F32),
            dma((3,)), dma((3,)), dma((2,)), dma((2,)),
            dma((2, 2, NZ)), dma((2, 2, NZ)), dma((2, 2, NZ)), dma((2, 2, NZ)), dma((2, 2, NZ)),
            dma((2, 2, NTY)), dma((2, 2, NTY)),
            dma((3, 3)), dma((3, 3)), dma((3,)),
            dma((3, NTY)), dma((3, NTY)), dma((3, NTY)), dma((2,)),
        ],
        compiler_params=pltpu.CompilerParams(collective_id=0, has_side_effects=True,
                                             vmem_limit_bytes=66_000_000),
        cost_estimate=pl.CostEstimate(flops=6 * tokens * d_model * fh, bytes_accessed=40_000_000,
                                      transcendentals=tokens * fh),
    )(x_blk, dy_blk, gain_blk, w1, w3, w2)


def solution(mesh):
    tx_size = mesh.shape["tx"]

    def local_step(x_blk, dy_blk, gain_blk, w_gate_blk, w_up_blk, w_down_blk):
        d_model = x_blk.shape[1] * tx_size
        gain_row = gain_blk[None, :]
        act_all, d_gate_all, d_up_all, h_all, dy_all, stats = gather_step(
            x_blk, dy_blk, gain_row, w_gate_blk, w_up_blk, w_down_blk)
        x_float = x_blk.astype(F32)
        mean_x, inv_std = stats[:, 0:1], stats[:, 1:2]
        x_hat = (x_float - mean_x) * inv_std
        mlp_out = lax.psum_scatter(jnp.dot(act_all, w_down_blk, preferred_element_type=F32),
                                   "ty", scatter_dimension=0, tiled=True)
        y_blk = (x_float + mlp_out).astype(BF16)
        dw_down_blk = contract_rows(act_all, dy_all)
        dw_gate_blk = contract_rows(h_all, d_gate_all)
        dw_up_blk = contract_rows(h_all, d_up_all)
        d_hnorm = lax.psum_scatter(contract_cols(d_gate_all, w_gate_blk) + contract_cols(d_up_all, w_up_blk),
                                   "ty", scatter_dimension=0, tiled=True)
        d_xhat = d_hnorm * gain_blk
        bwd_stats = lax.psum(jnp.stack([jnp.sum(d_xhat, axis=1), jnp.sum(d_xhat * x_hat, axis=1)]), "tx") / d_model
        dx_ln = inv_std * (d_xhat - bwd_stats[0][:, None] - x_hat * bwd_stats[1][:, None])
        dx_blk = (dy_blk.astype(F32) + dx_ln).astype(BF16)
        d_gain_blk = lax.psum(jnp.sum(d_hnorm * x_hat, axis=0), "ty")
        return (y_blk, dx_blk, dw_gate_blk, dw_up_blk, dw_down_blk, d_gain_blk)

    return jax.shard_map(
        local_step, mesh=mesh,
        in_specs=(P("ty", "tx"), P("ty", "tx"), P("tx"), P("tx", "ty"), P("tx", "ty"), P("ty", "tx")),
        out_specs=(P("ty", "tx"), P("ty", "tx"), P("tx", "ty"), P("tx", "ty"), P("ty", "tx"), P("tx")),
        check_vma=False)
```

```python
import functools

import jax
import jax.numpy as jnp
from jax import lax
from jax.experimental import pallas as pl
from jax.experimental.pallas import tpu as pltpu
from jax.sharding import PartitionSpec as P

LN_EPS = 1e-6
MESH = pl.DeviceIdType.MESH
F32 = jnp.float32
BF16 = jnp.bfloat16
NZ = 4
NTY = 8
NTX = 4
SUB = 64
SUBS = 4
LAG = 2


def contract_rows(left_op, right_op):
    return lax.dot_general(left_op, right_op, (((0,), (0,)), ((), ())), preferred_element_type=F32)


def contract_cols(left_op, right_op):
    return lax.dot_general(left_op, right_op, (((1,), (1,)), ((), ())), preferred_element_type=F32)


def remote(src, dst, send_sem, recv_sem, device):
    return pltpu.make_async_remote_copy(src_ref=src, dst_ref=dst, send_sem=send_sem, recv_sem=recv_sem,
                                        device_id=device, device_id_type=MESH)


def gather_kernel(x_ref, dy_ref, gain_ref, w1_ref, w3_ref, w2_ref,
                  a_out, du_out, dv_out, hq_out, dyq_out, stat_out,
                  h_buf, dy_buf, w1f, w3f, w2f, u_buf, v_buf, a_buf, du_buf, dv_buf, st_src, st_buf,
                  st_s, st_r, x_s, x_r, up_s, dn_s, z_r, y_s, y_r, d_s, d_r, w_s, w_r, w_l, e_s, e_r, e_l, o_l):
    ty, tx = lax.axis_index("ty"), lax.axis_index("tx")
    z, y, core = ty // 2, ty % 2, tx % 2
    yp, up, dn = ty + 1 - 2 * y, ty + 2, ty - 2
    cp, xp, dp = tx + 1 - 2 * core, (tx + 2) % NTX, NTX - 1 - tx
    tb, dq = x_ref.shape
    d_model = dq * NTX
    fh = w1_ref.shape[1] // 2

    barrier = pltpu.get_barrier_semaphore()
    for dev in ((yp, tx), (ty, cp), (ty, xp), (ty, dp)):
        pl.semaphore_signal(barrier, inc=1, device_id=dev, device_id_type=MESH)

    @pl.when(z < NZ - 1)
    def _():
        pl.semaphore_signal(barrier, inc=1, device_id=(up, tx), device_id_type=MESH)

    @pl.when(z > 0)
    def _():
        pl.semaphore_signal(barrier, inc=1, device_id=(dn, tx), device_id_type=MESH)

    x_float = x_ref[...].astype(F32)
    lane = lax.broadcasted_iota(jnp.int32, (tb, 128), 1)
    sum_1 = jnp.sum(x_float, axis=1, keepdims=True)
    sum_2 = jnp.sum(x_float * x_float, axis=1, keepdims=True)
    packed = jnp.where(lane == 0, sum_1, jnp.where(lane == 1, sum_2, 0.0))
    st_src[...] = packed.T[:8]

    pl.semaphore_wait(barrier, 5 + z * (NZ - 1 - z) // 2)

    tx_peers = ((0, cp), (1, xp), (2, dp))
    bufs = (h_buf, dy_buf)

    def block(t, q, row_ty):
        return bufs[t].at[pl.ds(pl.multiple_of(row_ty * tb, tb), tb), pl.ds(pl.multiple_of(q * dq, dq), dq)]

    def quarter(s, q):
        return q if s == 0 else (q + 2) % NTX

    def stat_copy(r, dev):
        return remote(st_src, st_buf.at[r], st_s.at[r], st_r.at[r], (ty, dev))

    def x_copy(t):
        ref = block(t, tx, ty)
        return remote(ref, ref, x_s.at[t], x_r.at[t], (ty, xp))

    def x_arrive(t):
        ref = block(t, xp, ty)
        return remote(ref, ref, x_s.at[t], x_r.at[t], (ty, xp))

    def z_copy(t, s, layer, sem, dev):
        ref = block(t, quarter(s, tx), layer * 2 + y)
        return remote(ref, ref, sem.at[t, s, layer], z_r.at[t, s, layer], (dev, tx))

    def y_copy(t, s, layer, row_ty):
        ref = block(t, quarter(s, tx), row_ty)
        return remote(ref, ref, y_s.at[t, s, layer], y_r.at[t, s, layer], (yp, tx))

    def d_copy(t, s, row_ty, q):
        ref = block(t, quarter(s, q), row_ty)
        return remote(ref, ref, d_s.at[t, s, row_ty], d_r.at[t, s, row_ty], (ty, cp))

    def spread(t, s, layer):
        y_copy(t, s, layer, layer * 2 + y).start()
        d_copy(t, s, layer * 2 + y, tx).start()

    def send_own(t, s):
        @pl.when(z < NZ - 1)
        def _():
            z_copy(t, s, z, up_s, up).start()

        @pl.when(z > 0)
        def _():
            z_copy(t, s, z, dn_s, dn).start()

        spread(t, s, z)

    w_shards = (w1_ref, w3_ref, w2_ref)
    w_full = (w1f, w3f, w2f)

    def w_copy(w, r, dev):
        half = pl.ds(pl.multiple_of((dev % 2) * fh, fh), fh)
        mine = pl.ds(pl.multiple_of(tx * dq, dq), dq)
        src = w_shards[w].at[half, :] if w == 2 else w_shards[w].at[:, half]
        dst = w_full[w].at[:, mine] if w == 2 else w_full[w].at[mine, :]
        return remote(src, dst, w_s.at[w, r], w_r.at[w, r], (ty, dev))

    def w_arrive(w, r, dev):
        theirs = pl.ds(pl.multiple_of(dev * dq, dq), dq)
        dst = w_full[w].at[:, theirs] if w == 2 else w_full[w].at[theirs, :]
        return remote(dst, dst, w_s.at[w, r], w_r.at[w, r], (ty, dev))

    def w_local(w):
        half = pl.ds(pl.multiple_of(core * fh, fh), fh)
        mine = pl.ds(pl.multiple_of(tx * dq, dq), dq)
        src = w_shards[w].at[half, :] if w == 2 else w_shards[w].at[:, half]
        dst = w_full[w].at[:, mine] if w == 2 else w_full[w].at[mine, :]
        return pltpu.make_async_copy(src, dst, w_l.at[w])

    for r, dev in tx_peers:
        stat_copy(r, dev).start()
    own_rows = pl.ds(pl.multiple_of(ty * tb, tb), tb)
    own_cols = pl.ds(pl.multiple_of(tx * dq, dq), dq)
    dy_buf[own_rows, own_cols] = dy_ref[...]
    for w in range(3):
        w_local(w).start()
        w_copy(w, 0, cp).start()
    x_copy(1).start()
    send_own(1, 0)
    for r, dev in tx_peers:
        stat_copy(r, dev).wait_recv()
    total = st_src[...] + st_buf[0] + st_buf[1] + st_buf[2]
    total = jnp.concatenate([total, jnp.zeros((120, tb), F32)], axis=0).T
    mean_x = total[:, 0:1] / d_model
    inv_std = lax.rsqrt(total[:, 1:2] / d_model - mean_x * mean_x + LN_EPS)
    x_hat = (x_float - mean_x) * inv_std
    h_buf[own_rows, own_cols] = (gain_ref[...] * x_hat).astype(BF16)
    stat_out[...] = jnp.where(lane == 0, mean_x, jnp.where(lane == 1, inv_std, 0.0))
    x_copy(0).start()
    send_own(0, 0)
    for w in range(3):
        w_copy(w, 1, xp).start()
        w_copy(w, 2, dp).start()

    for t in (1, 0):
        x_arrive(t).wait_recv()
        send_own(t, 1)
    order = ((1, 0), (0, 0), (1, 1), (0, 1))
    for k in range(1, NZ):
        for t, s in order:
            @pl.when(z >= k)
            def _():
                layer = z - k
                z_copy(t, s, layer, up_s, dn).wait_recv()

                @pl.when(z < NZ - 1)
                def _():
                    z_copy(t, s, layer, up_s, up).start()

                spread(t, s, layer)

            @pl.when(z + k < NZ)
            def _():
                layer = z + k
                z_copy(t, s, layer, dn_s, up).wait_recv()

                @pl.when(z > 0)
                def _():
                    z_copy(t, s, layer, dn_s, dn).start()

                spread(t, s, layer)

    def wait_w(w):
        w_local(w).wait()
        for r, dev in tx_peers:
            w_arrive(w, r, dev).wait_recv()

    def up_proj(row_ty):
        rows = pl.ds(pl.multiple_of(row_ty * tb, tb), tb)
        for s in (0, 1):
            d_copy(0, s, row_ty, cp).wait_recv()
        h_rows = h_buf[rows, :]
        u_buf[rows, :] = jnp.dot(h_rows, w1f[...], preferred_element_type=F32)
        v_buf[rows, :] = jnp.dot(h_rows, w3f[...], preferred_element_type=F32)

    wait_w(0)
    wait_w(1)

    def own_y(n, _):
        up_proj(n * 2 + y)
        return 0

    def other_y(n, _):
        row_ty = n * 2 + 1 - y
        for t, s in order:
            y_copy(t, s, n, row_ty).wait_recv()
            d_copy(t, s, row_ty, tx).start()
        up_proj(row_ty)
        return 0

    lax.fori_loop(0, NZ, own_y, 0)
    lax.fori_loop(0, NZ, other_y, 0)

    hq_copy = pltpu.make_async_copy(h_buf.at[:, own_cols], hq_out, o_l.at[0])
    dyq_copy = pltpu.make_async_copy(dy_buf.at[:, own_cols], dyq_out, o_l.at[1])
    hq_copy.start()
    dyq_copy.start()
    wait_w(2)

    res_bufs = (a_buf, du_buf, dv_buf)
    res_outs = (a_out, du_out, dv_out)

    def e_copy(i, row_ty, c):
        rows = pl.ds(pl.multiple_of(row_ty * tb, tb), tb)
        cols = pl.ds(pl.multiple_of(c * fh, fh), fh)
        return remote(res_bufs[i].at[rows, :], res_outs[i].at[rows, cols], e_s.at[i, row_ty], e_r.at[i, row_ty],
                      (ty, cp))

    def e_local(i, row_ty):
        rows = pl.ds(pl.multiple_of(row_ty * tb, tb), tb)
        cols = pl.ds(pl.multiple_of(core * fh, fh), fh)
        return pltpu.make_async_copy(res_bufs[i].at[rows, :], res_outs[i].at[rows, cols], e_l.at[i, row_ty])

    def down_proj(row_ty, _):
        rows = pl.ds(pl.multiple_of(row_ty * tb, tb), tb)
        for s in (0, 1):
            d_copy(1, s, row_ty, cp).wait_recv()
        d_act = contract_cols(dy_buf[rows, :], w2f[...])
        gate, up_v = u_buf[rows, :], v_buf[rows, :]
        sig = jax.nn.sigmoid(gate)
        swish = gate * sig
        a_buf[rows, :] = (swish * up_v).astype(BF16)
        du_buf[rows, :] = (d_act * up_v * sig * (1.0 + gate * (1.0 - sig))).astype(BF16)
        dv_buf[rows, :] = (d_act * swish).astype(BF16)

        @pl.when(row_ty > 0)
        def _():
            for i in range(3):
                e_copy(i, row_ty - 1, core).start()
                e_local(i, row_ty - 1).start()

        return 0

    lax.fori_loop(0, NTY, down_proj, 0)
    for i in range(3):
        e_copy(i, NTY - 1, core).start()
        e_local(i, NTY - 1).start()

    for r, dev in tx_peers:
        stat_copy(r, dev).wait_send()
        for w in range(3):
            w_copy(w, r, dev).wait_send()
    for t in (0, 1):
        x_copy(t).wait_send()

    def drain(layer, _):
        for t, s in order:
            @pl.when(jnp.logical_and(z < NZ - 1, layer <= z))
            def _():
                z_copy(t, s, layer, up_s, up).wait_send()

            @pl.when(jnp.logical_and(z > 0, layer >= z))
            def _():
                z_copy(t, s, layer, dn_s, dn).wait_send()

            y_copy(t, s, layer, layer * 2 + y).wait_send()
            d_copy(t, s, layer * 2, tx).wait_send()
            d_copy(t, s, layer * 2 + 1, tx).wait_send()
        return 0

    lax.fori_loop(0, NZ, drain, 0)

    def drain_e(row_ty, _):
        for i in range(3):
            e_copy(i, row_ty, core).wait_send()
            e_copy(i, row_ty, 1 - core).wait_recv()
            e_local(i, row_ty).wait()
        return 0

    lax.fori_loop(0, NTY, drain_e, 0)
    hq_copy.wait()
    dyq_copy.wait()


def gather_step(x_blk, dy_blk, gain_blk, w1, w3, w2):
    tb, dq = x_blk.shape
    tokens, d_model, f_loc = tb * NTY, dq * NTX, w1.shape[1]
    fh = f_loc // 2
    dma = pltpu.SemaphoreType.DMA
    vmem = pl.BlockSpec(memory_space=pltpu.VMEM)
    hbm = pl.BlockSpec(memory_space=pl.ANY)
    return pl.pallas_call(
        gather_kernel,
        out_shape=(
            [jax.ShapeDtypeStruct((tokens, f_loc), BF16)] * 3
            + [jax.ShapeDtypeStruct((tokens, dq), BF16)] * 2
            + [jax.ShapeDtypeStruct((tb, 128), F32)]),
        in_specs=[vmem, vmem, vmem, hbm, hbm, hbm],
        out_specs=[hbm] * 5 + [vmem],
        scratch_shapes=[
            pltpu.VMEM((tokens, d_model), BF16), pltpu.VMEM((tokens, d_model), BF16),
            pltpu.VMEM((d_model, fh), BF16), pltpu.VMEM((d_model, fh), BF16), pltpu.VMEM((fh, d_model), BF16),
            pltpu.VMEM((tokens, fh), F32), pltpu.VMEM((tokens, fh), F32),
            pltpu.VMEM((tokens, fh), BF16), pltpu.VMEM((tokens, fh), BF16), pltpu.VMEM((tokens, fh), BF16),
            pltpu.VMEM((8, tb), F32), pltpu.VMEM((3, 8, tb), F32),
            dma((3,)), dma((3,)), dma((2,)), dma((2,)),
            dma((2, 2, NZ)), dma((2, 2, NZ)), dma((2, 2, NZ)), dma((2, 2, NZ)), dma((2, 2, NZ)),
            dma((2, 2, NTY)), dma((2, 2, NTY)),
            dma((3, 3)), dma((3, 3)), dma((3,)),
            dma((3, NTY)), dma((3, NTY)), dma((3, NTY)), dma((2,)),
        ],
        compiler_params=pltpu.CompilerParams(collective_id=0, has_side_effects=True,
                                             vmem_limit_bytes=66_000_000),
        cost_estimate=pl.CostEstimate(flops=6 * tokens * d_model * fh, bytes_accessed=40_000_000,
                                      transcendentals=tokens * fh),
    )(x_blk, dy_blk, gain_blk, w1, w3, w2)


def scatter_kernel(x_ref, dy_ref, gain_ref, stat_ref, a_in, du_in, dv_in, hq_in, dyq_in, w1_in, w3_in, w2_in,
                   y_out, dx_out, dw1_out, dw3_out, dw2_out, dg_out,
                   a_all, du_all, dv_all, hq, dyq, w1, w3, w2, y_send, y_recv, own, z_buf, z_fin,
                   dw1_st, dw3_st, dw2_st, pack, sb_src, sb_buf, dg_buf,
                   in_l, y_s, y_r, z_s, z_r, f_r, dw_l, sb_s, sb_r, dg_s, dg_r):
    ty, tx = lax.axis_index("ty"), lax.axis_index("tx")
    z, y, core = ty // 2, ty % 2, tx % 2
    yp, up, dn = ty + 1 - 2 * y, ty + 2, ty - 2
    cp, xp, dp = tx + 1 - 2 * core, (tx + 2) % NTX, NTX - 1 - tx
    tx_peers = ((0, cp), (1, xp), (2, dp))
    tb, dq = x_ref.shape
    d_model = dq * NTX
    f_loc = w1.shape[1]
    far = z // 2 * z + (1 - z // 2) * (NZ - 1 - z)

    loads = []
    for n, (src, dst) in enumerate(((a_in, a_all), (w2_in, w2), (du_in, du_all), (dv_in, dv_all), (w1_in, w1),
                                    (w3_in, w3), (dyq_in, dyq), (hq_in, hq))):
        copy = pltpu.make_async_copy(src, dst, in_l.at[n])
        copy.start()
        loads.append(copy)

    barrier = pltpu.get_barrier_semaphore()
    for _, dev in tx_peers:
        pl.semaphore_signal(barrier, inc=1, device_id=(ty, dev), device_id_type=MESH)
    for r in range(1, NTY):
        pl.semaphore_signal(barrier, inc=1, device_id=((ty + r) % NTY, tx), device_id_type=MESH)
    pl.semaphore_wait(barrier, NTY + NTX - 2)

    def where_of(i):
        return i // (NZ * SUBS), 3 * (i % (NZ * SUBS) // SUBS) % NZ, i % SUBS

    def sub_rows(sub):
        return pl.ds(pl.multiple_of(sub * SUB, SUB), SUB)

    def y_copy(i):
        mat, layer, sub = where_of(i)
        return remote(y_send.at[mat, layer, sub_rows(sub), :], y_recv.at[mat, layer, sub_rows(sub), :],
                      y_s.at[i], y_r.at[i], (yp, tx))

    def partial(mat, row_ty):
        rows = pl.ds(pl.multiple_of(row_ty * tb, tb), tb)
        if mat == 0:
            return jnp.dot(a_all[rows, :], w2[...], preferred_element_type=F32)
        return contract_cols(du_all[rows, :], w1[...]) + contract_cols(dv_all[rows, :], w3[...])

    def send_block(mat, j):
        for sub in range(SUBS):
            y_copy((mat * NZ + j) * SUBS + sub).start()

    def partner_rows(mat):
        def step(j, _):
            layer = 3 * j % NZ
            y_send[mat, layer] = partial(mat, layer * 2 + 1 - y)

            @pl.when(j > 0)
            def _():
                send_block(mat, j - 1)

            return 0

        lax.fori_loop(0, NZ, step, 0)
        send_block(mat, NZ - 1)

    def own_rows(mat):
        def step(layer, _):
            own[mat, layer] = partial(mat, layer * 2 + y)
            return 0

        lax.fori_loop(0, NZ, step, 0)

    loads[0].wait()
    loads[1].wait()
    partner_rows(0)
    for n in range(2, 6):
        loads[n].wait()
    partner_rows(1)
    own_rows(0)
    own_rows(1)
    loads[6].wait()
    loads[7].wait()

    x_float = x_ref[...].astype(F32)
    mean_x, inv_std = stat_ref[:, 0:1], stat_ref[:, 1:2]
    dg_row = pl.ds(pl.multiple_of(ty * 8, 8), 8)
    dg_buf[dg_row, :] = jnp.zeros((8, dq), F32)
    pack[...] = jnp.zeros(pack.shape, F32)

    def z_copy_up(i):
        mat, layer, sub = where_of(i)
        return remote(own.at[mat, layer, sub_rows(sub), :], z_buf.at[i], z_s.at[i], z_r.at[i], (up, tx))

    def z_copy_dn(i):
        mat, layer, sub = where_of(i)
        return remote(own.at[mat, layer, sub_rows(sub), :], z_buf.at[i], z_s.at[i], z_r.at[i], (dn, tx))

    def z_copy_fin(i):
        mat, layer, sub = where_of(i)
        k = mat * SUBS + sub
        return remote(own.at[mat, layer, sub_rows(sub), :], z_fin.at[k], z_s.at[i], f_r.at[k], (dn, tx))

    def add_run(i):
        mat, layer, sub = where_of(i)
        z_copy_up(i).wait_recv()
        own[mat, layer, sub_rows(sub), :] = own[mat, layer, sub_rows(sub), :] + z_buf[i]

    n_items = 2 * NZ * SUBS
    chunk = 256
    n_chunks = f_loc // chunk

    def dw_copy(w, c):
        cols = pl.ds(pl.multiple_of(c * chunk, chunk), chunk)
        if w == 2:
            return pltpu.make_async_copy(dw2_st.at[cols, :], dw2_out.at[cols, :], dw_l.at[w, c])
        src, dst = ((dw1_st, dw1_out), (dw3_st, dw3_out))[w]
        return pltpu.make_async_copy(src.at[:, cols], dst.at[:, cols], dw_l.at[w, c])

    def weight_grads(slot):
        for w in (2, 0, 1):
            first = {2: 0, 0: n_chunks, 1: 2 * n_chunks}[w]

            @pl.when(jnp.logical_and(slot >= first, slot < first + n_chunks))
            def _():
                c = slot - first
                cols = pl.ds(pl.multiple_of(c * chunk, chunk), chunk)
                if w == 2:
                    dw2_st[cols, :] = contract_rows(a_all[:, cols], dyq[...])
                elif w == 0:
                    dw1_st[:, cols] = contract_rows(hq[...], du_all[:, cols])
                else:
                    dw3_st[:, cols] = contract_rows(hq[...], dv_all[:, cols])
                dw_copy(w, c).start()

    def slot_step(slot, _):
        weight_grads(slot)

        @pl.when(slot < n_items)
        def _():
            mat, layer, sub = where_of(slot)
            y_copy(slot).wait_recv()
            own[mat, layer, sub_rows(sub), :] = (own[mat, layer, sub_rows(sub), :]
                                                 + y_recv[mat, layer, sub_rows(sub), :])

        i_up = slot - LAG * z
        l_up = where_of(jnp.maximum(i_up, 0))[1]

        @pl.when(jnp.logical_and(jnp.logical_and(i_up >= 0, i_up < n_items), l_up > z))
        def _():
            @pl.when(z > 0)
            def _():
                add_run(i_up)

            z_copy_up(i_up).start()

        i_dn = slot - LAG * (NZ - 1 - z)
        l_dn = where_of(jnp.maximum(i_dn, 0))[1]

        @pl.when(jnp.logical_and(jnp.logical_and(i_dn >= 0, i_dn < n_items), l_dn < z))
        def _():
            @pl.when(z < NZ - 1)
            def _():
                add_run(i_dn)

            @pl.when(l_dn < z - 1)
            def _():
                z_copy_dn(i_dn).start()

            @pl.when(l_dn == z - 1)
            def _():
                z_copy_fin(i_dn).start()

        i_fin = slot - LAG * far
        l_fin = where_of(jnp.maximum(i_fin, 0))[1]

        @pl.when(jnp.logical_and(jnp.logical_and(i_fin >= 0, i_fin < n_items), l_fin == z))
        def _():
            mat, layer, sub = where_of(i_fin)

            @pl.when(z > 0)
            def _():
                add_run(i_fin)

            @pl.when(z < NZ - 1)
            def _():
                z_copy_fin(i_fin).wait_recv()
                own[mat, layer, sub_rows(sub), :] = own[mat, layer, sub_rows(sub), :] + z_fin[mat * SUBS + sub]

            rows = sub_rows(sub)

            @pl.when(mat == 0)
            def _():
                y_out[rows, :] = (x_ref[rows, :].astype(F32) + own[0, layer, rows, :]).astype(BF16)

            @pl.when(mat == 1)
            def _():
                d_h = own[1, layer, rows, :]
                x_hat = (x_ref[rows, :].astype(F32) - stat_ref[rows, 0:1]) * stat_ref[rows, 1:2]
                d_xhat = d_h * gain_ref[...]
                lane = lax.broadcasted_iota(jnp.int32, (SUB, 128), 1)
                pack[rows, :] = jnp.where(lane == 0, jnp.sum(d_xhat, axis=1, keepdims=True),
                                          jnp.where(lane == 1, jnp.sum(d_xhat * x_hat, axis=1, keepdims=True), 0.0))
                dg_buf[dg_row, :] = dg_buf[dg_row, :] + jnp.sum((d_h * x_hat).reshape(SUB // 8, 8, dq), axis=0)

        return 0

    lax.fori_loop(0, n_items + LAG * (NZ - 2), slot_step, 0)

    def dg_copy(r, row):
        ref = dg_buf.at[pl.ds(pl.multiple_of(row * 8, 8), 8), :]
        return remote(ref, ref, dg_s.at[r], dg_r.at[row], ((ty + r) % NTY, tx))

    def sb_copy(r, dev):
        return remote(sb_src, sb_buf.at[r], sb_s.at[r], sb_r.at[r], (ty, dev))

    sb_src[...] = pack[...].T[:8]
    for r in range(1, NTY):
        dg_copy(r, ty).start()
    for r, dev in tx_peers:
        sb_copy(r, dev).start()
    x_hat = (x_float - mean_x) * inv_std
    d_xhat = own[1, z] * gain_ref[...]
    for r, dev in tx_peers:
        sb_copy(r, dev).wait_recv()
    total = sb_src[...] + sb_buf[0] + sb_buf[1] + sb_buf[2]
    total = jnp.concatenate([total, jnp.zeros((120, tb), F32)], axis=0).T / d_model
    dx_ln = inv_std * (d_xhat - total[:, 0:1] - x_hat * total[:, 1:2])
    dx_out[...] = (dy_ref[...].astype(F32) + dx_ln).astype(BF16)
    for r in range(1, NTY):
        dg_copy(r, (ty + NTY - r) % NTY).wait_recv()
    dg_out[...] = jnp.sum(dg_buf[...], axis=0, keepdims=True)

    for r in range(1, NTY):
        dg_copy(r, ty).wait_send()
    for r, dev in tx_peers:
        sb_copy(r, dev).wait_send()

    def drain(i, _):
        y_copy(i).wait_send()
        layer = where_of(i)[1]

        @pl.when(layer > z)
        def _():
            z_copy_up(i).wait_send()

        @pl.when(layer < z)
        def _():
            z_copy_dn(i).wait_send()

        return 0

    lax.fori_loop(0, n_items, drain, 0)

    def drain_dw(c, _):
        for w in range(3):
            dw_copy(w, c).wait()
        return 0

    lax.fori_loop(0, n_chunks, drain_dw, 0)


def scatter_step(x_blk, dy_blk, gain_row, stats, act_all, d_gate_all, d_up_all, hq, dyq, w1, w3, w2):
    tb, dq = x_blk.shape
    tokens, f_loc = tb * NTY, w1.shape[1]
    dma = pltpu.SemaphoreType.DMA
    vmem = pl.BlockSpec(memory_space=pltpu.VMEM)
    hbm = pl.BlockSpec(memory_space=pl.ANY)
    items = 2 * NZ * SUBS
    return pl.pallas_call(
        scatter_kernel,
        out_shape=[
            jax.ShapeDtypeStruct((tb, dq), BF16), jax.ShapeDtypeStruct((tb, dq), BF16),
            jax.ShapeDtypeStruct((dq, f_loc), F32), jax.ShapeDtypeStruct((dq, f_loc), F32),
            jax.ShapeDtypeStruct((f_loc, dq), F32), jax.ShapeDtypeStruct((1, dq), F32)],
        in_specs=[vmem] * 4 + [hbm] * 8,
        out_specs=[vmem, vmem, hbm, hbm, hbm, vmem],
        scratch_shapes=[
            pltpu.VMEM((tokens, f_loc), BF16), pltpu.VMEM((tokens, f_loc), BF16), pltpu.VMEM((tokens, f_loc), BF16),
            pltpu.VMEM((tokens, dq), BF16), pltpu.VMEM((tokens, dq), BF16),
            pltpu.VMEM((dq, f_loc), BF16), pltpu.VMEM((dq, f_loc), BF16), pltpu.VMEM((f_loc, dq), BF16),
            pltpu.VMEM((2, NZ, tb, dq), F32), pltpu.VMEM((2, NZ, tb, dq), F32), pltpu.VMEM((2, NZ, tb, dq), F32),
            pltpu.VMEM((items, SUB, dq), F32), pltpu.VMEM((2 * SUBS, SUB, dq), F32),
            pltpu.VMEM((dq, f_loc), F32), pltpu.VMEM((dq, f_loc), F32), pltpu.VMEM((f_loc, dq), F32),
            pltpu.VMEM((tb, 128), F32), pltpu.VMEM((8, tb), F32), pltpu.VMEM((3, 8, tb), F32),
            pltpu.VMEM((8 * NTY, dq), F32),
            dma((8,)), dma((items,)), dma((items,)), dma((items,)), dma((items,)), dma((2 * SUBS,)),
            dma((3, f_loc // 256)), dma((3,)), dma((3,)), dma((NTY,)), dma((NTY,)),
        ],
        compiler_params=pltpu.CompilerParams(collective_id=1, has_side_effects=True,
                                             vmem_limit_bytes=66_500_000),
        cost_estimate=pl.CostEstimate(flops=12 * tokens * dq * f_loc, bytes_accessed=40_000_000, transcendentals=0),
    )(x_blk, dy_blk, gain_row, stats, act_all, d_gate_all, d_up_all, hq, dyq, w1, w3, w2)


def solution(mesh):
    def local_step(x_blk, dy_blk, gain_blk, w_gate_blk, w_up_blk, w_down_blk):
        gain_row = gain_blk[None, :]
        act_all, d_gate_all, d_up_all, h_all, dy_all, stats = gather_step(
            x_blk, dy_blk, gain_row, w_gate_blk, w_up_blk, w_down_blk)
        y_blk, dx_blk, dw_gate_blk, dw_up_blk, dw_down_blk, d_gain_row = scatter_step(
            x_blk, dy_blk, gain_row, stats, act_all, d_gate_all, d_up_all, h_all, dy_all,
            w_gate_blk, w_up_blk, w_down_blk)
        return (y_blk, dx_blk, dw_gate_blk, dw_up_blk, dw_down_blk, d_gain_row[0])

    return jax.shard_map(
        local_step, mesh=mesh,
        in_specs=(P("ty", "tx"), P("ty", "tx"), P("tx"), P("tx", "ty"), P("tx", "ty"), P("ty", "tx")),
        out_specs=(P("ty", "tx"), P("ty", "tx"), P("tx", "ty"), P("tx", "ty"), P("ty", "tx"), P("tx")),
        check_vma=False)
```

```python
import jax
import jax.numpy as jnp
from jax import lax
from jax.experimental import pallas as pl
from jax.experimental.pallas import tpu as pltpu
from jax.sharding import PartitionSpec as P

LN_EPS = 1e-6
MESH = pl.DeviceIdType.MESH
F32 = jnp.float32
BF16 = jnp.bfloat16
NZ = 4
NTY = 8
NTX = 4
SUB = 64
SUBS = 4
ITEMS = 2 * NZ * SUBS
LAG = 2
DW_FIRST = 8
DW_GAP = 2
DW_ROWS = 512


def contract_rows(left_op, right_op):
    return lax.dot_general(left_op, right_op, (((0,), (0,)), ((), ())), preferred_element_type=F32)


def contract_cols(left_op, right_op):
    return lax.dot_general(left_op, right_op, (((1,), (1,)), ((), ())), preferred_element_type=F32)


def matmul(left_op, right_op):
    return jnp.dot(left_op, right_op, preferred_element_type=F32)


def remote(src, dst, send_sem, recv_sem, device):
    return pltpu.make_async_remote_copy(src_ref=src, dst_ref=dst, send_sem=send_sem, recv_sem=recv_sem,
                                        device_id=device, device_id_type=MESH)


def span(index, size):
    return pl.ds(pl.multiple_of(index * size, size), size)


def item_of(i):
    return i // (NZ * SUBS), 3 * (i % (NZ * SUBS) // SUBS) % NZ, i % SUBS


def step_kernel(x_ref, dy_ref, gain_ref, w1_ref, w3_ref, w2_ref,
                y_out, dx_out, dw1_out, dw3_out, dw2_out, dg_out, hg, dyg,
                h_blk, tiles, w1f, w3f, w2f, w2_own, part, v_buf, act, gate_g, up_g, y_recv, z_buf, z_fin, stage,
                st_src, st_buf, pack, sb_src, sb_buf, dg_buf, norm,
                st_s, st_r, x_s, x_r, up_s, dn_s, z_r, y_s, y_r, d_s, d_r, w_s, w_r, w_l, e_s, e_r, t_l, o_l, l_l,
                q_s, q_r, c_s, c_r, f_r, dw_l, sb_s, sb_r, dg_s, dg_r):
    ty, tx = lax.axis_index("ty"), lax.axis_index("tx")
    z, y, core = ty // 2, ty % 2, tx % 2
    yp, up, dn = ty + 1 - 2 * y, ty + 2, ty - 2
    cp, xp, dp = tx + 1 - 2 * core, (tx + 2) % NTX, NTX - 1 - tx
    tx_peers = ((0, cp), (1, xp), (2, dp))
    tb, dq = x_ref.shape
    d_model = dq * NTX
    tokens = tb * NTY
    f_loc = w1_ref.shape[1]
    fh = f_loc // 2
    hi = z // 2
    near = z * (1 - hi) + (NZ - 1 - z) * hi
    far = NZ - 1 - near

    barrier = pltpu.get_barrier_semaphore()
    for _, dev in tx_peers:
        pl.semaphore_signal(barrier, inc=1, device_id=(ty, dev), device_id_type=MESH)
    for r in range(1, NTY):
        pl.semaphore_signal(barrier, inc=1, device_id=((ty + r) % NTY, tx), device_id_type=MESH)

    w_shards = (w1_ref, w3_ref, w2_ref)
    w_full = (w1f, w3f, w2f)

    def w_refs(w, c):
        mine = span(tx, dq)
        if w == 2:
            return w_shards[w].at[span(c, fh), :], w_full[w].at[:, mine]
        return w_shards[w].at[:, span(c, fh)], w_full[w].at[mine, :]

    def w_local(w):
        src, dst = w_refs(w, core)
        return pltpu.make_async_copy(src, dst, w_l.at[w])

    def w_copy(w, r, dev):
        src, dst = w_refs(w, dev % 2)
        return remote(src, dst, w_s.at[w, r], w_r.at[w, r], (ty, dev))

    def w_arrive(w, r, dev):
        theirs = span(dev, dq)
        dst = w_full[w].at[:, theirs] if w == 2 else w_full[w].at[theirs, :]
        return remote(dst, dst, w_s.at[w, r], w_r.at[w, r], (ty, dev))

    def wait_w(w):
        w_local(w).wait()
        for r, dev in tx_peers:
            w_arrive(w, r, dev).wait_recv()

    for w in range(3):
        w_local(w).start()
    w2_own_copy = pltpu.make_async_copy(w2_ref, w2_own, l_l.at[0])
    w2_own_copy.start()
    gathered = (hg, dyg)
    own_blk = (h_blk, dy_ref)

    def block(t, q, row_ty):
        return gathered[t].at[span(row_ty, tb), span(q, dq)]

    def own_local(t):
        return pltpu.make_async_copy(own_blk[t], block(t, tx, ty), o_l.at[t])

    own_local(1).start()

    x_float = x_ref[...].astype(F32)
    lane = lax.broadcasted_iota(jnp.int32, (tb, 128), 1)
    sum_1 = jnp.sum(x_float, axis=1, keepdims=True)
    sum_2 = jnp.sum(x_float * x_float, axis=1, keepdims=True)
    st_src[...] = jnp.where(lane == 0, sum_1, jnp.where(lane == 1, sum_2, 0.0)).T[:8]
    dg_row = span(ty, 8)
    dg_buf[dg_row, :] = jnp.zeros((8, dq), F32)

    pl.semaphore_wait(barrier, NTY + NTX - 2)

    def quarter(s, q):
        return q if s == 0 else (q + 2) % NTX

    def stat_copy(r, dev):
        return remote(st_src, st_buf.at[r], st_s.at[r], st_r.at[r], (ty, dev))

    def x_copy(t):
        return remote(own_blk[t], block(t, tx, ty), x_s.at[t], x_r.at[t], (ty, xp))

    def x_arrive(t):
        ref = block(t, xp, ty)
        return remote(ref, ref, x_s.at[t], x_r.at[t], (ty, xp))

    def z_copy(t, s, layer, sem, dev, own=False):
        ref = block(t, quarter(s, tx), layer * 2 + y)
        return remote(own_blk[t] if own else ref, ref, sem.at[t, s, layer], z_r.at[t, s, layer], (dev, tx))

    def y_copy(t, s, layer, row_ty, own=False):
        ref = block(t, quarter(s, tx), row_ty)
        return remote(own_blk[t] if own else ref, ref, y_s.at[t, s, layer], y_r.at[t, s, layer], (yp, tx))

    def d_copy(t, s, row_ty, q, own=False):
        ref = block(t, quarter(s, q), row_ty)
        return remote(own_blk[t] if own else ref, ref, d_s.at[t, s, row_ty], d_r.at[t, s, row_ty], (ty, cp))

    def spread(t, s, layer, own=False):
        y_copy(t, s, layer, layer * 2 + y, own).start()
        d_copy(t, s, layer * 2 + y, tx, own).start()

    def send_own(t, s):
        @pl.when(z < NZ - 1)
        def _():
            z_copy(t, s, z, up_s, up, s == 0).start()

        @pl.when(z > 0)
        def _():
            z_copy(t, s, z, dn_s, dn, s == 0).start()

        spread(t, s, z, s == 0)

    for r, dev in tx_peers:
        stat_copy(r, dev).start()
    for w in range(3):
        w_copy(w, 0, cp).start()
    x_copy(1).start()
    send_own(1, 0)
    for r, dev in tx_peers:
        stat_copy(r, dev).wait_recv()
    total = st_src[...] + st_buf[0] + st_buf[1] + st_buf[2]
    total = jnp.concatenate([total, jnp.zeros((120, tb), F32)], axis=0).T
    mean_x = total[:, 0:1] / d_model
    inv_std = lax.rsqrt(total[:, 1:2] / d_model - mean_x * mean_x + LN_EPS)
    gain_row = gain_ref[...].reshape(1, dq)
    h_blk[...] = (gain_row * ((x_float - mean_x) * inv_std)).astype(BF16)
    norm[...] = jnp.where(lane == 0, mean_x, jnp.where(lane == 1, inv_std, 0.0))
    own_local(0).start()
    x_copy(0).start()
    send_own(0, 0)
    for w in range(3):
        w_copy(w, 1, xp).start()
        w_copy(w, 2, dp).start()

    for t in (1, 0):
        x_arrive(t).wait_recv()
        send_own(t, 1)
    order = ((1, 0), (0, 0), (1, 1), (0, 1))
    for k in range(1, NZ):
        for t, s in order:
            @pl.when(z >= k)
            def _():
                layer = z - k
                z_copy(t, s, layer, up_s, dn).wait_recv()

                @pl.when(z < NZ - 1)
                def _():
                    z_copy(t, s, layer, up_s, up).start()

                spread(t, s, layer)

            @pl.when(z + k < NZ)
            def _():
                layer = z + k
                z_copy(t, s, layer, dn_s, up).wait_recv()

                @pl.when(z > 0)
                def _():
                    z_copy(t, s, layer, dn_s, dn).start()

                spread(t, s, layer)

    own_local(0).wait()
    own_local(1).wait()

    def layer_of(n):
        m = n % NZ
        base = m + near * (1 - 2 * m) * (1 - m // 2)
        return base + hi * (NZ - 1 - 2 * base)

    def tile_row(n):
        return layer_of(n) * 2 + y + (n // NZ) * (1 - 2 * y)

    def tile_copy(t, n):
        return pltpu.make_async_copy(gathered[t].at[span(tile_row(n), tb), :], tiles.at[n % 2], t_l.at[n % 2])

    def fetch(t, n):
        row_ty = tile_row(n)
        for s in (0, 1):
            d_copy(t, s, row_ty, cp).wait_recv()
        tile_copy(t, n).start()

    def arrive(n):
        @pl.when(n >= NZ)
        def _():
            row_ty, layer = tile_row(n), layer_of(n)
            for t, s in order:
                y_copy(t, s, layer, row_ty).wait_recv()
                d_copy(t, s, row_ty, tx).start()

    swaps = (act, gate_g, up_g)

    def e_copy(i, row_ty):
        rows = span(row_ty, tb)
        return remote(swaps[i].at[0, rows, :], swaps[i].at[1, rows, :], e_s.at[i, row_ty], e_r.at[i, row_ty],
                      (ty, cp))

    wait_w(0)
    wait_w(1)
    fetch(0, 0)

    def up_step(n, _):
        @pl.when(n > 0)
        def _():
            e_copy(0, tile_row(n - 1)).start()

        @pl.when(n < NTY - 1)
        def _():
            arrive(n + 1)
            fetch(0, n + 1)

        row_ty = tile_row(n)
        tile_copy(0, n).wait()
        h_rows = tiles[n % 2]
        gate = matmul(h_rows, w1f[...])
        up_v = matmul(h_rows, w3f[...])
        part[1, row_ty] = gate
        v_buf[row_ty] = up_v
        act[0, span(row_ty, tb), :] = (gate * jax.nn.sigmoid(gate) * up_v).astype(BF16)
        return 0

    lax.fori_loop(0, NTY, up_step, 0)
    e_copy(0, tile_row(NTY - 1)).start()
    hq, dyq = w1f.at[pl.ds(0, tokens), :], w3f.at[pl.ds(0, tokens), :]
    hq_copy = pltpu.make_async_copy(hg.at[:, span(tx, dq)], hq, l_l.at[1])
    dyq_copy = pltpu.make_async_copy(dyg.at[:, span(tx, dq)], dyq, l_l.at[2])
    hq_copy.start()
    dyq_copy.start()
    w2_own_copy.wait()

    def sub_rows(sub):
        return span(sub, SUB)

    def q_copy(i):
        mat, layer, sub = item_of(i)
        return remote(part.at[mat, layer * 2 + 1 - y, sub_rows(sub), :], y_recv.at[mat, layer, sub_rows(sub), :],
                      q_s.at[i], q_r.at[i], (yp, tx))

    def send_block(mat, j):
        for sub in range(SUBS):
            q_copy((mat * NZ + j) * SUBS + sub).start()

    def part_row(jj):
        return (3 * (jj % NZ) % NZ) * 2 + 1 - y + (jj // NZ) * (2 * y - 1)

    def m_step(jj, _):
        row_ty = part_row(jj)
        rows = span(row_ty, tb)
        e_copy(0, row_ty).wait_recv()
        part[0, row_ty] = (matmul(act[0, rows, :], w2_own[span(core, fh), :])
                           + matmul(act[1, rows, :], w2_own[span(1 - core, fh), :]))

        @pl.when(jnp.logical_and(jj > 0, jj <= NZ))
        def _():
            send_block(0, jj - 1)

        return 0

    lax.fori_loop(0, NTY, m_step, 0)

    def c_refs(i):
        mat, layer, sub = item_of(i)
        return part.at[mat, layer * 2 + y, sub_rows(sub), :]

    def c_up(i):
        return remote(c_refs(i), z_buf.at[i], c_s.at[i], c_r.at[i], (up, tx))

    def c_dn(i):
        return remote(c_refs(i), z_buf.at[i], c_s.at[i], c_r.at[i], (dn, tx))

    def c_fin(i):
        mat, _, sub = item_of(i)
        k = mat * SUBS + sub
        return remote(c_refs(i), z_fin.at[k], c_s.at[i], f_r.at[k], (dn, tx))

    def add_to(i, value):
        mat, layer, sub = item_of(i)
        part[mat, layer * 2 + y, sub_rows(sub), :] = part[mat, layer * 2 + y, sub_rows(sub), :] + value

    def add_run(i):
        c_up(i).wait_recv()
        add_to(i, z_buf[i])

    def slot_step(slot):
        @pl.when(slot < ITEMS)
        def _():
            mat, layer, sub = item_of(slot)
            q_copy(slot).wait_recv()
            add_to(slot, y_recv[mat, layer, sub_rows(sub), :])

        i_up = slot - LAG * z
        l_up = item_of(jnp.maximum(i_up, 0))[1]

        @pl.when(jnp.logical_and(jnp.logical_and(i_up >= 0, i_up < ITEMS), l_up > z))
        def _():
            @pl.when(z > 0)
            def _():
                add_run(i_up)

            c_up(i_up).start()

        i_dn = slot - LAG * (NZ - 1 - z)
        l_dn = item_of(jnp.maximum(i_dn, 0))[1]

        @pl.when(jnp.logical_and(jnp.logical_and(i_dn >= 0, i_dn < ITEMS), l_dn < z))
        def _():
            @pl.when(z < NZ - 1)
            def _():
                add_run(i_dn)

            @pl.when(l_dn < z - 1)
            def _():
                c_dn(i_dn).start()

            @pl.when(l_dn == z - 1)
            def _():
                c_fin(i_dn).start()

        i_fin = slot - LAG * far
        l_fin = item_of(jnp.maximum(i_fin, 0))[1]

        @pl.when(jnp.logical_and(jnp.logical_and(i_fin >= 0, i_fin < ITEMS), l_fin == z))
        def _():
            mat, layer, sub = item_of(i_fin)

            @pl.when(z > 0)
            def _():
                add_run(i_fin)

            @pl.when(z < NZ - 1)
            def _():
                c_fin(i_fin).wait_recv()
                add_to(i_fin, z_fin[mat * SUBS + sub])

            rows = sub_rows(sub)

            @pl.when(mat == 0)
            def _():
                y_out[rows, :] = (x_ref[rows, :].astype(F32) + part[0, layer * 2 + y, rows, :]).astype(BF16)

            @pl.when(mat == 1)
            def _():
                d_h = part[1, layer * 2 + y, rows, :]
                x_hat = (x_ref[rows, :].astype(F32) - norm[rows, 0:1]) * norm[rows, 1:2]
                d_xhat = d_h * gain_ref[...].reshape(1, dq)
                sub_lane = lax.broadcasted_iota(jnp.int32, (SUB, 128), 1)
                pack[rows, :] = jnp.where(sub_lane == 0, jnp.sum(d_xhat, axis=1, keepdims=True),
                                          jnp.where(sub_lane == 1, jnp.sum(d_xhat * x_hat, axis=1, keepdims=True), 0.0))
                dg_buf[dg_row, :] = dg_buf[dg_row, :] + jnp.sum((d_h * x_hat).reshape(SUB // 8, 8, dq), axis=0)

    wait_w(2)
    fetch(1, 0)

    def down_step(n, _):
        @pl.when(n > 0)
        def _():
            e_copy(1, tile_row(n - 1)).start()
            e_copy(2, tile_row(n - 1)).start()

        @pl.when(n < NTY - 1)
        def _():
            fetch(1, n + 1)

        row_ty = tile_row(n)
        rows = span(row_ty, tb)
        tile_copy(1, n).wait()
        d_act = contract_cols(tiles[n % 2], w2f[...])
        gate, up_v = part[1, row_ty], v_buf[row_ty]
        sig = jax.nn.sigmoid(gate)
        gate_g[0, rows, :] = (d_act * up_v * sig * (1.0 + gate * (1.0 - sig))).astype(BF16)
        up_g[0, rows, :] = (d_act * (gate * sig)).astype(BF16)

        @pl.when(n % 2 == 1)
        def _():
            slot_step(n // 2)

        return 0

    lax.fori_loop(0, NTY, down_step, 0)
    e_copy(1, tile_row(NTY - 1)).start()
    e_copy(2, tile_row(NTY - 1)).start()
    w1_own, w3_own = w2f.at[:, pl.ds(0, f_loc)], w2f.at[:, pl.ds(f_loc, f_loc)]
    w1_own_copy = pltpu.make_async_copy(w1_ref, w1_own, l_l.at[3])
    w3_own_copy = pltpu.make_async_copy(w3_ref, w3_own, l_l.at[4])
    w1_own_copy.start()
    w3_own_copy.start()
    w1_own_copy.wait()
    w3_own_copy.wait()

    def dh_step(jj, _):
        row_ty = part_row(jj)
        rows = span(row_ty, tb)
        e_copy(1, row_ty).wait_recv()
        e_copy(2, row_ty).wait_recv()
        acc = contract_cols(gate_g[0, rows, :], w1_own[:, span(core, fh)])
        acc += contract_cols(gate_g[1, rows, :], w1_own[:, span(1 - core, fh)])
        acc += contract_cols(up_g[0, rows, :], w3_own[:, span(core, fh)])
        acc += contract_cols(up_g[1, rows, :], w3_own[:, span(1 - core, fh)])
        part[1, row_ty] = acc

        @pl.when(jnp.logical_and(jj > 0, jj <= NZ))
        def _():
            send_block(1, jj - 1)

        @pl.when(jj % 2 == 1)
        def _():
            slot_step(NTY // 2 + jj // 2)

        return 0

    lax.fori_loop(0, NTY, dh_step, 0)
    hq_copy.wait()
    dyq_copy.wait()

    def dw_copy(c, w):
        half = c % 2
        cols = span(core + half * (1 - 2 * core), fh)
        dst = (dw2_out.at[cols, :], dw1_out.at[:, cols], dw3_out.at[:, cols])[w]
        return pltpu.make_async_copy(stage, dst, dw_l.at[0])

    def weight_grads(slot):
        c = (slot - DW_FIRST) // DW_GAP
        half = c % 2

        def over_tokens(left, right):
            def piece(k, _):
                rows = span(k, DW_ROWS)
                stage[...] = stage[...] + contract_rows(left[rows, :], right[rows, :])
                return 0

            stage[...] = jnp.zeros(stage.shape, F32)
            lax.fori_loop(0, tokens // DW_ROWS, piece, 0)

        @pl.when(jnp.logical_and((slot - DW_FIRST) % DW_GAP == 0, slot < DW_FIRST + 6 * DW_GAP))
        def _():
            @pl.when(c >= 1)
            def _():
                dw_copy(c, 0).wait()

            for w in range(3):
                @pl.when(c // 2 == w)
                def _():
                    over_tokens(act.at[half] if w == 0 else hq, (dyq, gate_g.at[half], up_g.at[half])[w])
                    dw_copy(c, w).start()

    def last_slots(slot, _):
        weight_grads(slot)
        slot_step(slot)
        return 0

    lax.fori_loop(NTY, ITEMS + LAG * (NZ - 2), last_slots, 0)

    def dg_copy(r, row):
        ref = dg_buf.at[span(row, 8), :]
        return remote(ref, ref, dg_s.at[r], dg_r.at[row], ((ty + r) % NTY, tx))

    def sb_copy(r, dev):
        return remote(sb_src, sb_buf.at[r], sb_s.at[r], sb_r.at[r], (ty, dev))

    sb_src[...] = pack[...].T[:8]
    for r in range(1, NTY):
        dg_copy(r, ty).start()
    for r, dev in tx_peers:
        sb_copy(r, dev).start()
    inv_std = norm[:, 1:2]
    x_hat = (x_ref[...].astype(F32) - norm[:, 0:1]) * inv_std
    d_xhat = part[1, ty] * gain_ref[...].reshape(1, dq)
    for r, dev in tx_peers:
        sb_copy(r, dev).wait_recv()
    total = sb_src[...] + sb_buf[0] + sb_buf[1] + sb_buf[2]
    total = jnp.concatenate([total, jnp.zeros((120, tb), F32)], axis=0).T / d_model
    dx_ln = inv_std * (d_xhat - total[:, 0:1] - x_hat * total[:, 1:2])
    dx_out[...] = (dy_ref[...].astype(F32) + dx_ln).astype(BF16)
    for r in range(1, NTY):
        dg_copy(r, (ty + NTY - r) % NTY).wait_recv()
    dg_out[...] = jnp.sum(dg_buf[...], axis=0)

    dw_copy(0, 0).wait()
    for r in range(1, NTY):
        dg_copy(r, ty).wait_send()
    for r, dev in tx_peers:
        sb_copy(r, dev).wait_send()
        stat_copy(r, dev).wait_send()
        for w in range(3):
            w_copy(w, r, dev).wait_send()
    for t in (0, 1):
        x_copy(t).wait_send()

    def drain(layer, _):
        for t, s in order:
            @pl.when(jnp.logical_and(z < NZ - 1, layer <= z))
            def _():
                z_copy(t, s, layer, up_s, up).wait_send()

            @pl.when(jnp.logical_and(z > 0, layer >= z))
            def _():
                z_copy(t, s, layer, dn_s, dn).wait_send()

            y_copy(t, s, layer, layer * 2 + y).wait_send()
            d_copy(t, s, layer * 2, tx).wait_send()
            d_copy(t, s, layer * 2 + 1, tx).wait_send()
        return 0

    lax.fori_loop(0, NZ, drain, 0)

    def drain_swap(row_ty, _):
        for i in range(3):
            e_copy(i, row_ty).wait_send()
        return 0

    lax.fori_loop(0, NTY, drain_swap, 0)

    def drain_items(i, _):
        q_copy(i).wait_send()
        layer = item_of(i)[1]

        @pl.when(layer > z)
        def _():
            c_up(i).wait_send()

        @pl.when(layer < z)
        def _():
            c_dn(i).wait_send()

        return 0

    lax.fori_loop(0, ITEMS, drain_items, 0)


def solution(mesh):
    def local_step(x_blk, dy_blk, gain_blk, w1, w3, w2):
        tb, dq = x_blk.shape
        tokens, d_model, f_loc = tb * NTY, dq * NTX, w1.shape[1]
        fh = f_loc // 2
        dma = pltpu.SemaphoreType.DMA
        vmem = pl.BlockSpec(memory_space=pltpu.VMEM)
        hbm = pl.BlockSpec(memory_space=pl.ANY)
        outs = pl.pallas_call(
            step_kernel,
            out_shape=[
                jax.ShapeDtypeStruct((tb, dq), BF16), jax.ShapeDtypeStruct((tb, dq), BF16),
                jax.ShapeDtypeStruct((dq, f_loc), F32), jax.ShapeDtypeStruct((dq, f_loc), F32),
                jax.ShapeDtypeStruct((f_loc, dq), F32), jax.ShapeDtypeStruct((dq,), F32),
                jax.ShapeDtypeStruct((tokens, d_model), BF16), jax.ShapeDtypeStruct((tokens, d_model), BF16)],
            in_specs=[vmem, vmem, vmem, hbm, hbm, hbm],
            out_specs=[vmem, vmem, hbm, hbm, hbm, vmem, hbm, hbm],
            scratch_shapes=[
                pltpu.VMEM((tb, dq), BF16), pltpu.VMEM((2, tb, d_model), BF16),
                pltpu.VMEM((d_model, fh), BF16), pltpu.VMEM((d_model, fh), BF16), pltpu.VMEM((fh, d_model), BF16),
                pltpu.VMEM((f_loc, dq), BF16),
                pltpu.VMEM((2, NTY, tb, dq), F32), pltpu.VMEM((NTY, tb, fh), F32),
                pltpu.VMEM((2, tokens, fh), BF16), pltpu.VMEM((2, tokens, fh), BF16), pltpu.VMEM((2, tokens, fh), BF16),
                pltpu.VMEM((2, NZ, tb, dq), F32), pltpu.VMEM((ITEMS, SUB, dq), F32), pltpu.VMEM((2 * SUBS, SUB, dq), F32),
                pltpu.VMEM((fh, dq), F32),
                pltpu.VMEM((8, tb), F32), pltpu.VMEM((3, 8, tb), F32),
                pltpu.VMEM((tb, 128), F32), pltpu.VMEM((8, tb), F32), pltpu.VMEM((3, 8, tb), F32),
                pltpu.VMEM((8 * NTY, dq), F32), pltpu.VMEM((tb, 128), F32),
                dma((3,)), dma((3,)), dma((2,)), dma((2,)),
                dma((2, 2, NZ)), dma((2, 2, NZ)), dma((2, 2, NZ)), dma((2, 2, NZ)), dma((2, 2, NZ)),
                dma((2, 2, NTY)), dma((2, 2, NTY)),
                dma((3, 3)), dma((3, 3)), dma((3,)),
                dma((3, NTY)), dma((3, NTY)), dma((2,)), dma((2,)), dma((5,)),
                dma((ITEMS,)), dma((ITEMS,)), dma((ITEMS,)), dma((ITEMS,)), dma((2 * SUBS,)),
                dma((1,)), dma((3,)), dma((3,)), dma((NTY,)), dma((NTY,)),
            ],
            compiler_params=pltpu.CompilerParams(collective_id=0, has_side_effects=True,
                                                 vmem_limit_bytes=67_000_000),
            cost_estimate=pl.CostEstimate(flops=24 * tokens * d_model * fh, bytes_accessed=80_000_000,
                                          transcendentals=2 * tokens * fh),
        )(x_blk, dy_blk, gain_blk, w1, w3, w2)
        return tuple(outs[:6])

    return jax.shard_map(
        local_step, mesh=mesh,
        in_specs=(P("ty", "tx"), P("ty", "tx"), P("tx"), P("tx", "ty"), P("tx", "ty"), P("ty", "tx")),
        out_specs=(P("ty", "tx"), P("ty", "tx"), P("tx", "ty"), P("tx", "ty"), P("ty", "tx"), P("tx")),
        check_vma=False)
```

```python
import jax
import jax.numpy as jnp
from jax import lax
from jax.experimental import pallas as pl
from jax.experimental.pallas import tpu as pltpu
from jax.sharding import PartitionSpec as P

LN_EPS = 1e-6
MESH = pl.DeviceIdType.MESH
F32 = jnp.float32
BF16 = jnp.bfloat16
NZ = 4
NTY = 8
NTX = 4
SUB = 32
SUBS = 8
ITEMS = 2 * NZ * SUBS
LAG = 2
DW_FIRST = 16
DW_GAP = 4
DW_ROWS = 512


def contract_rows(left_op, right_op):
    return lax.dot_general(left_op, right_op, (((0,), (0,)), ((), ())), preferred_element_type=F32)


def contract_cols(left_op, right_op):
    return lax.dot_general(left_op, right_op, (((1,), (1,)), ((), ())), preferred_element_type=F32)


def matmul(left_op, right_op):
    return jnp.dot(left_op, right_op, preferred_element_type=F32)


def remote(src, dst, send_sem, recv_sem, device):
    return pltpu.make_async_remote_copy(src_ref=src, dst_ref=dst, send_sem=send_sem, recv_sem=recv_sem,
                                        device_id=device, device_id_type=MESH)


def span(index, size):
    return pl.ds(pl.multiple_of(index * size, size), size)


def item_of(i):
    return i // (NZ * SUBS), 3 * (i % (NZ * SUBS) // SUBS) % NZ, i % SUBS


def step_kernel(x_ref, dy_ref, gain_ref, w1_ref, w3_ref, w2_ref,
                y_out, dx_out, dw1_out, dw3_out, dw2_out, dg_out, hg, dyg,
                h_blk, tiles, w1f, w3f, w2f, w2_own, part, v_buf, act, gate_g, up_g, y_recv, z_buf, z_fin, stage,
                st_src, st_buf, pack, sb_src, sb_buf, dg_buf, norm,
                st_s, st_r, x_s, x_r, up_s, dn_s, z_r, uo_s, do_s, zo_r, y_s, y_r, d_s, d_r, w_s, w_r, w_l, e_s, e_r, t_l, o_l, l_l,
                q_s, q_r, c_s, c_r, f_r, dw_l, sb_s, sb_r, dg_s, dg_r):
    ty, tx = lax.axis_index("ty"), lax.axis_index("tx")
    z, y, core = ty // 2, ty % 2, tx % 2
    yp, up, dn = ty + 1 - 2 * y, ty + 2, ty - 2
    cp, xp, dp = tx + 1 - 2 * core, (tx + 2) % NTX, NTX - 1 - tx
    tx_peers = ((0, cp), (1, xp), (2, dp))
    tb, dq = x_ref.shape
    d_model = dq * NTX
    tokens = tb * NTY
    f_loc = w1_ref.shape[1]
    fh = f_loc // 2
    hi = z // 2
    near = z * (1 - hi) + (NZ - 1 - z) * hi
    far = NZ - 1 - near

    barrier = pltpu.get_barrier_semaphore()
    for _, dev in tx_peers:
        pl.semaphore_signal(barrier, inc=1, device_id=(ty, dev), device_id_type=MESH)
    for r in range(1, NTY):
        pl.semaphore_signal(barrier, inc=1, device_id=((ty + r) % NTY, tx), device_id_type=MESH)

    w_shards = (w1_ref, w3_ref, w2_ref)
    w_full = (w1f, w3f, w2f)

    def w_refs(w, c):
        mine = span(tx, dq)
        if w == 2:
            return w_shards[w].at[span(c, fh), :], w_full[w].at[:, mine]
        return w_shards[w].at[:, span(c, fh)], w_full[w].at[mine, :]

    def w_local(w):
        src, dst = w_refs(w, core)
        return pltpu.make_async_copy(src, dst, w_l.at[w])

    def w_copy(w, r, dev):
        src, dst = w_refs(w, dev % 2)
        return remote(src, dst, w_s.at[w, r], w_r.at[w, r], (ty, dev))

    def w_arrive(w, r, dev):
        theirs = span(dev, dq)
        dst = w_full[w].at[:, theirs] if w == 2 else w_full[w].at[theirs, :]
        return remote(dst, dst, w_s.at[w, r], w_r.at[w, r], (ty, dev))

    def wait_w(w):
        w_local(w).wait()
        for r, dev in tx_peers:
            w_arrive(w, r, dev).wait_recv()

    for w in range(3):
        w_local(w).start()
    w2_own_copy = pltpu.make_async_copy(w2_ref, w2_own, l_l.at[0])
    w2_own_copy.start()
    gathered = (hg, dyg)
    own_blk = (h_blk, dy_ref)

    def block(t, q, row_ty):
        return gathered[t].at[span(row_ty, tb), span(q, dq)]

    def own_local(t):
        return pltpu.make_async_copy(own_blk[t], block(t, tx, ty), o_l.at[t])

    own_local(1).start()

    x_float = x_ref[...].astype(F32)
    lane = lax.broadcasted_iota(jnp.int32, (tb, 128), 1)
    sum_1 = jnp.sum(x_float, axis=1, keepdims=True)
    sum_2 = jnp.sum(x_float * x_float, axis=1, keepdims=True)
    st_src[...] = jnp.where(lane == 0, sum_1, jnp.where(lane == 1, sum_2, 0.0)).T[:8]
    dg_row = span(ty, 8)
    dg_buf[dg_row, :] = jnp.zeros((8, dq), F32)

    pl.semaphore_wait(barrier, NTY + NTX - 2)

    def quarter(s, q):
        return q if s == 0 else (q + 2) % NTX

    def stat_copy(r, dev):
        return remote(st_src, st_buf.at[r], st_s.at[r], st_r.at[r], (ty, dev))

    def x_copy(t):
        return remote(own_blk[t], block(t, tx, ty), x_s.at[t], x_r.at[t], (ty, xp))

    def x_arrive(t):
        ref = block(t, xp, ty)
        return remote(ref, ref, x_s.at[t], x_r.at[t], (ty, xp))

    def z_copy(t, s, layer, sem, dev, own=False):
        ref = block(t, quarter(s, tx), layer * 2 + y)
        return remote(own_blk[t] if own else ref, ref, sem.at[t, s, layer], z_r.at[t, s, layer], (dev, tx))

    def y_copy(t, s, layer, row_ty, own=False):
        ref = block(t, quarter(s, tx), row_ty)
        return remote(own_blk[t] if own else ref, ref, y_s.at[t, s, layer], y_r.at[t, s, layer], (yp, tx))

    def d_copy(t, s, row_ty, q, own=False):
        ref = block(t, quarter(s, q), row_ty)
        return remote(own_blk[t] if own else ref, ref, d_s.at[t, s, row_ty], d_r.at[t, s, row_ty], (ty, cp))

    def spread(t, s, layer, own=False):
        y_copy(t, s, layer, layer * 2 + y, own).start()
        d_copy(t, s, layer * 2 + y, tx, own).start()

    def send_own(t, s):
        @pl.when(z < NZ - 1)
        def _():
            z_copy(t, s, z, up_s, up, s == 0).start()

        @pl.when(z > 0)
        def _():
            z_copy(t, s, z, dn_s, dn, s == 0).start()

        spread(t, s, z, s == 0)

    for r, dev in tx_peers:
        stat_copy(r, dev).start()
    for w in range(3):
        w_copy(w, 0, cp).start()
    x_copy(1).start()
    send_own(1, 0)
    for r, dev in tx_peers:
        stat_copy(r, dev).wait_recv()
    total = st_src[...] + st_buf[0] + st_buf[1] + st_buf[2]
    total = jnp.concatenate([total, jnp.zeros((120, tb), F32)], axis=0).T
    mean_x = total[:, 0:1] / d_model
    inv_std = lax.rsqrt(total[:, 1:2] / d_model - mean_x * mean_x + LN_EPS)
    gain_row = gain_ref[...].reshape(1, dq)
    h_blk[...] = (gain_row * ((x_float - mean_x) * inv_std)).astype(BF16)
    norm[...] = jnp.where(lane == 0, mean_x, jnp.where(lane == 1, inv_std, 0.0))
    own_local(0).start()
    x_copy(0).start()
    send_own(0, 0)
    for w in range(3):
        w_copy(w, 1, xp).start()
        w_copy(w, 2, dp).start()

    def zo_copy(layer, sem, dev):
        ref = block(1, quarter(1, tx), layer * 2 + 1 - y)
        return remote(ref, ref, sem.at[layer], zo_r.at[layer], (dev, tx))

    order = ((0, 0), (0, 1), (1, 0), (1, 1))

    def pass_up(layer, copy, sem, after):
        copy(layer, sem, dn).wait_recv()

        @pl.when(z < NZ - 1)
        def _():
            copy(layer, sem, up).start()

        after(layer)

    def pass_down(layer, copy, sem, after):
        copy(layer, sem, up).wait_recv()

        @pl.when(z > 0)
        def _():
            copy(layer, sem, dn).start()

        after(layer)

    def relay(k, t, s):
        def copy(layer, sem, dev):
            return z_copy(t, s, layer, sem, dev)

        def after(layer):
            if (t, s) != (1, 1):
                y_copy(t, s, layer, layer * 2 + y).start()
            d_copy(t, s, layer * 2 + y, tx).start()

        def after_other(layer):
            d_copy(1, 1, layer * 2 + 1 - y, tx).start()

        @pl.when(z >= k)
        def _():
            pass_up(z - k, copy, up_s, after)
            if (t, s) == (1, 1):
                pass_up(z - k, zo_copy, uo_s, after_other)

        @pl.when(z + k < NZ)
        def _():
            pass_down(z + k, copy, dn_s, after)
            if (t, s) == (1, 1):
                pass_down(z + k, zo_copy, do_s, after_other)

    for t in (1, 0):
        x_arrive(t).wait_recv()
        send_own(t, 1)
    for s in (0, 1):
        relay(1, 0, s)
    y_copy(1, 1, z, ty + 1 - 2 * y).wait_recv()

    @pl.when(z < NZ - 1)
    def _():
        zo_copy(z, uo_s, up).start()

    @pl.when(z > 0)
    def _():
        zo_copy(z, do_s, dn).start()

    d_copy(1, 1, yp, tx).start()
    for s in (0, 1):
        relay(2, 0, s)
    for s in (0, 1):
        relay(1, 1, s)
    for s in (0, 1):
        relay(3, 0, s)
    own_local(0).wait()
    own_local(1).wait()

    def layer_of(n):
        m = n % NZ
        base = m + near * (1 - 2 * m) * (1 - m // 2)
        return base + hi * (NZ - 1 - 2 * base)

    def tile_row(n):
        return layer_of(n) * 2 + y + (n // NZ) * (1 - 2 * y)

    chip = tx // 2

    def tile_copy(t, n, half=None):
        rows = span(tile_row(n), tb)
        if half is None:
            return pltpu.make_async_copy(gathered[t].at[rows, :], tiles.at[n % 2], t_l.at[n % 2])
        return pltpu.make_async_copy(gathered[t].at[rows, span(half, 2 * dq)], tiles.at[n % 2, :, pl.ds(0, 2 * dq)],
                                     t_l.at[n % 2])

    swaps = (act, gate_g, up_g)

    def e_copy(i, row_ty):
        rows = span(row_ty, tb)
        return remote(swaps[i].at[0, rows, :], swaps[i].at[1, rows, :], e_s.at[i, row_ty], e_r.at[i, row_ty],
                      (ty, cp))

    def fetch_near(n):
        row_ty = tile_row(n)

        @pl.when(n >= NZ)
        def _():
            for s in (0, 1):
                y_copy(0, s, layer_of(n), row_ty).wait_recv()
                d_copy(0, s, row_ty, tx).start()

        d_copy(0, 0, row_ty, cp).wait_recv()
        tile_copy(0, n, chip).start()

    def fetch_far(n):
        d_copy(0, 1, tile_row(n), cp).wait_recv()
        tile_copy(0, n, 1 - chip).start()

    def near_step(n, _):
        @pl.when(n < NTY - 1)
        def _():
            fetch_near(n + 1)

        row_ty = tile_row(n)
        tile_copy(0, n, chip).wait()
        h_rows = tiles[n % 2, :, pl.ds(0, 2 * dq)]
        part[1, row_ty] = matmul(h_rows, w1f[span(chip, 2 * dq), :])
        v_buf[row_ty] = matmul(h_rows, w3f[span(chip, 2 * dq), :])
        return 0

    for w in (0, 1):
        w_local(w).wait()
        w_arrive(w, 0, cp).wait_recv()
    fetch_near(0)
    lax.fori_loop(0, NTY, near_step, 0)
    for s in (0, 1):
        relay(2, 1, s)
    for w in (0, 1):
        w_arrive(w, 1, xp).wait_recv()
        w_arrive(w, 2, dp).wait_recv()
    fetch_far(0)

    def far_step(n, _):
        @pl.when(n > 0)
        def _():
            e_copy(0, tile_row(n - 1)).start()

        @pl.when(n < NTY - 1)
        def _():
            fetch_far(n + 1)

        row_ty = tile_row(n)
        tile_copy(0, n, 1 - chip).wait()
        h_rows = tiles[n % 2, :, pl.ds(0, 2 * dq)]
        gate = part[1, row_ty] + matmul(h_rows, w1f[span(1 - chip, 2 * dq), :])
        up_v = v_buf[row_ty] + matmul(h_rows, w3f[span(1 - chip, 2 * dq), :])
        part[1, row_ty] = gate
        v_buf[row_ty] = up_v
        act[0, span(row_ty, tb), :] = (gate * jax.nn.sigmoid(gate) * up_v).astype(BF16)
        return 0

    lax.fori_loop(0, NTY, far_step, 0)
    relay(3, 1, 0)
    e_copy(0, tile_row(NTY - 1)).start()
    hq, dyq = w1f.at[pl.ds(0, tokens), :], w3f.at[pl.ds(0, tokens), :]
    hq_copy = pltpu.make_async_copy(hg.at[:, span(tx, dq)], hq, l_l.at[1])
    dyq_copy = pltpu.make_async_copy(dyg.at[:, span(tx, dq)], dyq, l_l.at[2])
    hq_copy.start()
    w2_own_copy.wait()

    def sub_rows(sub):
        return span(sub, SUB)

    def q_copy(i):
        mat, layer, sub = item_of(i)
        return remote(part.at[mat, layer * 2 + 1 - y, sub_rows(sub), :], y_recv.at[mat, layer, sub_rows(sub), :],
                      q_s.at[i], q_r.at[i], (yp, tx))

    def send_block(mat, j):
        for sub in range(SUBS):
            q_copy((mat * NZ + j) * SUBS + sub).start()

    def part_row(jj):
        return (3 * (jj % NZ) % NZ) * 2 + 1 - y + (jj // NZ) * (2 * y - 1)

    def m_step(jj, _):
        row_ty = part_row(jj)
        rows = span(row_ty, tb)
        e_copy(0, row_ty).wait_recv()
        part[0, row_ty] = (matmul(act[0, rows, :], w2_own[span(core, fh), :])
                           + matmul(act[1, rows, :], w2_own[span(1 - core, fh), :]))

        @pl.when(jnp.logical_and(jj > 0, jj <= NZ))
        def _():
            send_block(0, jj - 1)

        return 0

    lax.fori_loop(0, NTY, m_step, 0)
    relay(3, 1, 1)

    def dy_arrive(layer, _):
        row_ty = layer * 2 + 1 - y
        y_copy(1, 0, layer, row_ty).wait_recv()
        d_copy(1, 0, row_ty, tx).start()
        return 0

    lax.fori_loop(0, NZ, dy_arrive, 0)
    dyq_copy.start()

    def c_refs(i):
        mat, layer, sub = item_of(i)
        return part.at[mat, layer * 2 + y, sub_rows(sub), :]

    def c_up(i):
        return remote(c_refs(i), z_buf.at[i], c_s.at[i], c_r.at[i], (up, tx))

    def c_dn(i):
        return remote(c_refs(i), z_buf.at[i], c_s.at[i], c_r.at[i], (dn, tx))

    def c_fin(i):
        mat, _, sub = item_of(i)
        k = mat * SUBS + sub
        return remote(c_refs(i), z_fin.at[k], c_s.at[i], f_r.at[k], (dn, tx))

    def add_to(i, value):
        mat, layer, sub = item_of(i)
        part[mat, layer * 2 + y, sub_rows(sub), :] = part[mat, layer * 2 + y, sub_rows(sub), :] + value

    def add_run(i):
        c_up(i).wait_recv()
        add_to(i, z_buf[i])

    def slot_step(slot):
        @pl.when(slot < ITEMS)
        def _():
            mat, layer, sub = item_of(slot)
            q_copy(slot).wait_recv()
            add_to(slot, y_recv[mat, layer, sub_rows(sub), :])

        i_up = slot - LAG * z
        l_up = item_of(jnp.maximum(i_up, 0))[1]

        @pl.when(jnp.logical_and(jnp.logical_and(i_up >= 0, i_up < ITEMS), l_up > z))
        def _():
            @pl.when(z > 0)
            def _():
                add_run(i_up)

            c_up(i_up).start()

        i_dn = slot - LAG * (NZ - 1 - z)
        l_dn = item_of(jnp.maximum(i_dn, 0))[1]

        @pl.when(jnp.logical_and(jnp.logical_and(i_dn >= 0, i_dn < ITEMS), l_dn < z))
        def _():
            @pl.when(z < NZ - 1)
            def _():
                add_run(i_dn)

            @pl.when(l_dn < z - 1)
            def _():
                c_dn(i_dn).start()

            @pl.when(l_dn == z - 1)
            def _():
                c_fin(i_dn).start()

        i_fin = slot - LAG * far
        l_fin = item_of(jnp.maximum(i_fin, 0))[1]

        @pl.when(jnp.logical_and(jnp.logical_and(i_fin >= 0, i_fin < ITEMS), l_fin == z))
        def _():
            mat, layer, sub = item_of(i_fin)

            @pl.when(z > 0)
            def _():
                add_run(i_fin)

            @pl.when(z < NZ - 1)
            def _():
                c_fin(i_fin).wait_recv()
                add_to(i_fin, z_fin[mat * SUBS + sub])

            rows = sub_rows(sub)

            @pl.when(mat == 0)
            def _():
                y_out[rows, :] = (x_ref[rows, :].astype(F32) + part[0, layer * 2 + y, rows, :]).astype(BF16)

            @pl.when(mat == 1)
            def _():
                d_h = part[1, layer * 2 + y, rows, :]
                x_hat = (x_ref[rows, :].astype(F32) - norm[rows, 0:1]) * norm[rows, 1:2]
                d_xhat = d_h * gain_ref[...].reshape(1, dq)
                sub_lane = lax.broadcasted_iota(jnp.int32, (SUB, 128), 1)
                pack[rows, :] = jnp.where(sub_lane == 0, jnp.sum(d_xhat, axis=1, keepdims=True),
                                          jnp.where(sub_lane == 1, jnp.sum(d_xhat * x_hat, axis=1, keepdims=True), 0.0))
                dg_buf[dg_row, :] = dg_buf[dg_row, :] + jnp.sum((d_h * x_hat).reshape(SUB // 8, 8, dq), axis=0)

    def fetch_dy(n):
        for s in (0, 1):
            d_copy(1, s, tile_row(n), cp).wait_recv()
        tile_copy(1, n).start()

    wait_w(2)
    fetch_dy(0)

    def down_step(n, _):
        @pl.when(n > 0)
        def _():
            e_copy(1, tile_row(n - 1)).start()
            e_copy(2, tile_row(n - 1)).start()

        @pl.when(n < NTY - 1)
        def _():
            fetch_dy(n + 1)

        row_ty = tile_row(n)
        rows = span(row_ty, tb)
        tile_copy(1, n).wait()
        d_act = contract_cols(tiles[n % 2], w2f[...])
        gate, up_v = part[1, row_ty], v_buf[row_ty]
        sig = jax.nn.sigmoid(gate)
        gate_g[0, rows, :] = (d_act * up_v * sig * (1.0 + gate * (1.0 - sig))).astype(BF16)
        up_g[0, rows, :] = (d_act * (gate * sig)).astype(BF16)

        slot_step(n)
        return 0

    lax.fori_loop(0, NTY, down_step, 0)
    e_copy(1, tile_row(NTY - 1)).start()
    e_copy(2, tile_row(NTY - 1)).start()
    w1_own, w3_own = w2f.at[:, pl.ds(0, f_loc)], w2f.at[:, pl.ds(f_loc, f_loc)]
    w1_own_copy = pltpu.make_async_copy(w1_ref, w1_own, l_l.at[3])
    w3_own_copy = pltpu.make_async_copy(w3_ref, w3_own, l_l.at[4])
    w1_own_copy.start()
    w3_own_copy.start()
    w1_own_copy.wait()
    w3_own_copy.wait()

    def dh_step(jj, _):
        row_ty = part_row(jj)
        rows = span(row_ty, tb)
        e_copy(1, row_ty).wait_recv()
        e_copy(2, row_ty).wait_recv()
        acc = contract_cols(gate_g[0, rows, :], w1_own[:, span(core, fh)])
        acc += contract_cols(gate_g[1, rows, :], w1_own[:, span(1 - core, fh)])
        acc += contract_cols(up_g[0, rows, :], w3_own[:, span(core, fh)])
        acc += contract_cols(up_g[1, rows, :], w3_own[:, span(1 - core, fh)])
        part[1, row_ty] = acc

        @pl.when(jnp.logical_and(jj > 0, jj <= NZ))
        def _():
            send_block(1, jj - 1)

        slot_step(NTY + jj)
        return 0

    lax.fori_loop(0, NTY, dh_step, 0)
    hq_copy.wait()
    dyq_copy.wait()

    def dw_copy(c, w):
        half = c % 2
        cols = span(core + half * (1 - 2 * core), fh)
        dst = (dw2_out.at[cols, :], dw1_out.at[:, cols], dw3_out.at[:, cols])[w]
        return pltpu.make_async_copy(stage, dst, dw_l.at[0])

    def weight_grads(slot):
        c = (slot - DW_FIRST) // DW_GAP
        half = c % 2

        def over_tokens(left, right):
            def piece(k, _):
                rows = span(k, DW_ROWS)
                stage[...] = stage[...] + contract_rows(left[rows, :], right[rows, :])
                return 0

            stage[...] = jnp.zeros(stage.shape, F32)
            lax.fori_loop(0, tokens // DW_ROWS, piece, 0)

        @pl.when(jnp.logical_and((slot - DW_FIRST) % DW_GAP == 0, slot < DW_FIRST + 6 * DW_GAP))
        def _():
            @pl.when(c >= 1)
            def _():
                dw_copy(c, 0).wait()

            for w in range(3):
                @pl.when(c // 2 == w)
                def _():
                    over_tokens(act.at[half] if w == 0 else hq, (dyq, gate_g.at[half], up_g.at[half])[w])
                    dw_copy(c, w).start()

    def last_slots(slot, _):
        weight_grads(slot)
        slot_step(slot)
        return 0

    lax.fori_loop(2 * NTY, ITEMS + LAG * (NZ - 2), last_slots, 0)

    def dg_copy(r, row):
        ref = dg_buf.at[span(row, 8), :]
        return remote(ref, ref, dg_s.at[r], dg_r.at[row], ((ty + r) % NTY, tx))

    def sb_copy(r, dev):
        return remote(sb_src, sb_buf.at[r], sb_s.at[r], sb_r.at[r], (ty, dev))

    sb_src[...] = pack[...].T[:8]
    for r in range(1, NTY):
        dg_copy(r, ty).start()
    for r, dev in tx_peers:
        sb_copy(r, dev).start()
    inv_std = norm[:, 1:2]
    x_hat = (x_ref[...].astype(F32) - norm[:, 0:1]) * inv_std
    d_xhat = part[1, ty] * gain_ref[...].reshape(1, dq)
    for r, dev in tx_peers:
        sb_copy(r, dev).wait_recv()
    total = sb_src[...] + sb_buf[0] + sb_buf[1] + sb_buf[2]
    total = jnp.concatenate([total, jnp.zeros((120, tb), F32)], axis=0).T / d_model
    dx_ln = inv_std * (d_xhat - total[:, 0:1] - x_hat * total[:, 1:2])
    dx_out[...] = (dy_ref[...].astype(F32) + dx_ln).astype(BF16)
    for r in range(1, NTY):
        dg_copy(r, (ty + NTY - r) % NTY).wait_recv()
    dg_out[...] = jnp.sum(dg_buf[...], axis=0)

    dw_copy(0, 0).wait()
    for r in range(1, NTY):
        dg_copy(r, ty).wait_send()
    for r, dev in tx_peers:
        sb_copy(r, dev).wait_send()
        stat_copy(r, dev).wait_send()
        for w in range(3):
            w_copy(w, r, dev).wait_send()
    for t in (0, 1):
        x_copy(t).wait_send()

    def drain(layer, _):
        for t, s in order:
            @pl.when(jnp.logical_and(z < NZ - 1, layer <= z))
            def _():
                z_copy(t, s, layer, up_s, up).wait_send()

            @pl.when(jnp.logical_and(z > 0, layer >= z))
            def _():
                z_copy(t, s, layer, dn_s, dn).wait_send()

            if (t, s) != (1, 1):
                y_copy(t, s, layer, layer * 2 + y).wait_send()
            d_copy(t, s, layer * 2, tx).wait_send()
            d_copy(t, s, layer * 2 + 1, tx).wait_send()

        @pl.when(jnp.logical_and(z < NZ - 1, layer <= z))
        def _():
            zo_copy(layer, uo_s, up).wait_send()

        @pl.when(jnp.logical_and(z > 0, layer >= z))
        def _():
            zo_copy(layer, do_s, dn).wait_send()

        return 0

    y_copy(1, 1, z, ty).wait_send()
    lax.fori_loop(0, NZ, drain, 0)

    def drain_swap(row_ty, _):
        for i in range(3):
            e_copy(i, row_ty).wait_send()
        return 0

    lax.fori_loop(0, NTY, drain_swap, 0)

    def drain_items(i, _):
        q_copy(i).wait_send()
        layer = item_of(i)[1]

        @pl.when(layer > z)
        def _():
            c_up(i).wait_send()

        @pl.when(layer < z)
        def _():
            c_dn(i).wait_send()

        return 0

    lax.fori_loop(0, ITEMS, drain_items, 0)


def pieces_of(arrays):
    out = []
    for n, array in enumerate(arrays):
        cuts = 4 if array.shape[0] * array.shape[1] > 400_000 else 1
        rows = array.shape[0] // cuts
        out += [(n, pl.ds(c * rows, rows)) for c in range(cuts)]
    return out


def hand_out_kernel(*refs):
    k = (len(refs) - 4) // 3
    gain_in, ins, gain_out, outs = refs[0], refs[1:1 + k], refs[1 + k], refs[2 + k:2 + 2 * k]
    bufs, (in_sem, out_sem) = refs[2 + 2 * k:2 + 3 * k], refs[2 + 3 * k:]
    pieces = pieces_of(ins)
    loads = [pltpu.make_async_copy(ins[n].at[rows, :], bufs[n].at[rows, :], in_sem.at[c])
             for c, (n, rows) in enumerate(pieces)]
    stores = [pltpu.make_async_copy(bufs[n].at[rows, :], outs[n].at[rows, :], out_sem.at[c])
              for c, (n, rows) in enumerate(pieces)]
    for load in loads:
        load.start()
    gain_out[...] = gain_in[...]
    for load, store in zip(loads, stores):
        load.wait()
        store.start()
    for store in stores:
        store.wait()


def hand_out(gain, arrays):
    k = len(arrays)
    vmem = pl.BlockSpec(memory_space=pltpu.VMEM)
    hbm = pl.BlockSpec(memory_space=pl.ANY)
    n_pieces = len(pieces_of(arrays))
    return pl.pallas_call(
        hand_out_kernel,
        out_shape=[jax.ShapeDtypeStruct(a.shape, a.dtype) for a in (gain, *arrays)],
        in_specs=[vmem] + [hbm] * k,
        out_specs=[vmem] + [hbm] * k,
        scratch_shapes=[pltpu.VMEM(a.shape, a.dtype) for a in arrays]
        + [pltpu.SemaphoreType.DMA((n_pieces,)), pltpu.SemaphoreType.DMA((n_pieces,))],
        compiler_params=pltpu.CompilerParams(vmem_limit_bytes=60_000_000),
    )(gain, *arrays)


def solution(mesh):
    def local_step(x_blk, dy_blk, gain_blk, w1, w3, w2):
        tb, dq = x_blk.shape
        tokens, d_model, f_loc = tb * NTY, dq * NTX, w1.shape[1]
        fh = f_loc // 2
        dma = pltpu.SemaphoreType.DMA
        vmem = pl.BlockSpec(memory_space=pltpu.VMEM)
        hbm = pl.BlockSpec(memory_space=pl.ANY)
        outs = pl.pallas_call(
            step_kernel,
            out_shape=[
                jax.ShapeDtypeStruct((tb, dq), BF16), jax.ShapeDtypeStruct((tb, dq), BF16),
                jax.ShapeDtypeStruct((dq, f_loc), F32), jax.ShapeDtypeStruct((dq, f_loc), F32),
                jax.ShapeDtypeStruct((f_loc, dq), F32), jax.ShapeDtypeStruct((dq,), F32),
                jax.ShapeDtypeStruct((tokens, d_model), BF16), jax.ShapeDtypeStruct((tokens, d_model), BF16)],
            in_specs=[vmem, vmem, vmem, hbm, hbm, hbm],
            out_specs=[vmem, vmem, hbm, hbm, hbm, vmem, hbm, hbm],
            scratch_shapes=[
                pltpu.VMEM((tb, dq), BF16), pltpu.VMEM((2, tb, d_model), BF16),
                pltpu.VMEM((d_model, fh), BF16), pltpu.VMEM((d_model, fh), BF16), pltpu.VMEM((fh, d_model), BF16),
                pltpu.VMEM((f_loc, dq), BF16),
                pltpu.VMEM((2, NTY, tb, dq), F32), pltpu.VMEM((NTY, tb, fh), F32),
                pltpu.VMEM((2, tokens, fh), BF16), pltpu.VMEM((2, tokens, fh), BF16), pltpu.VMEM((2, tokens, fh), BF16),
                pltpu.VMEM((2, NZ, tb, dq), F32), pltpu.VMEM((ITEMS, SUB, dq), F32), pltpu.VMEM((2 * SUBS, SUB, dq), F32),
                pltpu.VMEM((fh, dq), F32),
                pltpu.VMEM((8, tb), F32), pltpu.VMEM((3, 8, tb), F32),
                pltpu.VMEM((tb, 128), F32), pltpu.VMEM((8, tb), F32), pltpu.VMEM((3, 8, tb), F32),
                pltpu.VMEM((8 * NTY, dq), F32), pltpu.VMEM((tb, 128), F32),
                dma((3,)), dma((3,)), dma((2,)), dma((2,)),
                dma((2, 2, NZ)), dma((2, 2, NZ)), dma((2, 2, NZ)), dma((NZ,)), dma((NZ,)), dma((NZ,)),
                dma((2, 2, NZ)), dma((2, 2, NZ)),
                dma((2, 2, NTY)), dma((2, 2, NTY)),
                dma((3, 3)), dma((3, 3)), dma((3,)),
                dma((3, NTY)), dma((3, NTY)), dma((2,)), dma((2,)), dma((5,)),
                dma((ITEMS,)), dma((ITEMS,)), dma((ITEMS,)), dma((ITEMS,)), dma((2 * SUBS,)),
                dma((1,)), dma((3,)), dma((3,)), dma((NTY,)), dma((NTY,)),
            ],
            compiler_params=pltpu.CompilerParams(collective_id=0, has_side_effects=True,
                                                 vmem_limit_bytes=67_000_000),
            cost_estimate=pl.CostEstimate(flops=24 * tokens * d_model * fh, bytes_accessed=80_000_000,
                                          transcendentals=2 * tokens * fh),
        )(x_blk, dy_blk, gain_blk, w1, w3, w2)
        d_gain_blk, *rest = hand_out(outs[5], outs[:5])
        return (*rest, d_gain_blk)

    return jax.shard_map(
        local_step, mesh=mesh,
        in_specs=(P("ty", "tx"), P("ty", "tx"), P("tx"), P("tx", "ty"), P("tx", "ty"), P("ty", "tx")),
        out_specs=(P("ty", "tx"), P("ty", "tx"), P("tx", "ty"), P("tx", "ty"), P("ty", "tx"), P("tx")),
        check_vma=False)
```

```python
import jax
import jax.numpy as jnp
from jax import lax
from jax.experimental import pallas as pl
from jax.experimental.pallas import tpu as pltpu
from jax.sharding import PartitionSpec as P

LN_EPS = 1e-6
MESH = pl.DeviceIdType.MESH
F32 = jnp.float32
BF16 = jnp.bfloat16
NZ = 4
NTY = 8
NTX = 4
SUB = 32
SUBS = 8
ITEMS = 2 * NZ * SUBS
LAG = 3
DW_FIRST = 28
DW_GAP = 3
DW_ROWS = 512


def contract_rows(left_op, right_op):
    return lax.dot_general(left_op, right_op, (((0,), (0,)), ((), ())), preferred_element_type=F32)


def contract_cols(left_op, right_op):
    return lax.dot_general(left_op, right_op, (((1,), (1,)), ((), ())), preferred_element_type=F32)


def matmul(left_op, right_op):
    return jnp.dot(left_op, right_op, preferred_element_type=F32)


def remote(src, dst, send_sem, recv_sem, device):
    return pltpu.make_async_remote_copy(src_ref=src, dst_ref=dst, send_sem=send_sem, recv_sem=recv_sem,
                                        device_id=device, device_id_type=MESH)


def span(index, size):
    return pl.ds(pl.multiple_of(index * size, size), size)


def item_of(i):
    e = i % (NZ * SUBS)
    return i // (NZ * SUBS), pair_layer(e // (2 * SUBS), e % 2), e % (2 * SUBS) // 2


def pair_layer(pair, side):
    return pair + side * (NZ - 1 - 2 * pair)


def step_kernel(x_ref, dy_ref, gain_ref, w1_ref, w3_ref, w2_ref,
                y_out, dx_out, dw1_out, dw3_out, dw2_out, dg_out, hg, dyg,
                h_blk, tiles, w1f, w3f, w2f, w2_own, part, v_buf, act, gate_g, up_g, y_recv, z_buf, z_fin, stage,
                st_src, st_buf, pack, sb_src, sb_buf, dg_buf, norm,
                st_s, st_r, x_s, x_r, up_s, dn_s, z_r, uo_s, do_s, zo_r, y_s, y_r, d_s, d_r, w_s, w_r, w_l, e_s, e_r, t_l, o_l, l_l,
                q_s, q_r, c_s, c_r, f_r, dw_l, sb_s, sb_r, dg_s, dg_r):
    ty, tx = lax.axis_index("ty"), lax.axis_index("tx")
    z, y, core = ty // 2, ty % 2, tx % 2
    yp, up, dn = ty + 1 - 2 * y, ty + 2, ty - 2
    cp, xp, dp = tx + 1 - 2 * core, (tx + 2) % NTX, NTX - 1 - tx
    tx_peers = ((0, cp), (1, xp), (2, dp))
    tb, dq = x_ref.shape
    d_model = dq * NTX
    tokens = tb * NTY
    f_loc = w1_ref.shape[1]
    fh = f_loc // 2
    hi = z // 2
    near = z * (1 - hi) + (NZ - 1 - z) * hi
    far = NZ - 1 - near

    barrier = pltpu.get_barrier_semaphore()
    for _, dev in tx_peers:
        pl.semaphore_signal(barrier, inc=1, device_id=(ty, dev), device_id_type=MESH)
    for r in range(1, NTY):
        pl.semaphore_signal(barrier, inc=1, device_id=((ty + r) % NTY, tx), device_id_type=MESH)

    w_shards = (w1_ref, w3_ref, w2_ref)
    w_full = (w1f, w3f, w2f)

    def w_refs(w, c):
        mine = span(tx, dq)
        if w == 2:
            return w_shards[w].at[span(c, fh), :], w_full[w].at[:, mine]
        return w_shards[w].at[:, span(c, fh)], w_full[w].at[mine, :]

    def w_local(w):
        src, dst = w_refs(w, core)
        return pltpu.make_async_copy(src, dst, w_l.at[w])

    def w_copy(w, r, dev):
        src, dst = w_refs(w, dev % 2)
        return remote(src, dst, w_s.at[w, r], w_r.at[w, r], (ty, dev))

    def w_arrive(w, r, dev):
        theirs = span(dev, dq)
        dst = w_full[w].at[:, theirs] if w == 2 else w_full[w].at[theirs, :]
        return remote(dst, dst, w_s.at[w, r], w_r.at[w, r], (ty, dev))

    def wait_w(w):
        w_local(w).wait()
        for r, dev in tx_peers:
            w_arrive(w, r, dev).wait_recv()

    for w in range(3):
        w_local(w).start()
    w2_own_copy = pltpu.make_async_copy(w2_ref, w2_own, l_l.at[0])
    w2_own_copy.start()
    gathered = (hg, dyg)
    own_blk = (h_blk, dy_ref)

    def block(t, q, row_ty):
        return gathered[t].at[span(row_ty, tb), span(q, dq)]

    def own_local(t):
        return pltpu.make_async_copy(own_blk[t], block(t, tx, ty), o_l.at[t])

    own_local(1).start()

    x_float = x_ref[...].astype(F32)
    lane = lax.broadcasted_iota(jnp.int32, (tb, 128), 1)
    sum_1 = jnp.sum(x_float, axis=1, keepdims=True)
    sum_2 = jnp.sum(x_float * x_float, axis=1, keepdims=True)
    st_src[...] = jnp.where(lane == 0, sum_1, jnp.where(lane == 1, sum_2, 0.0)).T[:8]
    dg_row = span(ty, 8)
    dg_buf[dg_row, :] = jnp.zeros((8, dq), F32)

    pl.semaphore_wait(barrier, NTY + NTX - 2)

    def quarter(s, q):
        return q if s == 0 else (q + 2) % NTX

    def stat_copy(r, dev):
        return remote(st_src, st_buf.at[r], st_s.at[r], st_r.at[r], (ty, dev))

    def x_copy(t):
        return remote(own_blk[t], block(t, tx, ty), x_s.at[t], x_r.at[t], (ty, xp))

    def x_arrive(t):
        ref = block(t, xp, ty)
        return remote(ref, ref, x_s.at[t], x_r.at[t], (ty, xp))

    def z_copy(t, s, layer, sem, dev, own=False):
        ref = block(t, quarter(s, tx), layer * 2 + y)
        return remote(own_blk[t] if own else ref, ref, sem.at[t, s, layer], z_r.at[t, s, layer], (dev, tx))

    def y_copy(t, s, layer, row_ty, own=False):
        ref = block(t, quarter(s, tx), row_ty)
        return remote(own_blk[t] if own else ref, ref, y_s.at[t, s, layer], y_r.at[t, s, layer], (yp, tx))

    def d_copy(t, s, row_ty, q, own=False):
        ref = block(t, quarter(s, q), row_ty)
        return remote(own_blk[t] if own else ref, ref, d_s.at[t, s, row_ty], d_r.at[t, s, row_ty], (ty, cp))

    def spread(t, s, layer, own=False):
        y_copy(t, s, layer, layer * 2 + y, own).start()
        d_copy(t, s, layer * 2 + y, tx, own).start()

    def send_own(t, s):
        @pl.when(z < NZ - 1)
        def _():
            z_copy(t, s, z, up_s, up, s == 0).start()

        @pl.when(z > 0)
        def _():
            z_copy(t, s, z, dn_s, dn, s == 0).start()

        spread(t, s, z, s == 0)

    for r, dev in tx_peers:
        stat_copy(r, dev).start()
    for w in range(3):
        w_copy(w, 0, cp).start()
    x_copy(1).start()
    send_own(1, 0)
    for r, dev in tx_peers:
        stat_copy(r, dev).wait_recv()
    total = st_src[...] + st_buf[0] + st_buf[1] + st_buf[2]
    total = jnp.concatenate([total, jnp.zeros((120, tb), F32)], axis=0).T
    mean_x = total[:, 0:1] / d_model
    inv_std = lax.rsqrt(total[:, 1:2] / d_model - mean_x * mean_x + LN_EPS)
    gain_row = gain_ref[...].reshape(1, dq)
    h_blk[...] = (gain_row * ((x_float - mean_x) * inv_std)).astype(BF16)
    norm[...] = jnp.where(lane == 0, mean_x, jnp.where(lane == 1, inv_std, 0.0))
    own_local(0).start()
    x_copy(0).start()
    send_own(0, 0)
    for w in range(3):
        w_copy(w, 1, xp).start()
        w_copy(w, 2, dp).start()

    def zo_copy(layer, sem, dev):
        ref = block(1, quarter(1, tx), layer * 2 + 1 - y)
        return remote(ref, ref, sem.at[layer], zo_r.at[layer], (dev, tx))

    order = ((0, 0), (0, 1), (1, 0), (1, 1))

    def pass_up(layer, copy, sem, after):
        copy(layer, sem, dn).wait_recv()

        @pl.when(z < NZ - 1)
        def _():
            copy(layer, sem, up).start()

        after(layer)

    def pass_down(layer, copy, sem, after):
        copy(layer, sem, up).wait_recv()

        @pl.when(z > 0)
        def _():
            copy(layer, sem, dn).start()

        after(layer)

    def relay(k, t, s):
        def copy(layer, sem, dev):
            return z_copy(t, s, layer, sem, dev)

        def after(layer):
            if (t, s) != (1, 1):
                y_copy(t, s, layer, layer * 2 + y).start()
            d_copy(t, s, layer * 2 + y, tx).start()

        def after_other(layer):
            d_copy(1, 1, layer * 2 + 1 - y, tx).start()

        @pl.when(z >= k)
        def _():
            pass_up(z - k, copy, up_s, after)
            if (t, s) == (1, 1):
                pass_up(z - k, zo_copy, uo_s, after_other)

        @pl.when(z + k < NZ)
        def _():
            pass_down(z + k, copy, dn_s, after)
            if (t, s) == (1, 1):
                pass_down(z + k, zo_copy, do_s, after_other)

    for t in (1, 0):
        x_arrive(t).wait_recv()
        send_own(t, 1)
    for s in (0, 1):
        relay(1, 0, s)
    y_copy(1, 1, z, ty + 1 - 2 * y).wait_recv()

    @pl.when(z < NZ - 1)
    def _():
        zo_copy(z, uo_s, up).start()

    @pl.when(z > 0)
    def _():
        zo_copy(z, do_s, dn).start()

    d_copy(1, 1, yp, tx).start()
    for s in (0, 1):
        relay(2, 0, s)
    for s in (0, 1):
        relay(1, 1, s)
    for s in (0, 1):
        relay(3, 0, s)
    own_local(0).wait()
    own_local(1).wait()

    def layer_of(n):
        m = n % NZ
        base = m + near * (1 - 2 * m) * (1 - m // 2)
        return base + hi * (NZ - 1 - 2 * base)

    def tile_row(n):
        return layer_of(n) * 2 + y + (n // NZ) * (1 - 2 * y)

    chip = tx // 2

    def tile_copy(t, n, half=None):
        rows = span(tile_row(n), tb)
        if half is None:
            return pltpu.make_async_copy(gathered[t].at[rows, :], tiles.at[n % 2], t_l.at[n % 2])
        return pltpu.make_async_copy(gathered[t].at[rows, span(half, 2 * dq)], tiles.at[n % 2, :, pl.ds(0, 2 * dq)],
                                     t_l.at[n % 2])

    swaps = (act, gate_g, up_g)

    def e_copy(i, row_ty):
        rows = span(row_ty, tb)
        return remote(swaps[i].at[0, rows, :], swaps[i].at[1, rows, :], e_s.at[i, row_ty], e_r.at[i, row_ty],
                      (ty, cp))

    def fetch_near(n):
        row_ty = tile_row(n)

        @pl.when(n >= NZ)
        def _():
            for s in (0, 1):
                y_copy(0, s, layer_of(n), row_ty).wait_recv()
                d_copy(0, s, row_ty, tx).start()

        d_copy(0, 0, row_ty, cp).wait_recv()
        tile_copy(0, n, chip).start()

    def fetch_far(n):
        d_copy(0, 1, tile_row(n), cp).wait_recv()
        tile_copy(0, n, 1 - chip).start()

    def near_step(n, _):
        @pl.when(n < NTY - 1)
        def _():
            fetch_near(n + 1)

        row_ty = tile_row(n)
        tile_copy(0, n, chip).wait()
        h_rows = tiles[n % 2, :, pl.ds(0, 2 * dq)]
        part[1, row_ty] = matmul(h_rows, w1f[span(chip, 2 * dq), :])
        v_buf[row_ty] = matmul(h_rows, w3f[span(chip, 2 * dq), :])
        return 0

    for w in (0, 1):
        w_local(w).wait()
        w_arrive(w, 0, cp).wait_recv()
    fetch_near(0)
    lax.fori_loop(0, NTY, near_step, 0)
    for s in (0, 1):
        relay(2, 1, s)
    for w in (0, 1):
        w_arrive(w, 1, xp).wait_recv()
        w_arrive(w, 2, dp).wait_recv()
    fetch_far(0)

    def far_step(n, _):
        @pl.when(n > 0)
        def _():
            e_copy(0, tile_row(n - 1)).start()

        @pl.when(n < NTY - 1)
        def _():
            fetch_far(n + 1)

        row_ty = tile_row(n)
        tile_copy(0, n, 1 - chip).wait()
        h_rows = tiles[n % 2, :, pl.ds(0, 2 * dq)]
        gate = part[1, row_ty] + matmul(h_rows, w1f[span(1 - chip, 2 * dq), :])
        up_v = v_buf[row_ty] + matmul(h_rows, w3f[span(1 - chip, 2 * dq), :])
        part[1, row_ty] = gate
        v_buf[row_ty] = up_v
        act[0, span(row_ty, tb), :] = (gate * jax.nn.sigmoid(gate) * up_v).astype(BF16)
        return 0

    lax.fori_loop(0, NTY, far_step, 0)
    relay(3, 1, 0)
    e_copy(0, tile_row(NTY - 1)).start()
    hq, dyq = w1f.at[pl.ds(0, tokens), :], w3f.at[pl.ds(0, tokens), :]
    hq_copy = pltpu.make_async_copy(hg.at[:, span(tx, dq)], hq, l_l.at[1])
    dyq_copy = pltpu.make_async_copy(dyg.at[:, span(tx, dq)], dyq, l_l.at[2])
    hq_copy.start()
    w2_own_copy.wait()

    def sub_rows(sub):
        return span(sub, SUB)

    def q_copy(i):
        mat, layer, sub = item_of(i)
        return remote(part.at[mat, layer * 2 + 1 - y, sub_rows(sub), :], y_recv.at[mat, layer, sub_rows(sub), :],
                      q_s.at[i], q_r.at[i], (yp, tx))

    def send_pair(mat, pair):
        for e in range(2 * SUBS):
            q_copy((mat * 2 + pair) * 2 * SUBS + e).start()

    def part_row(jj):
        return pair_layer(jj % NZ // 2, jj % 2) * 2 + 1 - y + (jj // NZ) * (2 * y - 1)

    def m_step(jj, _):
        row_ty = part_row(jj)
        rows = span(row_ty, tb)
        e_copy(0, row_ty).wait_recv()
        part[0, row_ty] = (matmul(act[0, rows, :], w2_own[span(core, fh), :])
                           + matmul(act[1, rows, :], w2_own[span(1 - core, fh), :]))

        @pl.when(jnp.logical_and(jj % 2 == 0, jnp.logical_and(jj > 0, jj <= NZ)))
        def _():
            send_pair(0, jj // 2 - 1)

        return 0

    lax.fori_loop(0, NTY, m_step, 0)
    relay(3, 1, 1)

    def dy_arrive(layer, _):
        row_ty = layer * 2 + 1 - y
        y_copy(1, 0, layer, row_ty).wait_recv()
        d_copy(1, 0, row_ty, tx).start()
        return 0

    lax.fori_loop(0, NZ, dy_arrive, 0)
    dyq_copy.start()

    def c_refs(i):
        mat, layer, sub = item_of(i)
        return part.at[mat, layer * 2 + y, sub_rows(sub), :]

    def c_up(i):
        return remote(c_refs(i), z_buf.at[i], c_s.at[i], c_r.at[i], (up, tx))

    def c_dn(i):
        return remote(c_refs(i), z_buf.at[i], c_s.at[i], c_r.at[i], (dn, tx))

    def c_fin(i):
        mat, _, sub = item_of(i)
        k = mat * SUBS + sub
        return remote(c_refs(i), z_fin.at[k], c_s.at[i], f_r.at[k], (dn, tx))

    def add_to(i, value):
        mat, layer, sub = item_of(i)
        part[mat, layer * 2 + y, sub_rows(sub), :] = part[mat, layer * 2 + y, sub_rows(sub), :] + value

    def add_run(i):
        c_up(i).wait_recv()
        add_to(i, z_buf[i])

    def slot_step(slot):
        @pl.when(slot < ITEMS)
        def _():
            mat, layer, sub = item_of(slot)
            q_copy(slot).wait_recv()
            add_to(slot, y_recv[mat, layer, sub_rows(sub), :])

        i_up = slot - LAG * z
        l_up = item_of(jnp.maximum(i_up, 0))[1]

        @pl.when(jnp.logical_and(jnp.logical_and(i_up >= 0, i_up < ITEMS), l_up > z))
        def _():
            @pl.when(z > 0)
            def _():
                add_run(i_up)

            c_up(i_up).start()

        i_dn = slot - LAG * (NZ - 1 - z)
        l_dn = item_of(jnp.maximum(i_dn, 0))[1]

        @pl.when(jnp.logical_and(jnp.logical_and(i_dn >= 0, i_dn < ITEMS), l_dn < z))
        def _():
            @pl.when(z < NZ - 1)
            def _():
                add_run(i_dn)

            @pl.when(l_dn < z - 1)
            def _():
                c_dn(i_dn).start()

            @pl.when(l_dn == z - 1)
            def _():
                c_fin(i_dn).start()

        i_fin = slot - LAG * far
        l_fin = item_of(jnp.maximum(i_fin, 0))[1]

        @pl.when(jnp.logical_and(jnp.logical_and(i_fin >= 0, i_fin < ITEMS), l_fin == z))
        def _():
            mat, layer, sub = item_of(i_fin)

            @pl.when(z > 0)
            def _():
                add_run(i_fin)

            @pl.when(z < NZ - 1)
            def _():
                c_fin(i_fin).wait_recv()
                add_to(i_fin, z_fin[mat * SUBS + sub])

            rows = sub_rows(sub)

            @pl.when(mat == 0)
            def _():
                y_out[rows, :] = (x_ref[rows, :].astype(F32) + part[0, layer * 2 + y, rows, :]).astype(BF16)

            @pl.when(mat == 1)
            def _():
                d_h = part[1, layer * 2 + y, rows, :]
                x_hat = (x_ref[rows, :].astype(F32) - norm[rows, 0:1]) * norm[rows, 1:2]
                d_xhat = d_h * gain_ref[...].reshape(1, dq)
                sub_lane = lax.broadcasted_iota(jnp.int32, (SUB, 128), 1)
                pack[rows, :] = jnp.where(sub_lane == 0, jnp.sum(d_xhat, axis=1, keepdims=True),
                                          jnp.where(sub_lane == 1, jnp.sum(d_xhat * x_hat, axis=1, keepdims=True), 0.0))
                dg_buf[dg_row, :] = dg_buf[dg_row, :] + jnp.sum((d_h * x_hat).reshape(SUB // 8, 8, dq), axis=0)

    def fetch_dy(n):
        for s in (0, 1):
            d_copy(1, s, tile_row(n), cp).wait_recv()
        tile_copy(1, n).start()

    def early_slots(slot, _):
        slot_step(slot)
        return 0

    lax.fori_loop(0, NTY, early_slots, 0)
    wait_w(2)
    fetch_dy(0)

    def down_step(n, _):
        @pl.when(n > 0)
        def _():
            e_copy(1, tile_row(n - 1)).start()
            e_copy(2, tile_row(n - 1)).start()

        @pl.when(n < NTY - 1)
        def _():
            fetch_dy(n + 1)

        row_ty = tile_row(n)
        rows = span(row_ty, tb)
        tile_copy(1, n).wait()
        d_act = contract_cols(tiles[n % 2], w2f[...])
        gate, up_v = part[1, row_ty], v_buf[row_ty]
        sig = jax.nn.sigmoid(gate)
        gate_g[0, rows, :] = (d_act * up_v * sig * (1.0 + gate * (1.0 - sig))).astype(BF16)
        up_g[0, rows, :] = (d_act * (gate * sig)).astype(BF16)

        slot_step(NTY + n)
        return 0

    lax.fori_loop(0, NTY, down_step, 0)
    e_copy(1, tile_row(NTY - 1)).start()
    e_copy(2, tile_row(NTY - 1)).start()
    w1_own, w3_own = w2f.at[:, pl.ds(0, f_loc)], w2f.at[:, pl.ds(f_loc, f_loc)]
    w1_own_copy = pltpu.make_async_copy(w1_ref, w1_own, l_l.at[3])
    w3_own_copy = pltpu.make_async_copy(w3_ref, w3_own, l_l.at[4])
    w1_own_copy.start()
    w3_own_copy.start()
    w1_own_copy.wait()
    w3_own_copy.wait()

    def dh_step(jj, _):
        row_ty = part_row(jj)
        rows = span(row_ty, tb)
        e_copy(1, row_ty).wait_recv()
        e_copy(2, row_ty).wait_recv()
        acc = contract_cols(gate_g[0, rows, :], w1_own[:, span(core, fh)])
        acc += contract_cols(gate_g[1, rows, :], w1_own[:, span(1 - core, fh)])
        acc += contract_cols(up_g[0, rows, :], w3_own[:, span(core, fh)])
        acc += contract_cols(up_g[1, rows, :], w3_own[:, span(1 - core, fh)])
        part[1, row_ty] = acc

        @pl.when(jnp.logical_and(jj % 2 == 0, jnp.logical_and(jj > 0, jj <= NZ)))
        def _():
            send_pair(1, jj // 2 - 1)

        slot_step(2 * NTY + jj)
        return 0

    lax.fori_loop(0, NTY, dh_step, 0)
    hq_copy.wait()
    dyq_copy.wait()

    def dw_copy(c, w):
        half = c % 2
        cols = span(core + half * (1 - 2 * core), fh)
        dst = (dw2_out.at[cols, :], dw1_out.at[:, cols], dw3_out.at[:, cols])[w]
        return pltpu.make_async_copy(stage, dst, dw_l.at[0])

    def weight_grads(slot):
        c = (slot - DW_FIRST) // DW_GAP
        half = c % 2

        def over_tokens(left, right):
            def piece(k, _):
                rows = span(k, DW_ROWS)
                stage[...] = stage[...] + contract_rows(left[rows, :], right[rows, :])
                return 0

            stage[...] = jnp.zeros(stage.shape, F32)
            lax.fori_loop(0, tokens // DW_ROWS, piece, 0)

        @pl.when(jnp.logical_and((slot - DW_FIRST) % DW_GAP == 0, slot < DW_FIRST + 6 * DW_GAP))
        def _():
            @pl.when(c >= 1)
            def _():
                dw_copy(c, 0).wait()

            for w in range(3):
                @pl.when(c // 2 == w)
                def _():
                    over_tokens(act.at[half] if w == 0 else hq, (dyq, gate_g.at[half], up_g.at[half])[w])
                    dw_copy(c, w).start()

    def last_slots(slot, _):
        weight_grads(slot)
        slot_step(slot)
        return 0

    lax.fori_loop(3 * NTY, ITEMS + LAG * (NZ - 2), last_slots, 0)

    def dg_copy(r, row):
        ref = dg_buf.at[span(row, 8), :]
        return remote(ref, ref, dg_s.at[r], dg_r.at[row], ((ty + r) % NTY, tx))

    def sb_copy(r, dev):
        return remote(sb_src, sb_buf.at[r], sb_s.at[r], sb_r.at[r], (ty, dev))

    sb_src[...] = pack[...].T[:8]
    for r in range(1, NTY):
        dg_copy(r, ty).start()
    for r, dev in tx_peers:
        sb_copy(r, dev).start()
    inv_std = norm[:, 1:2]
    x_hat = (x_ref[...].astype(F32) - norm[:, 0:1]) * inv_std
    d_xhat = part[1, ty] * gain_ref[...].reshape(1, dq)
    for r, dev in tx_peers:
        sb_copy(r, dev).wait_recv()
    total = sb_src[...] + sb_buf[0] + sb_buf[1] + sb_buf[2]
    total = jnp.concatenate([total, jnp.zeros((120, tb), F32)], axis=0).T / d_model
    dx_ln = inv_std * (d_xhat - total[:, 0:1] - x_hat * total[:, 1:2])
    dx_out[...] = (dy_ref[...].astype(F32) + dx_ln).astype(BF16)
    for r in range(1, NTY):
        dg_copy(r, (ty + NTY - r) % NTY).wait_recv()
    dg_out[...] = jnp.sum(dg_buf[...], axis=0)

    dw_copy(0, 0).wait()
    for r in range(1, NTY):
        dg_copy(r, ty).wait_send()
    for r, dev in tx_peers:
        sb_copy(r, dev).wait_send()
        stat_copy(r, dev).wait_send()
        for w in range(3):
            w_copy(w, r, dev).wait_send()
    for t in (0, 1):
        x_copy(t).wait_send()

    def drain(layer, _):
        for t, s in order:
            @pl.when(jnp.logical_and(z < NZ - 1, layer <= z))
            def _():
                z_copy(t, s, layer, up_s, up).wait_send()

            @pl.when(jnp.logical_and(z > 0, layer >= z))
            def _():
                z_copy(t, s, layer, dn_s, dn).wait_send()

            if (t, s) != (1, 1):
                y_copy(t, s, layer, layer * 2 + y).wait_send()
            d_copy(t, s, layer * 2, tx).wait_send()
            d_copy(t, s, layer * 2 + 1, tx).wait_send()

        @pl.when(jnp.logical_and(z < NZ - 1, layer <= z))
        def _():
            zo_copy(layer, uo_s, up).wait_send()

        @pl.when(jnp.logical_and(z > 0, layer >= z))
        def _():
            zo_copy(layer, do_s, dn).wait_send()

        return 0

    y_copy(1, 1, z, ty).wait_send()
    lax.fori_loop(0, NZ, drain, 0)

    def drain_swap(row_ty, _):
        for i in range(3):
            e_copy(i, row_ty).wait_send()
        return 0

    lax.fori_loop(0, NTY, drain_swap, 0)

    def drain_items(i, _):
        q_copy(i).wait_send()
        layer = item_of(i)[1]

        @pl.when(layer > z)
        def _():
            c_up(i).wait_send()

        @pl.when(layer < z)
        def _():
            c_dn(i).wait_send()

        return 0

    lax.fori_loop(0, ITEMS, drain_items, 0)


def pieces_of(arrays):
    out = []
    for n, array in enumerate(arrays):
        cuts = 4 if array.shape[0] * array.shape[1] > 400_000 else 1
        rows = array.shape[0] // cuts
        out += [(n, pl.ds(c * rows, rows)) for c in range(cuts)]
    return out


def hand_out_kernel(*refs):
    k = (len(refs) - 4) // 3
    gain_in, ins, gain_out, outs = refs[0], refs[1:1 + k], refs[1 + k], refs[2 + k:2 + 2 * k]
    bufs, (in_sem, out_sem) = refs[2 + 2 * k:2 + 3 * k], refs[2 + 3 * k:]
    pieces = pieces_of(ins)
    loads = [pltpu.make_async_copy(ins[n].at[rows, :], bufs[n].at[rows, :], in_sem.at[c])
             for c, (n, rows) in enumerate(pieces)]
    stores = [pltpu.make_async_copy(bufs[n].at[rows, :], outs[n].at[rows, :], out_sem.at[c])
              for c, (n, rows) in enumerate(pieces)]
    for load in loads:
        load.start()
    gain_out[...] = gain_in[...]
    for load, store in zip(loads, stores):
        load.wait()
        store.start()
    for store in stores:
        store.wait()


def hand_out(gain, arrays):
    k = len(arrays)
    vmem = pl.BlockSpec(memory_space=pltpu.VMEM)
    hbm = pl.BlockSpec(memory_space=pl.ANY)
    n_pieces = len(pieces_of(arrays))
    return pl.pallas_call(
        hand_out_kernel,
        out_shape=[jax.ShapeDtypeStruct(a.shape, a.dtype) for a in (gain, *arrays)],
        in_specs=[vmem] + [hbm] * k,
        out_specs=[vmem] + [hbm] * k,
        scratch_shapes=[pltpu.VMEM(a.shape, a.dtype) for a in arrays]
        + [pltpu.SemaphoreType.DMA((n_pieces,)), pltpu.SemaphoreType.DMA((n_pieces,))],
        compiler_params=pltpu.CompilerParams(vmem_limit_bytes=60_000_000),
    )(gain, *arrays)


def solution(mesh):
    def local_step(x_blk, dy_blk, gain_blk, w1, w3, w2):
        tb, dq = x_blk.shape
        tokens, d_model, f_loc = tb * NTY, dq * NTX, w1.shape[1]
        fh = f_loc // 2
        dma = pltpu.SemaphoreType.DMA
        vmem = pl.BlockSpec(memory_space=pltpu.VMEM)
        hbm = pl.BlockSpec(memory_space=pl.ANY)
        outs = pl.pallas_call(
            step_kernel,
            out_shape=[
                jax.ShapeDtypeStruct((tb, dq), BF16), jax.ShapeDtypeStruct((tb, dq), BF16),
                jax.ShapeDtypeStruct((dq, f_loc), F32), jax.ShapeDtypeStruct((dq, f_loc), F32),
                jax.ShapeDtypeStruct((f_loc, dq), F32), jax.ShapeDtypeStruct((dq,), F32),
                jax.ShapeDtypeStruct((tokens, d_model), BF16), jax.ShapeDtypeStruct((tokens, d_model), BF16)],
            in_specs=[vmem, vmem, vmem, hbm, hbm, hbm],
            out_specs=[vmem, vmem, hbm, hbm, hbm, vmem, hbm, hbm],
            scratch_shapes=[
                pltpu.VMEM((tb, dq), BF16), pltpu.VMEM((2, tb, d_model), BF16),
                pltpu.VMEM((d_model, fh), BF16), pltpu.VMEM((d_model, fh), BF16), pltpu.VMEM((fh, d_model), BF16),
                pltpu.VMEM((f_loc, dq), BF16),
                pltpu.VMEM((2, NTY, tb, dq), F32), pltpu.VMEM((NTY, tb, fh), F32),
                pltpu.VMEM((2, tokens, fh), BF16), pltpu.VMEM((2, tokens, fh), BF16), pltpu.VMEM((2, tokens, fh), BF16),
                pltpu.VMEM((2, NZ, tb, dq), F32), pltpu.VMEM((ITEMS, SUB, dq), F32), pltpu.VMEM((2 * SUBS, SUB, dq), F32),
                pltpu.VMEM((fh, dq), F32),
                pltpu.VMEM((8, tb), F32), pltpu.VMEM((3, 8, tb), F32),
                pltpu.VMEM((tb, 128), F32), pltpu.VMEM((8, tb), F32), pltpu.VMEM((3, 8, tb), F32),
                pltpu.VMEM((8 * NTY, dq), F32), pltpu.VMEM((tb, 128), F32),
                dma((3,)), dma((3,)), dma((2,)), dma((2,)),
                dma((2, 2, NZ)), dma((2, 2, NZ)), dma((2, 2, NZ)), dma((NZ,)), dma((NZ,)), dma((NZ,)),
                dma((2, 2, NZ)), dma((2, 2, NZ)),
                dma((2, 2, NTY)), dma((2, 2, NTY)),
                dma((3, 3)), dma((3, 3)), dma((3,)),
                dma((3, NTY)), dma((3, NTY)), dma((2,)), dma((2,)), dma((5,)),
                dma((ITEMS,)), dma((ITEMS,)), dma((ITEMS,)), dma((ITEMS,)), dma((2 * SUBS,)),
                dma((1,)), dma((3,)), dma((3,)), dma((NTY,)), dma((NTY,)),
            ],
            compiler_params=pltpu.CompilerParams(collective_id=0, has_side_effects=True,
                                                 vmem_limit_bytes=67_000_000),
            cost_estimate=pl.CostEstimate(flops=24 * tokens * d_model * fh, bytes_accessed=80_000_000,
                                          transcendentals=2 * tokens * fh),
        )(x_blk, dy_blk, gain_blk, w1, w3, w2)
        d_gain_blk, *rest = hand_out(outs[5], outs[:5])
        return (*rest, d_gain_blk)

    return jax.shard_map(
        local_step, mesh=mesh,
        in_specs=(P("ty", "tx"), P("ty", "tx"), P("tx"), P("tx", "ty"), P("tx", "ty"), P("ty", "tx")),
        out_specs=(P("ty", "tx"), P("ty", "tx"), P("tx", "ty"), P("tx", "ty"), P("ty", "tx"), P("tx")),
        check_vma=False)
```

```python
import jax
import jax.numpy as jnp
from jax import lax
from jax.experimental import pallas as pl
from jax.experimental.pallas import tpu as pltpu
from jax.sharding import PartitionSpec as P

LN_EPS = 1e-6
MESH = pl.DeviceIdType.MESH
F32 = jnp.float32
BF16 = jnp.bfloat16
NZ = 4
NTY = 8
NTX = 4
SUB = 32
SUBS = 8
ITEMS = 2 * NZ * SUBS
LAG = 3
DW_FIRST = 28
DW_GAP = 3
DW_ROWS = 512
DRAIN_LAG = 24
DRAIN_SLOT = 46


def contract_rows(left_op, right_op):
    return lax.dot_general(left_op, right_op, (((0,), (0,)), ((), ())), preferred_element_type=F32)


def contract_cols(left_op, right_op):
    return lax.dot_general(left_op, right_op, (((1,), (1,)), ((), ())), preferred_element_type=F32)


def matmul(left_op, right_op):
    return jnp.dot(left_op, right_op, preferred_element_type=F32)


def remote(src, dst, send_sem, recv_sem, device):
    return pltpu.make_async_remote_copy(src_ref=src, dst_ref=dst, send_sem=send_sem, recv_sem=recv_sem,
                                        device_id=device, device_id_type=MESH)


def span(index, size):
    return pl.ds(pl.multiple_of(index * size, size), size)


def item_of(i):
    e = i % (NZ * SUBS)
    return i // (NZ * SUBS), pair_layer(e // (2 * SUBS), e % 2), e % (2 * SUBS) // 2


def pair_layer(pair, side):
    return pair + side * (NZ - 1 - 2 * pair)


def step_kernel(x_ref, dy_ref, gain_ref, w1_ref, w3_ref, w2_ref,
                y_out, dx_out, dw1_out, dw3_out, dw2_out, dg_out, hg, dyg,
                h_blk, tiles, w1f, w3f, w2f, w2_own, part, v_buf, act, gate_g, up_g, y_recv, z_buf, z_fin, stage,
                st_src, st_buf, pack, sb_src, sb_buf, dg_buf, norm,
                st_s, st_r, x_s, x_r, up_s, dn_s, z_r, uo_s, do_s, zo_r, y_s, y_r, d_s, d_r, w_s, w_r, w_l, e_s, e_r, t_l, o_l, l_l,
                q_s, q_r, c_s, c_r, f_r, dw_l, sb_s, sb_r, dg_s, dg_r):
    ty, tx = lax.axis_index("ty"), lax.axis_index("tx")
    z, y, core = ty // 2, ty % 2, tx % 2
    yp, up, dn = ty + 1 - 2 * y, ty + 2, ty - 2
    cp, xp, dp = tx + 1 - 2 * core, (tx + 2) % NTX, NTX - 1 - tx
    tx_peers = ((0, cp), (1, xp), (2, dp))
    tb, dq = x_ref.shape
    d_model = dq * NTX
    tokens = tb * NTY
    f_loc = w1_ref.shape[1]
    fh = f_loc // 2
    hi = z // 2
    near = z * (1 - hi) + (NZ - 1 - z) * hi
    far = NZ - 1 - near

    barrier = pltpu.get_barrier_semaphore()
    for _, dev in tx_peers:
        pl.semaphore_signal(barrier, inc=1, device_id=(ty, dev), device_id_type=MESH)
    for r in range(1, NTY):
        pl.semaphore_signal(barrier, inc=1, device_id=((ty + r) % NTY, tx), device_id_type=MESH)

    w_shards = (w1_ref, w3_ref, w2_ref)
    w_full = (w1f, w3f, w2f)

    def w_refs(w, c):
        mine = span(tx, dq)
        if w == 2:
            return w_shards[w].at[span(c, fh), :], w_full[w].at[:, mine]
        return w_shards[w].at[:, span(c, fh)], w_full[w].at[mine, :]

    def w_local(w):
        src, dst = w_refs(w, core)
        return pltpu.make_async_copy(src, dst, w_l.at[w])

    def w_copy(w, r, dev):
        src, dst = w_refs(w, dev % 2)
        return remote(src, dst, w_s.at[w, r], w_r.at[w, r], (ty, dev))

    def w_arrive(w, r, dev):
        theirs = span(dev, dq)
        dst = w_full[w].at[:, theirs] if w == 2 else w_full[w].at[theirs, :]
        return remote(dst, dst, w_s.at[w, r], w_r.at[w, r], (ty, dev))

    def wait_w(w):
        w_local(w).wait()
        for r, dev in tx_peers:
            w_arrive(w, r, dev).wait_recv()

    for w in range(3):
        w_local(w).start()
    w2_own_copy = pltpu.make_async_copy(w2_ref, w2_own, l_l.at[0])
    w2_own_copy.start()
    gathered = (hg, dyg)
    own_blk = (h_blk, dy_ref)

    def block(t, q, row_ty):
        return gathered[t].at[span(row_ty, tb), span(q, dq)]

    def own_local(t):
        return pltpu.make_async_copy(own_blk[t], block(t, tx, ty), o_l.at[t])

    own_local(1).start()

    x_float = x_ref[...].astype(F32)
    lane = lax.broadcasted_iota(jnp.int32, (tb, 128), 1)
    sum_1 = jnp.sum(x_float, axis=1, keepdims=True)
    sum_2 = jnp.sum(x_float * x_float, axis=1, keepdims=True)
    st_src[...] = jnp.where(lane == 0, sum_1, jnp.where(lane == 1, sum_2, 0.0)).T[:8]
    dg_row = span(ty, 8)
    dg_buf[dg_row, :] = jnp.zeros((8, dq), F32)

    pl.semaphore_wait(barrier, NTY + NTX - 2)

    def quarter(s, q):
        return q if s == 0 else (q + 2) % NTX

    def stat_copy(r, dev):
        return remote(st_src, st_buf.at[r], st_s.at[r], st_r.at[r], (ty, dev))

    def x_copy(t):
        return remote(own_blk[t], block(t, tx, ty), x_s.at[t], x_r.at[t], (ty, xp))

    def x_arrive(t):
        ref = block(t, xp, ty)
        return remote(ref, ref, x_s.at[t], x_r.at[t], (ty, xp))

    def z_copy(t, s, layer, sem, dev, own=False):
        ref = block(t, quarter(s, tx), layer * 2 + y)
        return remote(own_blk[t] if own else ref, ref, sem.at[t, s, layer], z_r.at[t, s, layer], (dev, tx))

    def y_copy(t, s, layer, row_ty, own=False):
        ref = block(t, quarter(s, tx), row_ty)
        return remote(own_blk[t] if own else ref, ref, y_s.at[t, s, layer], y_r.at[t, s, layer], (yp, tx))

    def d_copy(t, s, row_ty, q, own=False):
        ref = block(t, quarter(s, q), row_ty)
        return remote(own_blk[t] if own else ref, ref, d_s.at[t, s, row_ty], d_r.at[t, s, row_ty], (ty, cp))

    def spread(t, s, layer, own=False):
        y_copy(t, s, layer, layer * 2 + y, own).start()
        d_copy(t, s, layer * 2 + y, tx, own).start()

    def send_own(t, s):
        @pl.when(z < NZ - 1)
        def _():
            z_copy(t, s, z, up_s, up, s == 0).start()

        @pl.when(z > 0)
        def _():
            z_copy(t, s, z, dn_s, dn, s == 0).start()

        spread(t, s, z, s == 0)

    for r, dev in tx_peers:
        stat_copy(r, dev).start()
    for w in range(3):
        w_copy(w, 0, cp).start()
    x_copy(1).start()
    send_own(1, 0)
    for r, dev in tx_peers:
        stat_copy(r, dev).wait_recv()
    total = st_src[...] + st_buf[0] + st_buf[1] + st_buf[2]
    total = jnp.concatenate([total, jnp.zeros((120, tb), F32)], axis=0).T
    mean_x = total[:, 0:1] / d_model
    inv_std = lax.rsqrt(total[:, 1:2] / d_model - mean_x * mean_x + LN_EPS)
    gain_row = gain_ref[...].reshape(1, dq)
    h_blk[...] = (gain_row * ((x_float - mean_x) * inv_std)).astype(BF16)
    norm[...] = jnp.where(lane == 0, mean_x, jnp.where(lane == 1, inv_std, 0.0))
    own_local(0).start()
    x_copy(0).start()
    send_own(0, 0)
    for w in range(3):
        w_copy(w, 1, xp).start()
        w_copy(w, 2, dp).start()

    def zo_copy(layer, sem, dev):
        ref = block(1, quarter(1, tx), layer * 2 + 1 - y)
        return remote(ref, ref, sem.at[layer], zo_r.at[layer], (dev, tx))

    order = ((0, 0), (0, 1), (1, 0), (1, 1))

    def pass_up(layer, copy, sem, after):
        copy(layer, sem, dn).wait_recv()

        @pl.when(z < NZ - 1)
        def _():
            copy(layer, sem, up).start()

        after(layer)

    def pass_down(layer, copy, sem, after):
        copy(layer, sem, up).wait_recv()

        @pl.when(z > 0)
        def _():
            copy(layer, sem, dn).start()

        after(layer)

    def relay(k, t, s):
        def copy(layer, sem, dev):
            return z_copy(t, s, layer, sem, dev)

        def after(layer):
            if (t, s) != (1, 1):
                y_copy(t, s, layer, layer * 2 + y).start()
            d_copy(t, s, layer * 2 + y, tx).start()

        def after_other(layer):
            d_copy(1, 1, layer * 2 + 1 - y, tx).start()

        @pl.when(z >= k)
        def _():
            pass_up(z - k, copy, up_s, after)
            if (t, s) == (1, 1):
                pass_up(z - k, zo_copy, uo_s, after_other)

        @pl.when(z + k < NZ)
        def _():
            pass_down(z + k, copy, dn_s, after)
            if (t, s) == (1, 1):
                pass_down(z + k, zo_copy, do_s, after_other)

    for t in (1, 0):
        x_arrive(t).wait_recv()
        send_own(t, 1)
    for s in (0, 1):
        relay(1, 0, s)
    y_copy(1, 1, z, ty + 1 - 2 * y).wait_recv()

    @pl.when(z < NZ - 1)
    def _():
        zo_copy(z, uo_s, up).start()

    @pl.when(z > 0)
    def _():
        zo_copy(z, do_s, dn).start()

    d_copy(1, 1, yp, tx).start()
    for s in (0, 1):
        relay(2, 0, s)
    for s in (0, 1):
        relay(1, 1, s)
    for s in (0, 1):
        relay(3, 0, s)
    own_local(0).wait()
    own_local(1).wait()

    def layer_of(n):
        m = n % NZ
        base = m + near * (1 - 2 * m) * (1 - m // 2)
        return base + hi * (NZ - 1 - 2 * base)

    def tile_row(n):
        return layer_of(n) * 2 + y + (n // NZ) * (1 - 2 * y)

    chip = tx // 2

    def tile_copy(t, n, half=None):
        rows = span(tile_row(n), tb)
        if half is None:
            return pltpu.make_async_copy(gathered[t].at[rows, :], tiles.at[n % 2], t_l.at[n % 2])
        return pltpu.make_async_copy(gathered[t].at[rows, span(half, 2 * dq)], tiles.at[n % 2, :, pl.ds(0, 2 * dq)],
                                     t_l.at[n % 2])

    swaps = (act, gate_g, up_g)

    def e_copy(i, row_ty):
        rows = span(row_ty, tb)
        return remote(swaps[i].at[0, rows, :], swaps[i].at[1, rows, :], e_s.at[i, row_ty], e_r.at[i, row_ty],
                      (ty, cp))

    def fetch_near(n):
        row_ty = tile_row(n)

        @pl.when(n >= NZ)
        def _():
            for s in (0, 1):
                y_copy(0, s, layer_of(n), row_ty).wait_recv()
                d_copy(0, s, row_ty, tx).start()

        d_copy(0, 0, row_ty, cp).wait_recv()
        tile_copy(0, n, chip).start()

    def near_step(n, _):
        @pl.when(n < NTY - 1)
        def _():
            fetch_near(n + 1)

        row_ty = tile_row(n)
        tile_copy(0, n, chip).wait()
        h_rows = tiles[n % 2, :, pl.ds(0, 2 * dq)]
        part[1, row_ty] = matmul(h_rows, w1f[span(chip, 2 * dq), :])
        v_buf[row_ty] = matmul(h_rows, w3f[span(chip, 2 * dq), :])
        return 0

    for w in (0, 1):
        w_local(w).wait()
        w_arrive(w, 0, cp).wait_recv()
    fetch_near(0)
    lax.fori_loop(0, NTY, near_step, 0)
    for s in (0, 1):
        relay(2, 1, s)
    for w in (0, 1):
        w_arrive(w, 1, xp).wait_recv()
        w_arrive(w, 2, dp).wait_recv()
    def sub_rows(sub):
        return span(sub, SUB)

    def q_copy(i):
        mat, layer, sub = item_of(i)
        return remote(part.at[mat, layer * 2 + 1 - y, sub_rows(sub), :], y_recv.at[mat, layer, sub_rows(sub), :],
                      q_s.at[i], q_r.at[i], (yp, tx))

    def send_pair(mat, pair):
        for e in range(2 * SUBS):
            q_copy((mat * 2 + pair) * 2 * SUBS + e).start()

    def part_row(jj):
        return pair_layer(jj % NZ // 2, jj % 2) * 2 + 1 - y + (jj // NZ) * (2 * y - 1)

    def far_copy(jj):
        src = hg.at[span(part_row(jj), tb), span(1 - chip, 2 * dq)]
        return pltpu.make_async_copy(src, tiles.at[jj % 2, :, pl.ds(0, 2 * dq)], t_l.at[jj % 2])

    def fetch_far(jj):
        d_copy(0, 1, part_row(jj), cp).wait_recv()
        far_copy(jj).start()

    def far_step(jj, _):
        @pl.when(jj % 2 == 1)
        def _():
            e_copy(0, part_row(jj - 1)).start()

        @pl.when(jj < NTY - 1)
        def _():
            fetch_far(jj + 1)

        row_ty = part_row(jj)
        far_copy(jj).wait()
        h_rows = tiles[jj % 2, :, pl.ds(0, 2 * dq)]
        gate = part[1, row_ty] + matmul(h_rows, w1f[span(1 - chip, 2 * dq), :])
        up_v = v_buf[row_ty] + matmul(h_rows, w3f[span(1 - chip, 2 * dq), :])
        part[1, row_ty] = gate
        v_buf[row_ty] = up_v
        act[0, span(row_ty, tb), :] = (gate * jax.nn.sigmoid(gate) * up_v).astype(BF16)
        return 0

    def m_step(jj, _):
        row_ty = part_row(jj)
        rows = span(row_ty, tb)
        e_copy(0, row_ty).wait_recv()
        part[0, row_ty] = (matmul(act[0, rows, :], w2_own[span(core, fh), :])
                           + matmul(act[1, rows, :], w2_own[span(1 - core, fh), :]))
        return 0

    def two_tiles(g, _):
        lax.fori_loop(2 * g, 2 * g + 2, far_step, 0)
        e_copy(0, part_row(2 * g + 1)).start()
        lax.fori_loop(2 * g, 2 * g + 2, m_step, 0)

        @pl.when(g == 0)
        def _():
            relay(3, 1, 0)

        @pl.when(g < 2)
        def _():
            send_pair(0, g)

        return 0

    w2_own_copy.wait()
    fetch_far(0)
    lax.fori_loop(0, NTY // 2, two_tiles, 0)
    hq, dyq = w1f.at[pl.ds(0, tokens), :], w3f.at[pl.ds(0, tokens), :]
    hq_copy = pltpu.make_async_copy(hg.at[:, span(tx, dq)], hq, l_l.at[1])
    dyq_copy = pltpu.make_async_copy(dyg.at[:, span(tx, dq)], dyq, l_l.at[2])
    hq_copy.start()

    relay(3, 1, 1)

    def dy_arrive(layer, _):
        row_ty = layer * 2 + 1 - y
        y_copy(1, 0, layer, row_ty).wait_recv()
        d_copy(1, 0, row_ty, tx).start()
        return 0

    lax.fori_loop(0, NZ, dy_arrive, 0)
    dyq_copy.start()

    def c_refs(i):
        mat, layer, sub = item_of(i)
        return part.at[mat, layer * 2 + y, sub_rows(sub), :]

    def c_up(i):
        return remote(c_refs(i), z_buf.at[i], c_s.at[i], c_r.at[i], (up, tx))

    def c_dn(i):
        return remote(c_refs(i), z_buf.at[i], c_s.at[i], c_r.at[i], (dn, tx))

    def c_fin(i):
        mat, _, sub = item_of(i)
        k = mat * SUBS + sub
        return remote(c_refs(i), z_fin.at[k], c_s.at[i], f_r.at[k], (dn, tx))

    def add_to(i, value):
        mat, layer, sub = item_of(i)
        part[mat, layer * 2 + y, sub_rows(sub), :] = part[mat, layer * 2 + y, sub_rows(sub), :] + value

    def add_run(i):
        c_up(i).wait_recv()
        add_to(i, z_buf[i])

    def slot_step(slot):
        @pl.when(slot < ITEMS)
        def _():
            mat, layer, sub = item_of(slot)
            q_copy(slot).wait_recv()
            add_to(slot, y_recv[mat, layer, sub_rows(sub), :])

        i_up = slot - LAG * z
        l_up = item_of(jnp.maximum(i_up, 0))[1]

        @pl.when(jnp.logical_and(jnp.logical_and(i_up >= 0, i_up < ITEMS), l_up > z))
        def _():
            @pl.when(z > 0)
            def _():
                add_run(i_up)

            c_up(i_up).start()

        i_dn = slot - LAG * (NZ - 1 - z)
        l_dn = item_of(jnp.maximum(i_dn, 0))[1]

        @pl.when(jnp.logical_and(jnp.logical_and(i_dn >= 0, i_dn < ITEMS), l_dn < z))
        def _():
            @pl.when(z < NZ - 1)
            def _():
                add_run(i_dn)

            @pl.when(l_dn < z - 1)
            def _():
                c_dn(i_dn).start()

            @pl.when(l_dn == z - 1)
            def _():
                c_fin(i_dn).start()

        i_fin = slot - LAG * far
        l_fin = item_of(jnp.maximum(i_fin, 0))[1]

        @pl.when(jnp.logical_and(jnp.logical_and(i_fin >= 0, i_fin < ITEMS), l_fin == z))
        def _():
            mat, layer, sub = item_of(i_fin)

            @pl.when(z > 0)
            def _():
                add_run(i_fin)

            @pl.when(z < NZ - 1)
            def _():
                c_fin(i_fin).wait_recv()
                add_to(i_fin, z_fin[mat * SUBS + sub])

            rows = sub_rows(sub)

            @pl.when(mat == 0)
            def _():
                y_out[rows, :] = (x_ref[rows, :].astype(F32) + part[0, layer * 2 + y, rows, :]).astype(BF16)

            @pl.when(mat == 1)
            def _():
                d_h = part[1, layer * 2 + y, rows, :]
                x_hat = (x_ref[rows, :].astype(F32) - norm[rows, 0:1]) * norm[rows, 1:2]
                d_xhat = d_h * gain_ref[...].reshape(1, dq)
                sub_lane = lax.broadcasted_iota(jnp.int32, (SUB, 128), 1)
                pack[rows, :] = jnp.where(sub_lane == 0, jnp.sum(d_xhat, axis=1, keepdims=True),
                                          jnp.where(sub_lane == 1, jnp.sum(d_xhat * x_hat, axis=1, keepdims=True), 0.0))
                dg_buf[dg_row, :] = dg_buf[dg_row, :] + jnp.sum((d_h * x_hat).reshape(SUB // 8, 8, dq), axis=0)

    def fetch_dy(n):
        for s in (0, 1):
            d_copy(1, s, tile_row(n), cp).wait_recv()
        tile_copy(1, n).start()

    def early_slots(slot, _):
        slot_step(slot)
        return 0

    lax.fori_loop(0, NTY, early_slots, 0)
    wait_w(2)
    fetch_dy(0)

    def down_step(n, _):
        @pl.when(n > 0)
        def _():
            e_copy(1, tile_row(n - 1)).start()
            e_copy(2, tile_row(n - 1)).start()

        @pl.when(n < NTY - 1)
        def _():
            fetch_dy(n + 1)

        row_ty = tile_row(n)
        rows = span(row_ty, tb)
        tile_copy(1, n).wait()
        d_act = contract_cols(tiles[n % 2], w2f[...])
        gate, up_v = part[1, row_ty], v_buf[row_ty]
        sig = jax.nn.sigmoid(gate)
        gate_g[0, rows, :] = (d_act * up_v * sig * (1.0 + gate * (1.0 - sig))).astype(BF16)
        up_g[0, rows, :] = (d_act * (gate * sig)).astype(BF16)

        slot_step(NTY + n)
        return 0

    lax.fori_loop(0, NTY, down_step, 0)
    e_copy(1, tile_row(NTY - 1)).start()
    e_copy(2, tile_row(NTY - 1)).start()
    w1_own, w3_own = w2f.at[:, pl.ds(0, f_loc)], w2f.at[:, pl.ds(f_loc, f_loc)]
    w1_own_copy = pltpu.make_async_copy(w1_ref, w1_own, l_l.at[3])
    w3_own_copy = pltpu.make_async_copy(w3_ref, w3_own, l_l.at[4])
    w1_own_copy.start()
    w3_own_copy.start()
    w1_own_copy.wait()
    w3_own_copy.wait()

    def dh_step(jj, _):
        row_ty = part_row(jj)
        rows = span(row_ty, tb)
        e_copy(1, row_ty).wait_recv()
        e_copy(2, row_ty).wait_recv()
        acc = contract_cols(gate_g[0, rows, :], w1_own[:, span(core, fh)])
        acc += contract_cols(gate_g[1, rows, :], w1_own[:, span(1 - core, fh)])
        acc += contract_cols(up_g[0, rows, :], w3_own[:, span(core, fh)])
        acc += contract_cols(up_g[1, rows, :], w3_own[:, span(1 - core, fh)])
        part[1, row_ty] = acc

        @pl.when(jnp.logical_and(jj % 2 == 0, jnp.logical_and(jj > 0, jj <= NZ)))
        def _():
            send_pair(1, jj // 2 - 1)

        slot_step(2 * NTY + jj)
        return 0

    lax.fori_loop(0, NTY, dh_step, 0)
    hq_copy.wait()
    dyq_copy.wait()

    def dw_copy(c, w):
        half = c % 2
        cols = span(core + half * (1 - 2 * core), fh)
        dst = (dw2_out.at[cols, :], dw1_out.at[:, cols], dw3_out.at[:, cols])[w]
        return pltpu.make_async_copy(stage, dst, dw_l.at[0])

    def weight_grads(slot):
        c = (slot - DW_FIRST) // DW_GAP
        half = c % 2

        def over_tokens(left, right):
            def piece(k, _):
                rows = span(k, DW_ROWS)
                stage[...] = stage[...] + contract_rows(left[rows, :], right[rows, :])
                return 0

            stage[...] = jnp.zeros(stage.shape, F32)
            lax.fori_loop(0, tokens // DW_ROWS, piece, 0)

        @pl.when(jnp.logical_and((slot - DW_FIRST) % DW_GAP == 0, slot < DW_FIRST + 6 * DW_GAP))
        def _():
            @pl.when(c >= 1)
            def _():
                dw_copy(c, 0).wait()

            for w in range(3):
                @pl.when(c // 2 == w)
                def _():
                    over_tokens(act.at[half] if w == 0 else hq, (dyq, gate_g.at[half], up_g.at[half])[w])
                    dw_copy(c, w).start()

    def drain_gathers():
        for r, dev in tx_peers:
            stat_copy(r, dev).wait_send()
            for w in range(3):
                w_copy(w, r, dev).wait_send()
        for t in (0, 1):
            x_copy(t).wait_send()
        y_copy(1, 1, z, ty).wait_send()

        def drain_layer(layer, _):
            for t, s in order:
                @pl.when(jnp.logical_and(z < NZ - 1, layer <= z))
                def _():
                    z_copy(t, s, layer, up_s, up).wait_send()

                @pl.when(jnp.logical_and(z > 0, layer >= z))
                def _():
                    z_copy(t, s, layer, dn_s, dn).wait_send()

                if (t, s) != (1, 1):
                    y_copy(t, s, layer, layer * 2 + y).wait_send()
                d_copy(t, s, layer * 2, tx).wait_send()
                d_copy(t, s, layer * 2 + 1, tx).wait_send()

            @pl.when(jnp.logical_and(z < NZ - 1, layer <= z))
            def _():
                zo_copy(layer, uo_s, up).wait_send()

            @pl.when(jnp.logical_and(z > 0, layer >= z))
            def _():
                zo_copy(layer, do_s, dn).wait_send()

            return 0

        def drain_swap(row_ty, _):
            for i in range(3):
                e_copy(i, row_ty).wait_send()
            return 0

        lax.fori_loop(0, NZ, drain_layer, 0)
        lax.fori_loop(0, NTY, drain_swap, 0)

    def drain_item(i, _):
        q_copy(i).wait_send()
        layer = item_of(i)[1]

        @pl.when(layer > z)
        def _():
            c_up(i).wait_send()

        @pl.when(layer < z)
        def _():
            c_dn(i).wait_send()

        return 0

    def last_slots(slot, _):
        weight_grads(slot)
        slot_step(slot)
        drain_item(slot - DRAIN_LAG, 0)

        @pl.when(slot == DRAIN_SLOT)
        def _():
            drain_gathers()

        return 0

    lax.fori_loop(3 * NTY, ITEMS + LAG * (NZ - 2), last_slots, 0)

    def dg_copy(r, row):
        ref = dg_buf.at[span(row, 8), :]
        return remote(ref, ref, dg_s.at[r], dg_r.at[row], ((ty + r) % NTY, tx))

    def sb_copy(r, dev):
        return remote(sb_src, sb_buf.at[r], sb_s.at[r], sb_r.at[r], (ty, dev))

    sb_src[...] = pack[...].T[:8]
    for r in range(1, NTY):
        dg_copy(r, ty).start()
    for r, dev in tx_peers:
        sb_copy(r, dev).start()
    inv_std = norm[:, 1:2]
    x_hat = (x_ref[...].astype(F32) - norm[:, 0:1]) * inv_std
    d_xhat = part[1, ty] * gain_ref[...].reshape(1, dq)
    for r, dev in tx_peers:
        sb_copy(r, dev).wait_recv()
    total = sb_src[...] + sb_buf[0] + sb_buf[1] + sb_buf[2]
    total = jnp.concatenate([total, jnp.zeros((120, tb), F32)], axis=0).T / d_model
    dx_ln = inv_std * (d_xhat - total[:, 0:1] - x_hat * total[:, 1:2])
    dx_out[...] = (dy_ref[...].astype(F32) + dx_ln).astype(BF16)
    for r in range(1, NTY):
        dg_copy(r, (ty + NTY - r) % NTY).wait_recv()
    dg_out[...] = jnp.sum(dg_buf[...], axis=0)

    dw_copy(0, 0).wait()
    for r in range(1, NTY):
        dg_copy(r, ty).wait_send()
    for r, dev in tx_peers:
        sb_copy(r, dev).wait_send()
    lax.fori_loop(ITEMS + LAG * (NZ - 2) - DRAIN_LAG, ITEMS, drain_item, 0)


def pieces_of(arrays):
    out = []
    for n, array in enumerate(arrays):
        cuts = 4 if array.shape[0] * array.shape[1] > 400_000 else 1
        rows = array.shape[0] // cuts
        out += [(n, pl.ds(c * rows, rows)) for c in range(cuts)]
    return out


def hand_out_kernel(*refs):
    k = (len(refs) - 4) // 3
    gain_in, ins, gain_out, outs = refs[0], refs[1:1 + k], refs[1 + k], refs[2 + k:2 + 2 * k]
    bufs, (in_sem, out_sem) = refs[2 + 2 * k:2 + 3 * k], refs[2 + 3 * k:]
    pieces = pieces_of(ins)
    loads = [pltpu.make_async_copy(ins[n].at[rows, :], bufs[n].at[rows, :], in_sem.at[c])
             for c, (n, rows) in enumerate(pieces)]
    stores = [pltpu.make_async_copy(bufs[n].at[rows, :], outs[n].at[rows, :], out_sem.at[c])
              for c, (n, rows) in enumerate(pieces)]
    for load in loads:
        load.start()
    gain_out[...] = gain_in[...]
    for load, store in zip(loads, stores):
        load.wait()
        store.start()
    for store in stores:
        store.wait()


def hand_out(gain, arrays):
    k = len(arrays)
    vmem = pl.BlockSpec(memory_space=pltpu.VMEM)
    hbm = pl.BlockSpec(memory_space=pl.ANY)
    n_pieces = len(pieces_of(arrays))
    return pl.pallas_call(
        hand_out_kernel,
        out_shape=[jax.ShapeDtypeStruct(a.shape, a.dtype) for a in (gain, *arrays)],
        in_specs=[vmem] + [hbm] * k,
        out_specs=[vmem] + [hbm] * k,
        scratch_shapes=[pltpu.VMEM(a.shape, a.dtype) for a in arrays]
        + [pltpu.SemaphoreType.DMA((n_pieces,)), pltpu.SemaphoreType.DMA((n_pieces,))],
        compiler_params=pltpu.CompilerParams(vmem_limit_bytes=60_000_000),
    )(gain, *arrays)


def solution(mesh):
    def local_step(x_blk, dy_blk, gain_blk, w1, w3, w2):
        tb, dq = x_blk.shape
        tokens, d_model, f_loc = tb * NTY, dq * NTX, w1.shape[1]
        fh = f_loc // 2
        dma = pltpu.SemaphoreType.DMA
        vmem = pl.BlockSpec(memory_space=pltpu.VMEM)
        hbm = pl.BlockSpec(memory_space=pl.ANY)
        outs = pl.pallas_call(
            step_kernel,
            out_shape=[
                jax.ShapeDtypeStruct((tb, dq), BF16), jax.ShapeDtypeStruct((tb, dq), BF16),
                jax.ShapeDtypeStruct((dq, f_loc), F32), jax.ShapeDtypeStruct((dq, f_loc), F32),
                jax.ShapeDtypeStruct((f_loc, dq), F32), jax.ShapeDtypeStruct((dq,), F32),
                jax.ShapeDtypeStruct((tokens, d_model), BF16), jax.ShapeDtypeStruct((tokens, d_model), BF16)],
            in_specs=[vmem, vmem, vmem, hbm, hbm, hbm],
            out_specs=[vmem, vmem, hbm, hbm, hbm, vmem, hbm, hbm],
            scratch_shapes=[
                pltpu.VMEM((tb, dq), BF16), pltpu.VMEM((2, tb, d_model), BF16),
                pltpu.VMEM((d_model, fh), BF16), pltpu.VMEM((d_model, fh), BF16), pltpu.VMEM((fh, d_model), BF16),
                pltpu.VMEM((f_loc, dq), BF16),
                pltpu.VMEM((2, NTY, tb, dq), F32), pltpu.VMEM((NTY, tb, fh), F32),
                pltpu.VMEM((2, tokens, fh), BF16), pltpu.VMEM((2, tokens, fh), BF16), pltpu.VMEM((2, tokens, fh), BF16),
                pltpu.VMEM((2, NZ, tb, dq), F32), pltpu.VMEM((ITEMS, SUB, dq), F32), pltpu.VMEM((2 * SUBS, SUB, dq), F32),
                pltpu.VMEM((fh, dq), F32),
                pltpu.VMEM((8, tb), F32), pltpu.VMEM((3, 8, tb), F32),
                pltpu.VMEM((tb, 128), F32), pltpu.VMEM((8, tb), F32), pltpu.VMEM((3, 8, tb), F32),
                pltpu.VMEM((8 * NTY, dq), F32), pltpu.VMEM((tb, 128), F32),
                dma((3,)), dma((3,)), dma((2,)), dma((2,)),
                dma((2, 2, NZ)), dma((2, 2, NZ)), dma((2, 2, NZ)), dma((NZ,)), dma((NZ,)), dma((NZ,)),
                dma((2, 2, NZ)), dma((2, 2, NZ)),
                dma((2, 2, NTY)), dma((2, 2, NTY)),
                dma((3, 3)), dma((3, 3)), dma((3,)),
                dma((3, NTY)), dma((3, NTY)), dma((2,)), dma((2,)), dma((5,)),
                dma((ITEMS,)), dma((ITEMS,)), dma((ITEMS,)), dma((ITEMS,)), dma((2 * SUBS,)),
                dma((1,)), dma((3,)), dma((3,)), dma((NTY,)), dma((NTY,)),
            ],
            compiler_params=pltpu.CompilerParams(collective_id=0, has_side_effects=True,
                                                 vmem_limit_bytes=67_000_000),
            cost_estimate=pl.CostEstimate(flops=24 * tokens * d_model * fh, bytes_accessed=80_000_000,
                                          transcendentals=2 * tokens * fh),
        )(x_blk, dy_blk, gain_blk, w1, w3, w2)
        d_gain_blk, *rest = hand_out(outs[5], outs[:5])
        return (*rest, d_gain_blk)

    return jax.shard_map(
        local_step, mesh=mesh,
        in_specs=(P("ty", "tx"), P("ty", "tx"), P("tx"), P("tx", "ty"), P("tx", "ty"), P("ty", "tx")),
        out_specs=(P("ty", "tx"), P("ty", "tx"), P("tx", "ty"), P("tx", "ty"), P("ty", "tx"), P("tx")),
        check_vma=False)
```

```python
import jax
import jax.numpy as jnp
from jax import lax
from jax.experimental import pallas as pl
from jax.experimental.pallas import tpu as pltpu
from jax.sharding import PartitionSpec as P

LN_EPS = 1e-6
MESH = pl.DeviceIdType.MESH
F32 = jnp.float32
BF16 = jnp.bfloat16
NZ = 4
NTY = 8
NTX = 4
SUB = 32
SUBS = 8
ITEMS = 2 * NZ * SUBS
LAG = 3
DW_FIRST = 28
DW_GAP = 3
DW_ROWS = 512
DRAIN_LAG = 24
DRAIN_SLOT = 46


def contract_rows(left_op, right_op):
    return lax.dot_general(left_op, right_op, (((0,), (0,)), ((), ())), preferred_element_type=F32)


def contract_cols(left_op, right_op):
    return lax.dot_general(left_op, right_op, (((1,), (1,)), ((), ())), preferred_element_type=F32)


def matmul(left_op, right_op):
    return jnp.dot(left_op, right_op, preferred_element_type=F32)


def remote(src, dst, send_sem, recv_sem, device):
    return pltpu.make_async_remote_copy(src_ref=src, dst_ref=dst, send_sem=send_sem, recv_sem=recv_sem,
                                        device_id=device, device_id_type=MESH)


def span(index, size):
    return pl.ds(pl.multiple_of(index * size, size), size)


def item_of(i):
    e = i % (NZ * SUBS)
    return i // (NZ * SUBS), pair_layer(e // (2 * SUBS), e % 2), e % (2 * SUBS) // 2


def pair_layer(pair, side):
    return pair + side * (NZ - 1 - 2 * pair)


def step_kernel(x_ref, dy_ref, gain_ref, w1_ref, w3_ref, w2_ref,
                y_out, dx_out, dw1_out, dw3_out, dw2_out, dg_out, hg, dyg,
                h_blk, tiles, w1f, w3f, w2f, w2_own, part, v_buf, act, gate_g, up_g, y_recv, z_buf, z_fin, stage,
                st_src, st_buf, pack, sb_src, sb_buf, dg_buf, norm,
                st_s, st_r, x_s, x_r, up_s, dn_s, z_r, uo_s, do_s, zo_r, y_s, y_r, d_s, d_r, w_s, w_r, w_l, e_s, e_r, t_l, o_l, l_l,
                q_s, q_r, c_s, c_r, f_r, dw_l, sb_s, sb_r, dg_s, dg_r):
    ty, tx = lax.axis_index("ty"), lax.axis_index("tx")
    z, y, core = ty // 2, ty % 2, tx % 2
    yp, up, dn = ty + 1 - 2 * y, ty + 2, ty - 2
    cp, xp, dp = tx + 1 - 2 * core, (tx + 2) % NTX, NTX - 1 - tx
    tx_peers = ((0, cp), (1, xp), (2, dp))
    tb, dq = x_ref.shape
    d_model = dq * NTX
    tokens = tb * NTY
    f_loc = w1_ref.shape[1]
    fh = f_loc // 2
    hi = z // 2
    near = z * (1 - hi) + (NZ - 1 - z) * hi
    far = NZ - 1 - near

    barrier = pltpu.get_barrier_semaphore()
    for _, dev in tx_peers:
        pl.semaphore_signal(barrier, inc=1, device_id=(ty, dev), device_id_type=MESH)
    for r in range(1, NTY):
        pl.semaphore_signal(barrier, inc=1, device_id=((ty + r) % NTY, tx), device_id_type=MESH)

    w_shards = (w1_ref, w3_ref, w2_ref)
    w_full = (w1f, w3f, w2f)

    def w_refs(w, c):
        mine = span(tx, dq)
        if w == 2:
            return w_shards[w].at[span(c, fh), :], w_full[w].at[:, mine]
        return w_shards[w].at[:, span(c, fh)], w_full[w].at[mine, :]

    def w_local(w):
        src, dst = w_refs(w, core)
        return pltpu.make_async_copy(src, dst, w_l.at[w])

    def w_copy(w, r, dev):
        src, dst = w_refs(w, dev % 2)
        return remote(src, dst, w_s.at[w, r], w_r.at[w, r], (ty, dev))

    def w_arrive(w, r, dev):
        theirs = span(dev, dq)
        dst = w_full[w].at[:, theirs] if w == 2 else w_full[w].at[theirs, :]
        return remote(dst, dst, w_s.at[w, r], w_r.at[w, r], (ty, dev))

    def wait_w(w):
        w_local(w).wait()
        for r, dev in tx_peers:
            w_arrive(w, r, dev).wait_recv()

    for w in range(3):
        w_local(w).start()
    w2_own_copy = pltpu.make_async_copy(w2_ref, w2_own, l_l.at[0])
    w2_own_copy.start()
    gathered = (hg, dyg)
    own_blk = (h_blk, dy_ref)

    def block(t, q, row_ty):
        return gathered[t].at[span(row_ty, tb), span(q, dq)]

    def own_local(t):
        return pltpu.make_async_copy(own_blk[t], block(t, tx, ty), o_l.at[t])

    own_local(1).start()

    x_float = x_ref[...].astype(F32)
    lane = lax.broadcasted_iota(jnp.int32, (tb, 128), 1)
    sum_1 = jnp.sum(x_float, axis=1, keepdims=True)
    sum_2 = jnp.sum(x_float * x_float, axis=1, keepdims=True)
    st_src[...] = jnp.where(lane == 0, sum_1, jnp.where(lane == 1, sum_2, 0.0)).T[:8]
    dg_row = span(ty, 8)
    dg_buf[dg_row, :] = jnp.zeros((8, dq), F32)

    pl.semaphore_wait(barrier, NTY + NTX - 2)

    def quarter(s, q):
        return q if s == 0 else (q + 2) % NTX

    def stat_copy(r, dev):
        return remote(st_src, st_buf.at[r], st_s.at[r], st_r.at[r], (ty, dev))

    def x_copy(t):
        return remote(own_blk[t], block(t, tx, ty), x_s.at[t], x_r.at[t], (ty, xp))

    def x_arrive(t):
        ref = block(t, xp, ty)
        return remote(ref, ref, x_s.at[t], x_r.at[t], (ty, xp))

    def z_copy(t, s, layer, sem, dev, own=False):
        ref = block(t, quarter(s, tx), layer * 2 + y)
        return remote(own_blk[t] if own else ref, ref, sem.at[t, s, layer], z_r.at[t, s, layer], (dev, tx))

    def y_copy(t, s, layer, row_ty, own=False):
        ref = block(t, quarter(s, tx), row_ty)
        return remote(own_blk[t] if own else ref, ref, y_s.at[t, s, layer], y_r.at[t, s, layer], (yp, tx))

    def d_copy(t, s, row_ty, q, own=False):
        ref = block(t, quarter(s, q), row_ty)
        return remote(own_blk[t] if own else ref, ref, d_s.at[t, s, row_ty], d_r.at[t, s, row_ty], (ty, cp))

    def spread(t, s, layer, own=False):
        y_copy(t, s, layer, layer * 2 + y, own).start()
        d_copy(t, s, layer * 2 + y, tx, own).start()

    def send_own(t, s):
        @pl.when(z < NZ - 1)
        def _():
            z_copy(t, s, z, up_s, up, s == 0).start()

        @pl.when(z > 0)
        def _():
            z_copy(t, s, z, dn_s, dn, s == 0).start()

        spread(t, s, z, s == 0)

    for r, dev in tx_peers:
        stat_copy(r, dev).start()
    for w in range(3):
        w_copy(w, 0, cp).start()
    x_copy(1).start()
    send_own(1, 0)
    for r, dev in tx_peers:
        stat_copy(r, dev).wait_recv()
    total = st_src[...] + st_buf[0] + st_buf[1] + st_buf[2]
    total = jnp.concatenate([total, jnp.zeros((120, tb), F32)], axis=0).T
    mean_x = total[:, 0:1] / d_model
    inv_std = lax.rsqrt(total[:, 1:2] / d_model - mean_x * mean_x + LN_EPS)
    gain_row = gain_ref[...].reshape(1, dq)
    h_blk[...] = (gain_row * ((x_float - mean_x) * inv_std)).astype(BF16)
    norm[...] = jnp.where(lane == 0, mean_x, jnp.where(lane == 1, inv_std, 0.0))
    own_local(0).start()
    x_copy(0).start()
    send_own(0, 0)
    for w in range(3):
        w_copy(w, 1, xp).start()
        w_copy(w, 2, dp).start()

    def zo_copy(layer, sem, dev):
        ref = block(1, quarter(1, tx), layer * 2 + 1 - y)
        return remote(ref, ref, sem.at[layer], zo_r.at[layer], (dev, tx))

    order = ((0, 0), (0, 1), (1, 0), (1, 1))

    def pass_up(layer, copy, sem, after):
        copy(layer, sem, dn).wait_recv()

        @pl.when(z < NZ - 1)
        def _():
            copy(layer, sem, up).start()

        after(layer)

    def pass_down(layer, copy, sem, after):
        copy(layer, sem, up).wait_recv()

        @pl.when(z > 0)
        def _():
            copy(layer, sem, dn).start()

        after(layer)

    def relay(k, t, s, main=True, other=False):
        def copy(layer, sem, dev):
            return z_copy(t, s, layer, sem, dev)

        def after(layer):
            if (t, s) != (1, 1):
                y_copy(t, s, layer, layer * 2 + y).start()
            d_copy(t, s, layer * 2 + y, tx).start()

        def after_other(layer):
            d_copy(1, 1, layer * 2 + 1 - y, tx).start()

        @pl.when(z >= k)
        def _():
            if main:
                pass_up(z - k, copy, up_s, after)
            if other:
                pass_up(z - k, zo_copy, uo_s, after_other)

        @pl.when(z + k < NZ)
        def _():
            if main:
                pass_down(z + k, copy, dn_s, after)
            if other:
                pass_down(z + k, zo_copy, do_s, after_other)

    for t in (1, 0):
        x_arrive(t).wait_recv()
        send_own(t, 1)
    for s in (0, 1):
        relay(1, 0, s)
    for s in (0, 1):
        relay(2, 0, s)
    relay(1, 1, 0)
    for s in (0, 1):
        relay(3, 0, s)
    relay(2, 1, 0)
    y_copy(1, 1, z, yp).wait_recv()

    @pl.when(z < NZ - 1)
    def _():
        zo_copy(z, uo_s, up).start()

    @pl.when(z > 0)
    def _():
        zo_copy(z, do_s, dn).start()

    d_copy(1, 1, yp, tx).start()
    relay(1, 1, 1)
    own_local(0).wait()
    own_local(1).wait()

    def layer_of(n):
        m = n % NZ
        base = m + near * (1 - 2 * m) * (1 - m // 2)
        return base + hi * (NZ - 1 - 2 * base)

    def tile_row(n):
        return layer_of(n) * 2 + y + (n // NZ) * (1 - 2 * y)

    chip = tx // 2

    def tile_copy(t, n, half=None):
        rows = span(tile_row(n), tb)
        if half is None:
            return pltpu.make_async_copy(gathered[t].at[rows, :], tiles.at[n % 2], t_l.at[n % 2])
        return pltpu.make_async_copy(gathered[t].at[rows, span(half, 2 * dq)], tiles.at[n % 2, :, pl.ds(0, 2 * dq)],
                                     t_l.at[n % 2])

    swaps = (act, gate_g, up_g)

    def e_copy(i, row_ty):
        rows = span(row_ty, tb)
        return remote(swaps[i].at[0, rows, :], swaps[i].at[1, rows, :], e_s.at[i, row_ty], e_r.at[i, row_ty],
                      (ty, cp))

    def fetch_near(n):
        row_ty = tile_row(n)

        @pl.when(n >= NZ)
        def _():
            for s in (0, 1):
                y_copy(0, s, layer_of(n), row_ty).wait_recv()
                d_copy(0, s, row_ty, tx).start()

        d_copy(0, 0, row_ty, cp).wait_recv()
        tile_copy(0, n, chip).start()

    def near_step(n, _):
        @pl.when(n < NTY - 1)
        def _():
            fetch_near(n + 1)

        row_ty = tile_row(n)
        tile_copy(0, n, chip).wait()
        h_rows = tiles[n % 2, :, pl.ds(0, 2 * dq)]
        part[1, row_ty] = matmul(h_rows, w1f[span(chip, 2 * dq), :])
        v_buf[row_ty] = matmul(h_rows, w3f[span(chip, 2 * dq), :])
        return 0

    for w in (0, 1):
        w_local(w).wait()
        w_arrive(w, 0, cp).wait_recv()
    fetch_near(0)
    lax.fori_loop(0, NTY, near_step, 0)
    relay(1, 1, 1, main=False, other=True)
    relay(3, 1, 0)
    for w in (0, 1):
        w_arrive(w, 1, xp).wait_recv()
        w_arrive(w, 2, dp).wait_recv()
    def sub_rows(sub):
        return span(sub, SUB)

    def q_copy(i):
        mat, layer, sub = item_of(i)
        return remote(part.at[mat, layer * 2 + 1 - y, sub_rows(sub), :], y_recv.at[mat, layer, sub_rows(sub), :],
                      q_s.at[i], q_r.at[i], (yp, tx))

    def send_pair(mat, pair):
        for e in range(2 * SUBS):
            q_copy((mat * 2 + pair) * 2 * SUBS + e).start()

    def part_row(jj):
        return pair_layer(jj % NZ // 2, jj % 2) * 2 + 1 - y + (jj // NZ) * (2 * y - 1)

    def far_copy(jj):
        src = hg.at[span(part_row(jj), tb), span(1 - chip, 2 * dq)]
        return pltpu.make_async_copy(src, tiles.at[jj % 2, :, pl.ds(0, 2 * dq)], t_l.at[jj % 2])

    def fetch_far(jj):
        d_copy(0, 1, part_row(jj), cp).wait_recv()
        far_copy(jj).start()

    def far_step(jj, _):
        @pl.when(jj % 2 == 1)
        def _():
            e_copy(0, part_row(jj - 1)).start()

        @pl.when(jj < NTY - 1)
        def _():
            fetch_far(jj + 1)

        row_ty = part_row(jj)
        far_copy(jj).wait()
        h_rows = tiles[jj % 2, :, pl.ds(0, 2 * dq)]
        gate = part[1, row_ty] + matmul(h_rows, w1f[span(1 - chip, 2 * dq), :])
        up_v = v_buf[row_ty] + matmul(h_rows, w3f[span(1 - chip, 2 * dq), :])
        part[1, row_ty] = gate
        v_buf[row_ty] = up_v
        act[0, span(row_ty, tb), :] = (gate * jax.nn.sigmoid(gate) * up_v).astype(BF16)
        return 0

    def m_step(jj, _):
        row_ty = part_row(jj)
        rows = span(row_ty, tb)
        e_copy(0, row_ty).wait_recv()
        part[0, row_ty] = (matmul(act[0, rows, :], w2_own[span(core, fh), :])
                           + matmul(act[1, rows, :], w2_own[span(1 - core, fh), :]))
        return 0

    def two_tiles(g, _):
        lax.fori_loop(2 * g, 2 * g + 2, far_step, 0)
        e_copy(0, part_row(2 * g + 1)).start()
        lax.fori_loop(2 * g, 2 * g + 2, m_step, 0)

        @pl.when(g < 2)
        def _():
            send_pair(0, g)

        @pl.when(g == 0)
        def _():
            relay(2, 1, 1, other=True)

        return 0

    w2_own_copy.wait()
    fetch_far(0)
    lax.fori_loop(0, NTY // 2, two_tiles, 0)
    hq, dyq = w1f.at[pl.ds(0, tokens), :], w3f.at[pl.ds(0, tokens), :]
    hq_copy = pltpu.make_async_copy(hg.at[:, span(tx, dq)], hq, l_l.at[1])
    dyq_copy = pltpu.make_async_copy(dyg.at[:, span(tx, dq)], dyq, l_l.at[2])
    hq_copy.start()

    relay(3, 1, 1, other=True)

    def dy_arrive(layer, _):
        row_ty = layer * 2 + 1 - y
        y_copy(1, 0, layer, row_ty).wait_recv()
        d_copy(1, 0, row_ty, tx).start()
        return 0

    lax.fori_loop(0, NZ, dy_arrive, 0)
    dyq_copy.start()

    def c_refs(i):
        mat, layer, sub = item_of(i)
        return part.at[mat, layer * 2 + y, sub_rows(sub), :]

    def c_up(i):
        return remote(c_refs(i), z_buf.at[i], c_s.at[i], c_r.at[i], (up, tx))

    def c_dn(i):
        return remote(c_refs(i), z_buf.at[i], c_s.at[i], c_r.at[i], (dn, tx))

    def c_fin(i):
        mat, _, sub = item_of(i)
        k = mat * SUBS + sub
        return remote(c_refs(i), z_fin.at[k], c_s.at[i], f_r.at[k], (dn, tx))

    def add_to(i, value):
        mat, layer, sub = item_of(i)
        part[mat, layer * 2 + y, sub_rows(sub), :] = part[mat, layer * 2 + y, sub_rows(sub), :] + value

    def add_run(i):
        c_up(i).wait_recv()
        add_to(i, z_buf[i])

    def slot_step(slot):
        @pl.when(slot < ITEMS)
        def _():
            mat, layer, sub = item_of(slot)
            q_copy(slot).wait_recv()
            add_to(slot, y_recv[mat, layer, sub_rows(sub), :])

        i_up = slot - LAG * z
        l_up = item_of(jnp.maximum(i_up, 0))[1]

        @pl.when(jnp.logical_and(jnp.logical_and(i_up >= 0, i_up < ITEMS), l_up > z))
        def _():
            @pl.when(z > 0)
            def _():
                add_run(i_up)

            c_up(i_up).start()

        i_dn = slot - LAG * (NZ - 1 - z)
        l_dn = item_of(jnp.maximum(i_dn, 0))[1]

        @pl.when(jnp.logical_and(jnp.logical_and(i_dn >= 0, i_dn < ITEMS), l_dn < z))
        def _():
            @pl.when(z < NZ - 1)
            def _():
                add_run(i_dn)

            @pl.when(l_dn < z - 1)
            def _():
                c_dn(i_dn).start()

            @pl.when(l_dn == z - 1)
            def _():
                c_fin(i_dn).start()

        i_fin = slot - LAG * far
        l_fin = item_of(jnp.maximum(i_fin, 0))[1]

        @pl.when(jnp.logical_and(jnp.logical_and(i_fin >= 0, i_fin < ITEMS), l_fin == z))
        def _():
            mat, layer, sub = item_of(i_fin)

            @pl.when(z > 0)
            def _():
                add_run(i_fin)

            @pl.when(z < NZ - 1)
            def _():
                c_fin(i_fin).wait_recv()
                add_to(i_fin, z_fin[mat * SUBS + sub])

            rows = sub_rows(sub)

            @pl.when(mat == 0)
            def _():
                y_out[rows, :] = (x_ref[rows, :].astype(F32) + part[0, layer * 2 + y, rows, :]).astype(BF16)

            @pl.when(mat == 1)
            def _():
                d_h = part[1, layer * 2 + y, rows, :]
                x_hat = (x_ref[rows, :].astype(F32) - norm[rows, 0:1]) * norm[rows, 1:2]
                d_xhat = d_h * gain_ref[...].reshape(1, dq)
                sub_lane = lax.broadcasted_iota(jnp.int32, (SUB, 128), 1)
                pack[rows, :] = jnp.where(sub_lane == 0, jnp.sum(d_xhat, axis=1, keepdims=True),
                                          jnp.where(sub_lane == 1, jnp.sum(d_xhat * x_hat, axis=1, keepdims=True), 0.0))
                dg_buf[dg_row, :] = dg_buf[dg_row, :] + jnp.sum((d_h * x_hat).reshape(SUB // 8, 8, dq), axis=0)

    def fetch_dy(n):
        for s in (0, 1):
            d_copy(1, s, tile_row(n), cp).wait_recv()
        tile_copy(1, n).start()

    def early_slots(slot, _):
        slot_step(slot)
        return 0

    lax.fori_loop(0, NTY, early_slots, 0)
    wait_w(2)
    fetch_dy(0)

    def down_step(n, _):
        @pl.when(n > 0)
        def _():
            e_copy(1, tile_row(n - 1)).start()
            e_copy(2, tile_row(n - 1)).start()

        @pl.when(n < NTY - 1)
        def _():
            fetch_dy(n + 1)

        row_ty = tile_row(n)
        rows = span(row_ty, tb)
        tile_copy(1, n).wait()
        d_act = contract_cols(tiles[n % 2], w2f[...])
        gate, up_v = part[1, row_ty], v_buf[row_ty]
        sig = jax.nn.sigmoid(gate)
        gate_g[0, rows, :] = (d_act * up_v * sig * (1.0 + gate * (1.0 - sig))).astype(BF16)
        up_g[0, rows, :] = (d_act * (gate * sig)).astype(BF16)

        slot_step(NTY + n)
        return 0

    lax.fori_loop(0, NTY, down_step, 0)
    e_copy(1, tile_row(NTY - 1)).start()
    e_copy(2, tile_row(NTY - 1)).start()
    w1_own, w3_own = w2f.at[:, pl.ds(0, f_loc)], w2f.at[:, pl.ds(f_loc, f_loc)]
    w1_own_copy = pltpu.make_async_copy(w1_ref, w1_own, l_l.at[3])
    w3_own_copy = pltpu.make_async_copy(w3_ref, w3_own, l_l.at[4])
    w1_own_copy.start()
    w3_own_copy.start()
    w1_own_copy.wait()
    w3_own_copy.wait()

    def dh_step(jj, _):
        row_ty = part_row(jj)
        rows = span(row_ty, tb)
        e_copy(1, row_ty).wait_recv()
        e_copy(2, row_ty).wait_recv()
        acc = contract_cols(gate_g[0, rows, :], w1_own[:, span(core, fh)])
        acc += contract_cols(gate_g[1, rows, :], w1_own[:, span(1 - core, fh)])
        acc += contract_cols(up_g[0, rows, :], w3_own[:, span(core, fh)])
        acc += contract_cols(up_g[1, rows, :], w3_own[:, span(1 - core, fh)])
        part[1, row_ty] = acc

        @pl.when(jnp.logical_and(jj % 2 == 0, jnp.logical_and(jj > 0, jj <= NZ)))
        def _():
            send_pair(1, jj // 2 - 1)

        slot_step(2 * NTY + jj)
        return 0

    lax.fori_loop(0, NTY, dh_step, 0)
    hq_copy.wait()
    dyq_copy.wait()

    def dw_copy(c, w):
        half = c % 2
        cols = span(core + half * (1 - 2 * core), fh)
        dst = (dw2_out.at[cols, :], dw1_out.at[:, cols], dw3_out.at[:, cols])[w]
        return pltpu.make_async_copy(stage, dst, dw_l.at[0])

    def weight_grads(slot):
        c = (slot - DW_FIRST) // DW_GAP
        half = c % 2

        def over_tokens(left, right):
            def piece(k, _):
                rows = span(k, DW_ROWS)
                stage[...] = stage[...] + contract_rows(left[rows, :], right[rows, :])
                return 0

            stage[...] = jnp.zeros(stage.shape, F32)
            lax.fori_loop(0, tokens // DW_ROWS, piece, 0)

        @pl.when(jnp.logical_and((slot - DW_FIRST) % DW_GAP == 0, slot < DW_FIRST + 6 * DW_GAP))
        def _():
            @pl.when(c >= 1)
            def _():
                dw_copy(c, 0).wait()

            for w in range(3):
                @pl.when(c // 2 == w)
                def _():
                    over_tokens(act.at[half] if w == 0 else hq, (dyq, gate_g.at[half], up_g.at[half])[w])
                    dw_copy(c, w).start()

    def drain_gathers():
        for r, dev in tx_peers:
            stat_copy(r, dev).wait_send()
            for w in range(3):
                w_copy(w, r, dev).wait_send()
        for t in (0, 1):
            x_copy(t).wait_send()
        y_copy(1, 1, z, ty).wait_send()

        def drain_layer(layer, _):
            for t, s in order:
                @pl.when(jnp.logical_and(z < NZ - 1, layer <= z))
                def _():
                    z_copy(t, s, layer, up_s, up).wait_send()

                @pl.when(jnp.logical_and(z > 0, layer >= z))
                def _():
                    z_copy(t, s, layer, dn_s, dn).wait_send()

                if (t, s) != (1, 1):
                    y_copy(t, s, layer, layer * 2 + y).wait_send()
                d_copy(t, s, layer * 2, tx).wait_send()
                d_copy(t, s, layer * 2 + 1, tx).wait_send()

            @pl.when(jnp.logical_and(z < NZ - 1, layer <= z))
            def _():
                zo_copy(layer, uo_s, up).wait_send()

            @pl.when(jnp.logical_and(z > 0, layer >= z))
            def _():
                zo_copy(layer, do_s, dn).wait_send()

            return 0

        def drain_swap(row_ty, _):
            for i in range(3):
                e_copy(i, row_ty).wait_send()
            return 0

        lax.fori_loop(0, NZ, drain_layer, 0)
        lax.fori_loop(0, NTY, drain_swap, 0)

    def drain_item(i, _):
        q_copy(i).wait_send()
        layer = item_of(i)[1]

        @pl.when(layer > z)
        def _():
            c_up(i).wait_send()

        @pl.when(layer < z)
        def _():
            c_dn(i).wait_send()

        return 0

    def last_slots(slot, _):
        weight_grads(slot)
        slot_step(slot)
        drain_item(slot - DRAIN_LAG, 0)

        @pl.when(slot == DRAIN_SLOT)
        def _():
            drain_gathers()

        return 0

    lax.fori_loop(3 * NTY, ITEMS + LAG * (NZ - 2), last_slots, 0)

    def dg_copy(r, row):
        ref = dg_buf.at[span(row, 8), :]
        return remote(ref, ref, dg_s.at[r], dg_r.at[row], ((ty + r) % NTY, tx))

    def sb_copy(r, dev):
        return remote(sb_src, sb_buf.at[r], sb_s.at[r], sb_r.at[r], (ty, dev))

    sb_src[...] = pack[...].T[:8]
    for r in range(1, NTY):
        dg_copy(r, ty).start()
    for r, dev in tx_peers:
        sb_copy(r, dev).start()
    inv_std = norm[:, 1:2]
    x_hat = (x_ref[...].astype(F32) - norm[:, 0:1]) * inv_std
    d_xhat = part[1, ty] * gain_ref[...].reshape(1, dq)
    for r, dev in tx_peers:
        sb_copy(r, dev).wait_recv()
    total = sb_src[...] + sb_buf[0] + sb_buf[1] + sb_buf[2]
    total = jnp.concatenate([total, jnp.zeros((120, tb), F32)], axis=0).T / d_model
    dx_ln = inv_std * (d_xhat - total[:, 0:1] - x_hat * total[:, 1:2])
    dx_out[...] = (dy_ref[...].astype(F32) + dx_ln).astype(BF16)
    for r in range(1, NTY):
        dg_copy(r, (ty + NTY - r) % NTY).wait_recv()
    dg_out[...] = jnp.sum(dg_buf[...], axis=0)

    dw_copy(0, 0).wait()
    for r in range(1, NTY):
        dg_copy(r, ty).wait_send()
    for r, dev in tx_peers:
        sb_copy(r, dev).wait_send()
    lax.fori_loop(ITEMS + LAG * (NZ - 2) - DRAIN_LAG, ITEMS, drain_item, 0)


def pieces_of(arrays):
    out = []
    for n, array in enumerate(arrays):
        cuts = 4 if array.shape[0] * array.shape[1] > 400_000 else 1
        rows = array.shape[0] // cuts
        out += [(n, pl.ds(c * rows, rows)) for c in range(cuts)]
    return out


def hand_out_kernel(*refs):
    k = (len(refs) - 4) // 3
    gain_in, ins, gain_out, outs = refs[0], refs[1:1 + k], refs[1 + k], refs[2 + k:2 + 2 * k]
    bufs, (in_sem, out_sem) = refs[2 + 2 * k:2 + 3 * k], refs[2 + 3 * k:]
    pieces = pieces_of(ins)
    loads = [pltpu.make_async_copy(ins[n].at[rows, :], bufs[n].at[rows, :], in_sem.at[c])
             for c, (n, rows) in enumerate(pieces)]
    stores = [pltpu.make_async_copy(bufs[n].at[rows, :], outs[n].at[rows, :], out_sem.at[c])
              for c, (n, rows) in enumerate(pieces)]
    for load in loads:
        load.start()
    gain_out[...] = gain_in[...]
    for load, store in zip(loads, stores):
        load.wait()
        store.start()
    for store in stores:
        store.wait()


def hand_out(gain, arrays):
    k = len(arrays)
    vmem = pl.BlockSpec(memory_space=pltpu.VMEM)
    hbm = pl.BlockSpec(memory_space=pl.ANY)
    n_pieces = len(pieces_of(arrays))
    return pl.pallas_call(
        hand_out_kernel,
        out_shape=[jax.ShapeDtypeStruct(a.shape, a.dtype) for a in (gain, *arrays)],
        in_specs=[vmem] + [hbm] * k,
        out_specs=[vmem] + [hbm] * k,
        scratch_shapes=[pltpu.VMEM(a.shape, a.dtype) for a in arrays]
        + [pltpu.SemaphoreType.DMA((n_pieces,)), pltpu.SemaphoreType.DMA((n_pieces,))],
        compiler_params=pltpu.CompilerParams(vmem_limit_bytes=60_000_000),
    )(gain, *arrays)


def solution(mesh):
    def local_step(x_blk, dy_blk, gain_blk, w1, w3, w2):
        tb, dq = x_blk.shape
        tokens, d_model, f_loc = tb * NTY, dq * NTX, w1.shape[1]
        fh = f_loc // 2
        dma = pltpu.SemaphoreType.DMA
        vmem = pl.BlockSpec(memory_space=pltpu.VMEM)
        hbm = pl.BlockSpec(memory_space=pl.ANY)
        outs = pl.pallas_call(
            step_kernel,
            out_shape=[
                jax.ShapeDtypeStruct((tb, dq), BF16), jax.ShapeDtypeStruct((tb, dq), BF16),
                jax.ShapeDtypeStruct((dq, f_loc), F32), jax.ShapeDtypeStruct((dq, f_loc), F32),
                jax.ShapeDtypeStruct((f_loc, dq), F32), jax.ShapeDtypeStruct((dq,), F32),
                jax.ShapeDtypeStruct((tokens, d_model), BF16), jax.ShapeDtypeStruct((tokens, d_model), BF16)],
            in_specs=[vmem, vmem, vmem, hbm, hbm, hbm],
            out_specs=[vmem, vmem, hbm, hbm, hbm, vmem, hbm, hbm],
            scratch_shapes=[
                pltpu.VMEM((tb, dq), BF16), pltpu.VMEM((2, tb, d_model), BF16),
                pltpu.VMEM((d_model, fh), BF16), pltpu.VMEM((d_model, fh), BF16), pltpu.VMEM((fh, d_model), BF16),
                pltpu.VMEM((f_loc, dq), BF16),
                pltpu.VMEM((2, NTY, tb, dq), F32), pltpu.VMEM((NTY, tb, fh), F32),
                pltpu.VMEM((2, tokens, fh), BF16), pltpu.VMEM((2, tokens, fh), BF16), pltpu.VMEM((2, tokens, fh), BF16),
                pltpu.VMEM((2, NZ, tb, dq), F32), pltpu.VMEM((ITEMS, SUB, dq), F32), pltpu.VMEM((2 * SUBS, SUB, dq), F32),
                pltpu.VMEM((fh, dq), F32),
                pltpu.VMEM((8, tb), F32), pltpu.VMEM((3, 8, tb), F32),
                pltpu.VMEM((tb, 128), F32), pltpu.VMEM((8, tb), F32), pltpu.VMEM((3, 8, tb), F32),
                pltpu.VMEM((8 * NTY, dq), F32), pltpu.VMEM((tb, 128), F32),
                dma((3,)), dma((3,)), dma((2,)), dma((2,)),
                dma((2, 2, NZ)), dma((2, 2, NZ)), dma((2, 2, NZ)), dma((NZ,)), dma((NZ,)), dma((NZ,)),
                dma((2, 2, NZ)), dma((2, 2, NZ)),
                dma((2, 2, NTY)), dma((2, 2, NTY)),
                dma((3, 3)), dma((3, 3)), dma((3,)),
                dma((3, NTY)), dma((3, NTY)), dma((2,)), dma((2,)), dma((5,)),
                dma((ITEMS,)), dma((ITEMS,)), dma((ITEMS,)), dma((ITEMS,)), dma((2 * SUBS,)),
                dma((1,)), dma((3,)), dma((3,)), dma((NTY,)), dma((NTY,)),
            ],
            compiler_params=pltpu.CompilerParams(collective_id=0, has_side_effects=True,
                                                 vmem_limit_bytes=67_000_000),
            cost_estimate=pl.CostEstimate(flops=24 * tokens * d_model * fh, bytes_accessed=80_000_000,
                                          transcendentals=2 * tokens * fh),
        )(x_blk, dy_blk, gain_blk, w1, w3, w2)
        d_gain_blk, *rest = hand_out(outs[5], outs[:5])
        return (*rest, d_gain_blk)

    return jax.shard_map(
        local_step, mesh=mesh,
        in_specs=(P("ty", "tx"), P("ty", "tx"), P("tx"), P("tx", "ty"), P("tx", "ty"), P("ty", "tx")),
        out_specs=(P("ty", "tx"), P("ty", "tx"), P("tx", "ty"), P("tx", "ty"), P("ty", "tx"), P("tx")),
        check_vma=False)
```

```python
import jax
import jax.numpy as jnp
from jax import lax
from jax.experimental import pallas as pl
from jax.experimental.pallas import tpu as pltpu
from jax.sharding import PartitionSpec as P

LN_EPS = 1e-6
MESH = pl.DeviceIdType.MESH
F32 = jnp.float32
BF16 = jnp.bfloat16
NZ = 4
NTY = 8
NTX = 4
SUB = 16
SUBS = 16
ITEMS = 2 * NZ * SUBS
LAG = 5
DW_FIRST = 56
DW_GAP = 6
DW_ROWS = 512
DRAIN_LAG = 48
DRAIN_SLOT = 92


def contract_rows(left_op, right_op):
    return lax.dot_general(left_op, right_op, (((0,), (0,)), ((), ())), preferred_element_type=F32)


def contract_cols(left_op, right_op):
    return lax.dot_general(left_op, right_op, (((1,), (1,)), ((), ())), preferred_element_type=F32)


def matmul(left_op, right_op):
    return jnp.dot(left_op, right_op, preferred_element_type=F32)


def remote(src, dst, send_sem, recv_sem, device):
    return pltpu.make_async_remote_copy(src_ref=src, dst_ref=dst, send_sem=send_sem, recv_sem=recv_sem,
                                        device_id=device, device_id_type=MESH)


def span(index, size):
    return pl.ds(pl.multiple_of(index * size, size), size)


def item_of(i):
    e = i % (NZ * SUBS)
    return i // (NZ * SUBS), pair_layer(e // (2 * SUBS), e % 2), e % (2 * SUBS) // 2


def pair_layer(pair, side):
    return pair + side * (NZ - 1 - 2 * pair)


def step_kernel(x_ref, dy_ref, gain_ref, w1_ref, w3_ref, w2_ref,
                y_out, dx_out, dw1_out, dw3_out, dw2_out, dg_out, hg, dyg,
                h_blk, tiles, w1f, w3f, w2f, w2_own, part, v_buf, act, gate_g, up_g, y_recv, z_buf, z_fin, stage,
                st_src, st_buf, pack, sb_src, sb_buf, dg_buf, norm,
                st_s, st_r, x_s, x_r, up_s, dn_s, z_r, uo_s, do_s, zo_r, y_s, y_r, d_s, d_r, w_s, w_r, w_l, e_s, e_r, t_l, o_l, l_l,
                q_s, q_r, c_s, c_r, f_r, dw_l, sb_s, sb_r, dg_s, dg_r):
    ty, tx = lax.axis_index("ty"), lax.axis_index("tx")
    z, y, core = ty // 2, ty % 2, tx % 2
    yp, up, dn = ty + 1 - 2 * y, ty + 2, ty - 2
    cp, xp, dp = tx + 1 - 2 * core, (tx + 2) % NTX, NTX - 1 - tx
    tx_peers = ((0, cp), (1, xp), (2, dp))
    tb, dq = x_ref.shape
    d_model = dq * NTX
    tokens = tb * NTY
    f_loc = w1_ref.shape[1]
    fh = f_loc // 2
    hi = z // 2
    near = z * (1 - hi) + (NZ - 1 - z) * hi
    far = NZ - 1 - near

    barrier = pltpu.get_barrier_semaphore()
    for _, dev in tx_peers:
        pl.semaphore_signal(barrier, inc=1, device_id=(ty, dev), device_id_type=MESH)
    for r in range(1, NTY):
        pl.semaphore_signal(barrier, inc=1, device_id=((ty + r) % NTY, tx), device_id_type=MESH)

    w_shards = (w1_ref, w3_ref, w2_ref)
    w_full = (w1f, w3f, w2f)

    def w_refs(w, c):
        mine = span(tx, dq)
        if w == 2:
            return w_shards[w].at[span(c, fh), :], w_full[w].at[:, mine]
        return w_shards[w].at[:, span(c, fh)], w_full[w].at[mine, :]

    def w_local(w):
        src, dst = w_refs(w, core)
        return pltpu.make_async_copy(src, dst, w_l.at[w])

    def w_copy(w, r, dev):
        src, dst = w_refs(w, dev % 2)
        return remote(src, dst, w_s.at[w, r], w_r.at[w, r], (ty, dev))

    def w_arrive(w, r, dev):
        theirs = span(dev, dq)
        dst = w_full[w].at[:, theirs] if w == 2 else w_full[w].at[theirs, :]
        return remote(dst, dst, w_s.at[w, r], w_r.at[w, r], (ty, dev))

    def wait_w(w):
        w_local(w).wait()
        for r, dev in tx_peers:
            w_arrive(w, r, dev).wait_recv()

    for w in range(3):
        w_local(w).start()
    w2_own_copy = pltpu.make_async_copy(w2_ref, w2_own, l_l.at[0])
    w2_own_copy.start()
    gathered = (hg, dyg)
    own_blk = (h_blk, dy_ref)

    def block(t, q, row_ty):
        return gathered[t].at[span(row_ty, tb), span(q, dq)]

    def own_local(t):
        return pltpu.make_async_copy(own_blk[t], block(t, tx, ty), o_l.at[t])

    own_local(1).start()

    x_float = x_ref[...].astype(F32)
    lane = lax.broadcasted_iota(jnp.int32, (tb, 128), 1)
    sum_1 = jnp.sum(x_float, axis=1, keepdims=True)
    sum_2 = jnp.sum(x_float * x_float, axis=1, keepdims=True)
    st_src[...] = jnp.where(lane == 0, sum_1, jnp.where(lane == 1, sum_2, 0.0)).T[:8]
    dg_row = span(ty, 8)
    dg_buf[dg_row, :] = jnp.zeros((8, dq), F32)

    pl.semaphore_wait(barrier, NTY + NTX - 2)

    def quarter(s, q):
        return q if s == 0 else (q + 2) % NTX

    def stat_copy(r, dev):
        return remote(st_src, st_buf.at[r], st_s.at[r], st_r.at[r], (ty, dev))

    def x_copy(t):
        return remote(own_blk[t], block(t, tx, ty), x_s.at[t], x_r.at[t], (ty, xp))

    def x_arrive(t):
        ref = block(t, xp, ty)
        return remote(ref, ref, x_s.at[t], x_r.at[t], (ty, xp))

    def z_copy(t, s, layer, sem, dev, own=False):
        ref = block(t, quarter(s, tx), layer * 2 + y)
        return remote(own_blk[t] if own else ref, ref, sem.at[t, s, layer], z_r.at[t, s, layer], (dev, tx))

    def y_copy(t, s, layer, row_ty, own=False):
        ref = block(t, quarter(s, tx), row_ty)
        return remote(own_blk[t] if own else ref, ref, y_s.at[t, s, layer], y_r.at[t, s, layer], (yp, tx))

    def d_copy(t, s, row_ty, q, own=False):
        ref = block(t, quarter(s, q), row_ty)
        return remote(own_blk[t] if own else ref, ref, d_s.at[t, s, row_ty], d_r.at[t, s, row_ty], (ty, cp))

    def spread(t, s, layer, own=False):
        y_copy(t, s, layer, layer * 2 + y, own).start()
        d_copy(t, s, layer * 2 + y, tx, own).start()

    def send_own(t, s):
        @pl.when(z < NZ - 1)
        def _():
            z_copy(t, s, z, up_s, up, s == 0).start()

        @pl.when(z > 0)
        def _():
            z_copy(t, s, z, dn_s, dn, s == 0).start()

        spread(t, s, z, s == 0)

    for r, dev in tx_peers:
        stat_copy(r, dev).start()
    for w in range(3):
        w_copy(w, 0, cp).start()
    x_copy(1).start()
    send_own(1, 0)
    for r, dev in tx_peers:
        stat_copy(r, dev).wait_recv()
    total = st_src[...] + st_buf[0] + st_buf[1] + st_buf[2]
    total = jnp.concatenate([total, jnp.zeros((120, tb), F32)], axis=0).T
    mean_x = total[:, 0:1] / d_model
    inv_std = lax.rsqrt(total[:, 1:2] / d_model - mean_x * mean_x + LN_EPS)
    gain_row = gain_ref[...].reshape(1, dq)
    h_blk[...] = (gain_row * ((x_float - mean_x) * inv_std)).astype(BF16)
    norm[...] = jnp.where(lane == 0, mean_x, jnp.where(lane == 1, inv_std, 0.0))
    own_local(0).start()
    x_copy(0).start()
    send_own(0, 0)
    for w in range(3):
        w_copy(w, 1, xp).start()
        w_copy(w, 2, dp).start()

    def zo_copy(layer, sem, dev):
        ref = block(1, quarter(1, tx), layer * 2 + 1 - y)
        return remote(ref, ref, sem.at[layer], zo_r.at[layer], (dev, tx))

    order = ((0, 0), (0, 1), (1, 0), (1, 1))

    def pass_up(layer, copy, sem, after):
        copy(layer, sem, dn).wait_recv()

        @pl.when(z < NZ - 1)
        def _():
            copy(layer, sem, up).start()

        after(layer)

    def pass_down(layer, copy, sem, after):
        copy(layer, sem, up).wait_recv()

        @pl.when(z > 0)
        def _():
            copy(layer, sem, dn).start()

        after(layer)

    def relay(k, t, s, main=True, other=False):
        def copy(layer, sem, dev):
            return z_copy(t, s, layer, sem, dev)

        def after(layer):
            if (t, s) != (1, 1):
                y_copy(t, s, layer, layer * 2 + y).start()
            d_copy(t, s, layer * 2 + y, tx).start()

        def after_other(layer):
            d_copy(1, 1, layer * 2 + 1 - y, tx).start()

        @pl.when(z >= k)
        def _():
            if main:
                pass_up(z - k, copy, up_s, after)
            if other:
                pass_up(z - k, zo_copy, uo_s, after_other)

        @pl.when(z + k < NZ)
        def _():
            if main:
                pass_down(z + k, copy, dn_s, after)
            if other:
                pass_down(z + k, zo_copy, do_s, after_other)

    for t in (1, 0):
        x_arrive(t).wait_recv()
        send_own(t, 1)
    for s in (0, 1):
        relay(1, 0, s)
    for s in (0, 1):
        relay(2, 0, s)
    relay(1, 1, 0)
    for s in (0, 1):
        relay(3, 0, s)
    relay(2, 1, 0)
    y_copy(1, 1, z, yp).wait_recv()

    @pl.when(z < NZ - 1)
    def _():
        zo_copy(z, uo_s, up).start()

    @pl.when(z > 0)
    def _():
        zo_copy(z, do_s, dn).start()

    d_copy(1, 1, yp, tx).start()
    relay(1, 1, 1)
    own_local(0).wait()
    own_local(1).wait()

    def layer_of(n):
        m = n % NZ
        base = m + near * (1 - 2 * m) * (1 - m // 2)
        return base + hi * (NZ - 1 - 2 * base)

    def tile_row(n):
        return layer_of(n) * 2 + y + (n // NZ) * (1 - 2 * y)

    chip = tx // 2

    def tile_copy(t, n, half=None):
        rows = span(tile_row(n), tb)
        if half is None:
            return pltpu.make_async_copy(gathered[t].at[rows, :], tiles.at[n % 2], t_l.at[n % 2])
        return pltpu.make_async_copy(gathered[t].at[rows, span(half, 2 * dq)], tiles.at[n % 2, :, pl.ds(0, 2 * dq)],
                                     t_l.at[n % 2])

    swaps = (act, gate_g, up_g)

    def e_copy(i, row_ty):
        rows = span(row_ty, tb)
        return remote(swaps[i].at[0, rows, :], swaps[i].at[1, rows, :], e_s.at[i, row_ty], e_r.at[i, row_ty],
                      (ty, cp))

    def fetch_near(n):
        row_ty = tile_row(n)

        @pl.when(n >= NZ)
        def _():
            for s in (0, 1):
                y_copy(0, s, layer_of(n), row_ty).wait_recv()
                d_copy(0, s, row_ty, tx).start()

        d_copy(0, 0, row_ty, cp).wait_recv()
        tile_copy(0, n, chip).start()

    def near_step(n, _):
        @pl.when(n < NTY - 1)
        def _():
            fetch_near(n + 1)

        row_ty = tile_row(n)
        tile_copy(0, n, chip).wait()
        h_rows = tiles[n % 2, :, pl.ds(0, 2 * dq)]
        part[1, row_ty] = matmul(h_rows, w1f[span(chip, 2 * dq), :])
        v_buf[row_ty] = matmul(h_rows, w3f[span(chip, 2 * dq), :])
        return 0

    for w in (0, 1):
        w_local(w).wait()
        w_arrive(w, 0, cp).wait_recv()
    fetch_near(0)
    lax.fori_loop(0, NTY, near_step, 0)
    relay(1, 1, 1, main=False, other=True)
    relay(3, 1, 0)
    for w in (0, 1):
        w_arrive(w, 1, xp).wait_recv()
        w_arrive(w, 2, dp).wait_recv()
    def sub_rows(sub):
        return span(sub, SUB)

    def q_copy(i):
        mat, layer, sub = item_of(i)
        return remote(part.at[mat, layer * 2 + 1 - y, sub_rows(sub), :], y_recv.at[mat, layer, sub_rows(sub), :],
                      q_s.at[i], q_r.at[i], (yp, tx))

    def send_pair(mat, pair):
        for e in range(2 * SUBS):
            q_copy((mat * 2 + pair) * 2 * SUBS + e).start()

    def part_row(jj):
        return pair_layer(jj % NZ // 2, jj % 2) * 2 + 1 - y + (jj // NZ) * (2 * y - 1)

    def far_copy(jj):
        src = hg.at[span(part_row(jj), tb), span(1 - chip, 2 * dq)]
        return pltpu.make_async_copy(src, tiles.at[jj % 2, :, pl.ds(0, 2 * dq)], t_l.at[jj % 2])

    def fetch_far(jj):
        d_copy(0, 1, part_row(jj), cp).wait_recv()
        far_copy(jj).start()

    def far_step(jj, _):
        @pl.when(jj % 2 == 1)
        def _():
            e_copy(0, part_row(jj - 1)).start()

        @pl.when(jj < NTY - 1)
        def _():
            fetch_far(jj + 1)

        row_ty = part_row(jj)
        far_copy(jj).wait()
        h_rows = tiles[jj % 2, :, pl.ds(0, 2 * dq)]
        gate = part[1, row_ty] + matmul(h_rows, w1f[span(1 - chip, 2 * dq), :])
        up_v = v_buf[row_ty] + matmul(h_rows, w3f[span(1 - chip, 2 * dq), :])
        part[1, row_ty] = gate
        v_buf[row_ty] = up_v
        act[0, span(row_ty, tb), :] = (gate * jax.nn.sigmoid(gate) * up_v).astype(BF16)
        return 0

    def m_step(jj, _):
        row_ty = part_row(jj)
        rows = span(row_ty, tb)
        e_copy(0, row_ty).wait_recv()
        part[0, row_ty] = (matmul(act[0, rows, :], w2_own[span(core, fh), :])
                           + matmul(act[1, rows, :], w2_own[span(1 - core, fh), :]))
        return 0

    def two_tiles(g, _):
        lax.fori_loop(2 * g, 2 * g + 2, far_step, 0)
        e_copy(0, part_row(2 * g + 1)).start()
        lax.fori_loop(2 * g, 2 * g + 2, m_step, 0)

        @pl.when(g < 2)
        def _():
            send_pair(0, g)

        @pl.when(g == 0)
        def _():
            relay(2, 1, 1, other=True)

        return 0

    w2_own_copy.wait()
    fetch_far(0)
    lax.fori_loop(0, NTY // 2, two_tiles, 0)
    hq, dyq = w1f.at[pl.ds(0, tokens), :], w3f.at[pl.ds(0, tokens), :]
    hq_copy = pltpu.make_async_copy(hg.at[:, span(tx, dq)], hq, l_l.at[1])
    dyq_copy = pltpu.make_async_copy(dyg.at[:, span(tx, dq)], dyq, l_l.at[2])
    hq_copy.start()

    relay(3, 1, 1, other=True)

    def dy_arrive(layer, _):
        row_ty = layer * 2 + 1 - y
        y_copy(1, 0, layer, row_ty).wait_recv()
        d_copy(1, 0, row_ty, tx).start()
        return 0

    lax.fori_loop(0, NZ, dy_arrive, 0)
    dyq_copy.start()

    def c_refs(i):
        mat, layer, sub = item_of(i)
        return part.at[mat, layer * 2 + y, sub_rows(sub), :]

    def c_up(i):
        return remote(c_refs(i), z_buf.at[i], c_s.at[i], c_r.at[i], (up, tx))

    def c_dn(i):
        return remote(c_refs(i), z_buf.at[i], c_s.at[i], c_r.at[i], (dn, tx))

    def c_fin(i):
        mat, _, sub = item_of(i)
        k = mat * SUBS + sub
        return remote(c_refs(i), z_fin.at[k], c_s.at[i], f_r.at[k], (dn, tx))

    def add_to(i, value):
        mat, layer, sub = item_of(i)
        part[mat, layer * 2 + y, sub_rows(sub), :] = part[mat, layer * 2 + y, sub_rows(sub), :] + value

    def add_run(i):
        c_up(i).wait_recv()
        add_to(i, z_buf[i])

    def slot_step(slot):
        @pl.when(slot < ITEMS)
        def _():
            mat, layer, sub = item_of(slot)
            q_copy(slot).wait_recv()
            add_to(slot, y_recv[mat, layer, sub_rows(sub), :])

        i_up = slot - LAG * z
        l_up = item_of(jnp.maximum(i_up, 0))[1]

        @pl.when(jnp.logical_and(jnp.logical_and(i_up >= 0, i_up < ITEMS), l_up > z))
        def _():
            @pl.when(z > 0)
            def _():
                add_run(i_up)

            c_up(i_up).start()

        i_dn = slot - LAG * (NZ - 1 - z)
        l_dn = item_of(jnp.maximum(i_dn, 0))[1]

        @pl.when(jnp.logical_and(jnp.logical_and(i_dn >= 0, i_dn < ITEMS), l_dn < z))
        def _():
            @pl.when(z < NZ - 1)
            def _():
                add_run(i_dn)

            @pl.when(l_dn < z - 1)
            def _():
                c_dn(i_dn).start()

            @pl.when(l_dn == z - 1)
            def _():
                c_fin(i_dn).start()

        i_fin = slot - LAG * far
        l_fin = item_of(jnp.maximum(i_fin, 0))[1]

        @pl.when(jnp.logical_and(jnp.logical_and(i_fin >= 0, i_fin < ITEMS), l_fin == z))
        def _():
            mat, layer, sub = item_of(i_fin)

            @pl.when(z > 0)
            def _():
                add_run(i_fin)

            @pl.when(z < NZ - 1)
            def _():
                c_fin(i_fin).wait_recv()
                add_to(i_fin, z_fin[mat * SUBS + sub])

            rows = sub_rows(sub)

            @pl.when(mat == 0)
            def _():
                y_out[rows, :] = (x_ref[rows, :].astype(F32) + part[0, layer * 2 + y, rows, :]).astype(BF16)

            @pl.when(mat == 1)
            def _():
                d_h = part[1, layer * 2 + y, rows, :]
                x_hat = (x_ref[rows, :].astype(F32) - norm[rows, 0:1]) * norm[rows, 1:2]
                d_xhat = d_h * gain_ref[...].reshape(1, dq)
                sub_lane = lax.broadcasted_iota(jnp.int32, (SUB, 128), 1)
                pack[rows, :] = jnp.where(sub_lane == 0, jnp.sum(d_xhat, axis=1, keepdims=True),
                                          jnp.where(sub_lane == 1, jnp.sum(d_xhat * x_hat, axis=1, keepdims=True), 0.0))
                dg_buf[dg_row, :] = dg_buf[dg_row, :] + jnp.sum((d_h * x_hat).reshape(SUB // 8, 8, dq), axis=0)

    def fetch_dy(n):
        for s in (0, 1):
            d_copy(1, s, tile_row(n), cp).wait_recv()
        tile_copy(1, n).start()

    def early_slots(slot, _):
        slot_step(slot)
        return 0

    lax.fori_loop(0, 2 * NTY, early_slots, 0)
    wait_w(2)
    fetch_dy(0)

    def down_step(n, _):
        @pl.when(n > 0)
        def _():
            e_copy(1, tile_row(n - 1)).start()
            e_copy(2, tile_row(n - 1)).start()

        @pl.when(n < NTY - 1)
        def _():
            fetch_dy(n + 1)

        row_ty = tile_row(n)
        rows = span(row_ty, tb)
        tile_copy(1, n).wait()
        d_act = contract_cols(tiles[n % 2], w2f[...])
        gate, up_v = part[1, row_ty], v_buf[row_ty]
        sig = jax.nn.sigmoid(gate)
        gate_g[0, rows, :] = (d_act * up_v * sig * (1.0 + gate * (1.0 - sig))).astype(BF16)
        up_g[0, rows, :] = (d_act * (gate * sig)).astype(BF16)

        lax.fori_loop(2 * (NTY + n), 2 * (NTY + n) + 2, early_slots, 0)
        return 0

    lax.fori_loop(0, NTY, down_step, 0)
    e_copy(1, tile_row(NTY - 1)).start()
    e_copy(2, tile_row(NTY - 1)).start()
    w1_own, w3_own = w2f.at[:, pl.ds(0, f_loc)], w2f.at[:, pl.ds(f_loc, f_loc)]
    w1_own_copy = pltpu.make_async_copy(w1_ref, w1_own, l_l.at[3])
    w3_own_copy = pltpu.make_async_copy(w3_ref, w3_own, l_l.at[4])
    w1_own_copy.start()
    w3_own_copy.start()
    w1_own_copy.wait()
    w3_own_copy.wait()

    def dh_step(jj, _):
        row_ty = part_row(jj)
        rows = span(row_ty, tb)
        e_copy(1, row_ty).wait_recv()
        e_copy(2, row_ty).wait_recv()
        acc = contract_cols(gate_g[0, rows, :], w1_own[:, span(core, fh)])
        acc += contract_cols(gate_g[1, rows, :], w1_own[:, span(1 - core, fh)])
        acc += contract_cols(up_g[0, rows, :], w3_own[:, span(core, fh)])
        acc += contract_cols(up_g[1, rows, :], w3_own[:, span(1 - core, fh)])
        part[1, row_ty] = acc

        @pl.when(jnp.logical_and(jj % 2 == 0, jnp.logical_and(jj > 0, jj <= NZ)))
        def _():
            send_pair(1, jj // 2 - 1)

        lax.fori_loop(2 * (2 * NTY + jj), 2 * (2 * NTY + jj) + 2, early_slots, 0)
        return 0

    lax.fori_loop(0, NTY, dh_step, 0)
    hq_copy.wait()
    dyq_copy.wait()

    def dw_copy(c, w):
        half = c % 2
        cols = span(core + half * (1 - 2 * core), fh)
        dst = (dw2_out.at[cols, :], dw1_out.at[:, cols], dw3_out.at[:, cols])[w]
        return pltpu.make_async_copy(stage, dst, dw_l.at[0])

    def weight_grads(slot):
        c = (slot - DW_FIRST) // DW_GAP
        half = c % 2

        def over_tokens(left, right):
            def piece(k, _):
                rows = span(k, DW_ROWS)
                stage[...] = stage[...] + contract_rows(left[rows, :], right[rows, :])
                return 0

            stage[...] = jnp.zeros(stage.shape, F32)
            lax.fori_loop(0, tokens // DW_ROWS, piece, 0)

        @pl.when(jnp.logical_and((slot - DW_FIRST) % DW_GAP == 0, slot < DW_FIRST + 6 * DW_GAP))
        def _():
            @pl.when(c >= 1)
            def _():
                dw_copy(c, 0).wait()

            for w in range(3):
                @pl.when(c // 2 == w)
                def _():
                    over_tokens(act.at[half] if w == 0 else hq, (dyq, gate_g.at[half], up_g.at[half])[w])
                    dw_copy(c, w).start()

    def drain_gathers():
        for r, dev in tx_peers:
            stat_copy(r, dev).wait_send()
            for w in range(3):
                w_copy(w, r, dev).wait_send()
        for t in (0, 1):
            x_copy(t).wait_send()
        y_copy(1, 1, z, ty).wait_send()

        def drain_layer(layer, _):
            for t, s in order:
                @pl.when(jnp.logical_and(z < NZ - 1, layer <= z))
                def _():
                    z_copy(t, s, layer, up_s, up).wait_send()

                @pl.when(jnp.logical_and(z > 0, layer >= z))
                def _():
                    z_copy(t, s, layer, dn_s, dn).wait_send()

                if (t, s) != (1, 1):
                    y_copy(t, s, layer, layer * 2 + y).wait_send()
                d_copy(t, s, layer * 2, tx).wait_send()
                d_copy(t, s, layer * 2 + 1, tx).wait_send()

            @pl.when(jnp.logical_and(z < NZ - 1, layer <= z))
            def _():
                zo_copy(layer, uo_s, up).wait_send()

            @pl.when(jnp.logical_and(z > 0, layer >= z))
            def _():
                zo_copy(layer, do_s, dn).wait_send()

            return 0

        def drain_swap(row_ty, _):
            for i in range(3):
                e_copy(i, row_ty).wait_send()
            return 0

        lax.fori_loop(0, NZ, drain_layer, 0)
        lax.fori_loop(0, NTY, drain_swap, 0)

    def drain_item(i, _):
        q_copy(i).wait_send()
        layer = item_of(i)[1]

        @pl.when(layer > z)
        def _():
            c_up(i).wait_send()

        @pl.when(layer < z)
        def _():
            c_dn(i).wait_send()

        return 0

    def last_slots(slot, _):
        weight_grads(slot)
        slot_step(slot)
        drain_item(slot - DRAIN_LAG, 0)

        @pl.when(slot == DRAIN_SLOT)
        def _():
            drain_gathers()

        return 0

    lax.fori_loop(6 * NTY, ITEMS + LAG * (NZ - 2), last_slots, 0)

    def dg_copy(r, row):
        ref = dg_buf.at[span(row, 8), :]
        return remote(ref, ref, dg_s.at[r], dg_r.at[row], ((ty + r) % NTY, tx))

    def sb_copy(r, dev):
        return remote(sb_src, sb_buf.at[r], sb_s.at[r], sb_r.at[r], (ty, dev))

    sb_src[...] = pack[...].T[:8]
    for r in range(1, NTY):
        dg_copy(r, ty).start()
    for r, dev in tx_peers:
        sb_copy(r, dev).start()
    inv_std = norm[:, 1:2]
    x_hat = (x_ref[...].astype(F32) - norm[:, 0:1]) * inv_std
    d_xhat = part[1, ty] * gain_ref[...].reshape(1, dq)
    for r, dev in tx_peers:
        sb_copy(r, dev).wait_recv()
    total = sb_src[...] + sb_buf[0] + sb_buf[1] + sb_buf[2]
    total = jnp.concatenate([total, jnp.zeros((120, tb), F32)], axis=0).T / d_model
    dx_ln = inv_std * (d_xhat - total[:, 0:1] - x_hat * total[:, 1:2])
    dx_out[...] = (dy_ref[...].astype(F32) + dx_ln).astype(BF16)
    for r in range(1, NTY):
        dg_copy(r, (ty + NTY - r) % NTY).wait_recv()
    dg_out[...] = jnp.sum(dg_buf[...], axis=0)

    dw_copy(0, 0).wait()
    for r in range(1, NTY):
        dg_copy(r, ty).wait_send()
    for r, dev in tx_peers:
        sb_copy(r, dev).wait_send()
    lax.fori_loop(ITEMS + LAG * (NZ - 2) - DRAIN_LAG, ITEMS, drain_item, 0)


def pieces_of(arrays):
    out = []
    for n, array in enumerate(arrays):
        cuts = 4 if array.shape[0] * array.shape[1] > 400_000 else 1
        rows = array.shape[0] // cuts
        out += [(n, pl.ds(c * rows, rows)) for c in range(cuts)]
    return out


def hand_out_kernel(*refs):
    k = (len(refs) - 4) // 3
    gain_in, ins, gain_out, outs = refs[0], refs[1:1 + k], refs[1 + k], refs[2 + k:2 + 2 * k]
    bufs, (in_sem, out_sem) = refs[2 + 2 * k:2 + 3 * k], refs[2 + 3 * k:]
    pieces = pieces_of(ins)
    loads = [pltpu.make_async_copy(ins[n].at[rows, :], bufs[n].at[rows, :], in_sem.at[c])
             for c, (n, rows) in enumerate(pieces)]
    stores = [pltpu.make_async_copy(bufs[n].at[rows, :], outs[n].at[rows, :], out_sem.at[c])
              for c, (n, rows) in enumerate(pieces)]
    for load in loads:
        load.start()
    gain_out[...] = gain_in[...]
    for load, store in zip(loads, stores):
        load.wait()
        store.start()
    for store in stores:
        store.wait()


def hand_out(gain, arrays):
    k = len(arrays)
    vmem = pl.BlockSpec(memory_space=pltpu.VMEM)
    hbm = pl.BlockSpec(memory_space=pl.ANY)
    n_pieces = len(pieces_of(arrays))
    return pl.pallas_call(
        hand_out_kernel,
        out_shape=[jax.ShapeDtypeStruct(a.shape, a.dtype) for a in (gain, *arrays)],
        in_specs=[vmem] + [hbm] * k,
        out_specs=[vmem] + [hbm] * k,
        scratch_shapes=[pltpu.VMEM(a.shape, a.dtype) for a in arrays]
        + [pltpu.SemaphoreType.DMA((n_pieces,)), pltpu.SemaphoreType.DMA((n_pieces,))],
        compiler_params=pltpu.CompilerParams(vmem_limit_bytes=60_000_000),
    )(gain, *arrays)


def solution(mesh):
    def local_step(x_blk, dy_blk, gain_blk, w1, w3, w2):
        tb, dq = x_blk.shape
        tokens, d_model, f_loc = tb * NTY, dq * NTX, w1.shape[1]
        fh = f_loc // 2
        dma = pltpu.SemaphoreType.DMA
        vmem = pl.BlockSpec(memory_space=pltpu.VMEM)
        hbm = pl.BlockSpec(memory_space=pl.ANY)
        outs = pl.pallas_call(
            step_kernel,
            out_shape=[
                jax.ShapeDtypeStruct((tb, dq), BF16), jax.ShapeDtypeStruct((tb, dq), BF16),
                jax.ShapeDtypeStruct((dq, f_loc), F32), jax.ShapeDtypeStruct((dq, f_loc), F32),
                jax.ShapeDtypeStruct((f_loc, dq), F32), jax.ShapeDtypeStruct((dq,), F32),
                jax.ShapeDtypeStruct((tokens, d_model), BF16), jax.ShapeDtypeStruct((tokens, d_model), BF16)],
            in_specs=[vmem, vmem, vmem, hbm, hbm, hbm],
            out_specs=[vmem, vmem, hbm, hbm, hbm, vmem, hbm, hbm],
            scratch_shapes=[
                pltpu.VMEM((tb, dq), BF16), pltpu.VMEM((2, tb, d_model), BF16),
                pltpu.VMEM((d_model, fh), BF16), pltpu.VMEM((d_model, fh), BF16), pltpu.VMEM((fh, d_model), BF16),
                pltpu.VMEM((f_loc, dq), BF16),
                pltpu.VMEM((2, NTY, tb, dq), F32), pltpu.VMEM((NTY, tb, fh), F32),
                pltpu.VMEM((2, tokens, fh), BF16), pltpu.VMEM((2, tokens, fh), BF16), pltpu.VMEM((2, tokens, fh), BF16),
                pltpu.VMEM((2, NZ, tb, dq), F32), pltpu.VMEM((ITEMS, SUB, dq), F32), pltpu.VMEM((2 * SUBS, SUB, dq), F32),
                pltpu.VMEM((fh, dq), F32),
                pltpu.VMEM((8, tb), F32), pltpu.VMEM((3, 8, tb), F32),
                pltpu.VMEM((tb, 128), F32), pltpu.VMEM((8, tb), F32), pltpu.VMEM((3, 8, tb), F32),
                pltpu.VMEM((8 * NTY, dq), F32), pltpu.VMEM((tb, 128), F32),
                dma((3,)), dma((3,)), dma((2,)), dma((2,)),
                dma((2, 2, NZ)), dma((2, 2, NZ)), dma((2, 2, NZ)), dma((NZ,)), dma((NZ,)), dma((NZ,)),
                dma((2, 2, NZ)), dma((2, 2, NZ)),
                dma((2, 2, NTY)), dma((2, 2, NTY)),
                dma((3, 3)), dma((3, 3)), dma((3,)),
                dma((3, NTY)), dma((3, NTY)), dma((2,)), dma((2,)), dma((5,)),
                dma((ITEMS,)), dma((ITEMS,)), dma((ITEMS,)), dma((ITEMS,)), dma((2 * SUBS,)),
                dma((1,)), dma((3,)), dma((3,)), dma((NTY,)), dma((NTY,)),
            ],
            compiler_params=pltpu.CompilerParams(collective_id=0, has_side_effects=True,
                                                 vmem_limit_bytes=67_000_000),
            cost_estimate=pl.CostEstimate(flops=24 * tokens * d_model * fh, bytes_accessed=80_000_000,
                                          transcendentals=2 * tokens * fh),
        )(x_blk, dy_blk, gain_blk, w1, w3, w2)
        d_gain_blk, *rest = hand_out(outs[5], outs[:5])
        return (*rest, d_gain_blk)

    return jax.shard_map(
        local_step, mesh=mesh,
        in_specs=(P("ty", "tx"), P("ty", "tx"), P("tx"), P("tx", "ty"), P("tx", "ty"), P("ty", "tx")),
        out_specs=(P("ty", "tx"), P("ty", "tx"), P("tx", "ty"), P("tx", "ty"), P("ty", "tx"), P("tx")),
        check_vma=False)
```
